256 devices in a mesh: lat: 128 (over x, z, y), lev: 2 (over core).
Axes of the slice: x: 4, y: 4, z: 8, core: 2. Of those that a mesh axis runs over, the one named last changes fastest.
Arguments:
- fields: float32 [1280, 3, 16, 2560], P('lat', None, 'lev'), may hold values from 0.1 to 5
- lat_fraction: float32 [1280], P('lat'), may hold values from 0 to 1
- lon_fraction: float32 [1280], P('lat'), may hold values from 0 to 1
- lon_shift: int32 [1280], P('lat'), may hold values from 0 to 2559
- departure_row: int32 [1280], P('lat'), may hold values from 1 to 1277, as said below
- extents: int32 [128, 2], P('lat'), may hold values from 1 to 4
Outputs:
- advected: float32 [1280, 3, 16, 2560], P('lat', None, 'lev')
The draws below stay inside these ranges and needn't reach their ends.
Inputs may be any that keep to these rules, and one draw needn't show every extreme that they name: departure_row[r] lies within 39 rows of r.
All inputs are finite; a program needn't handle non-finite values.
Results may differ from the reference program's by a relative error of at most 0.0003.
Values sent between devices are 32-bit elements; how exact they have to be, the bound alone decides.
A program may use at most 128 MiB of HBM per device.

```python
import math
import jax
import jax.numpy as jnp
from jax import lax

ROWS = 10
LON = 2560
FIELDS = 3
REACH = 4
NLAT = 1280
LEV = 16
BANDS = 128


def band_phase(key):
    return jax.random.randint(jax.random.fold_in(key, 911), (), 0, 8 * ROWS)


def draw_fields(key, part):
    row_phase = band_phase(key)
    shifted_rows = (jnp.arange(NLAT, dtype=jnp.int32) + row_phase) % (8 * ROWS)
    row_angle = 2.0 * math.pi * shifted_rows.astype(jnp.float32) / (8 * ROWS)
    full_shape = (NLAT, FIELDS, LEV, LON)
    gain_row = jnp.exp(-0.5 * jnp.sin(row_angle))
    rough_part = jax.random.uniform(jax.random.fold_in(key, 23), full_shape, jnp.float32, 0.5, 2.0)
    return (gain_row[:, None, None, None] * rough_part).astype(jnp.float32)


def draw_departure_row(key, part):
    row_phase = band_phase(key)
    row_ids = jnp.arange(NLAT, dtype=jnp.int32)
    shifted_rows = (row_ids + row_phase) % (8 * ROWS)
    row_drift = jnp.clip(2 * (2 * ROWS - jnp.abs(shifted_rows - 4 * ROWS)), -2 * ROWS, 2 * ROWS)
    row_noise = jax.random.randint(jax.random.fold_in(key, 17), (NLAT,), -2 * ROWS, 2 * ROWS + 1)
    offsets = jnp.clip(row_drift + row_noise, -REACH * ROWS + 1, REACH * ROWS - 2)
    spread = jax.random.randint(jax.random.fold_in(key, 29), (NLAT,), 0, 1 << 20)
    north_offset = -(1 + spread % (REACH * ROWS - 1))
    south_offset = 1 + spread % (REACH * ROWS - 2)
    position = row_ids % ROWS
    offsets = jnp.where(position == 0, north_offset, offsets)
    offsets = jnp.where(position == ROWS - 1, south_offset, offsets)
    return jnp.clip(row_ids + offsets, 1, NLAT - 3).astype(jnp.int32)


def plant(array, rng, low, largest):
    spot = [jax.random.randint(jax.random.fold_in(rng, axis), (), 0, length) for axis, length in enumerate(array.shape)]
    widest = array.shape.index(max(array.shape))
    next_to = spot[:widest] + [(spot[widest] + 1) % array.shape[widest]] + spot[widest + 1:]
    return array.at[tuple(spot)].set(low).at[tuple(next_to)].set(largest)


def level_of(stream_key, shape, pieces, smallest, high):
    def one(axis_at, blocks):
        heights = jax.random.uniform(jax.random.fold_in(jax.random.fold_in(stream_key, 6), axis_at), (blocks,), jnp.float32, smallest / len(pieces), high / len(pieces))
        return jnp.repeat(jnp.exp(heights), shape[axis_at] // blocks).reshape((-1,) + (1,) * (len(shape) - axis_at - 1))

    gain = one(*pieces[0])
    for cut in pieces[1:]:
        gain = gain * one(*cut)
    return gain


def setup_inputs(seed: int = 0) -> dict:
    key_of = jax.random.split(jax.random.key(seed), 7)
    return {
        "fields": draw_fields(jax.random.fold_in(key_of[6], 71), 0),
        "lat_fraction": jnp.clip(1.0 * jax.random.uniform(key_of[1], (NLAT,), jnp.float32) ** level_of(key_of[1], (NLAT,), ((0, 128),), -0.2, 0.2), 0.0, 1.0),
        "lon_fraction": jnp.clip(1.0 * jax.random.uniform(key_of[2], (NLAT,), jnp.float32) ** level_of(key_of[2], (NLAT,), ((0, 128),), -0.2, 0.2), 0.0, 1.0),
        "lon_shift": plant(jax.random.randint(key_of[3], (NLAT,), 0, LON), jax.random.fold_in(key_of[3], 1), 0, LON - 1).astype(jnp.int32),
        "departure_row": draw_departure_row(jax.random.fold_in(key_of[6], 71), 0),
        "extents": plant(jax.random.randint(key_of[5], (BANDS, 2), 1, REACH + 1), jax.random.fold_in(key_of[5], 1), 1, REACH).astype(jnp.int32),
    }


def cubic_weights(fraction):
    return jnp.stack([-fraction * (fraction - 1.0) * (fraction - 2.0) / 6.0,
                      (fraction + 1.0) * (fraction - 1.0) * (fraction - 2.0) / 2.0,
                      -(fraction + 1.0) * fraction * (fraction - 2.0) / 2.0,
                      (fraction + 1.0) * fraction * (fraction - 1.0) / 6.0])


def along_lon(column, lon_w, shift_value):
    lon_count = column.shape[-1]
    doubled = jnp.concatenate([column, column], axis=-1)
    result = jnp.zeros_like(column)
    for offset in range(4):
        first = ((shift_value + offset - 1) % lon_count).astype(jnp.int32)
        result = result + lon_w[offset] * lax.dynamic_slice_in_dim(doubled, first, lon_count, 2)
    return result


def reference(fields, lat_fraction, lon_fraction, lon_shift, departure_row, extents):
    row_ids = jnp.arange(NLAT, dtype=jnp.int32)
    band_ids = row_ids // ROWS
    low_bound = band_ids * ROWS - extents[band_ids, 0] * ROWS + 1
    high_bound = band_ids * ROWS + ROWS - 3 + extents[band_ids, 1] * ROWS
    departure = jnp.clip(jnp.clip(departure_row, low_bound, high_bound), 1, NLAT - 3).astype(jnp.int32)

    def one_row(inputs):
        dep_value, lat_t, lon_t, shift_value = inputs
        row_block = lax.dynamic_slice_in_dim(fields, (dep_value - 1).astype(jnp.int32), 4, 0)
        lat_w = cubic_weights(lat_t)
        column = lat_w[0] * row_block[0] + lat_w[1] * row_block[1] + lat_w[2] * row_block[2] + lat_w[3] * row_block[3]
        return along_lon(column, cubic_weights(lon_t), shift_value)

    moved = lax.map(one_row, (departure, lat_fraction, lon_fraction, lon_shift))
    area = jnp.cos(math.pi * (row_ids.astype(jnp.float32) + 0.5) / NLAT - math.pi / 2.0)
    mass_before = jnp.sum(area[:, None, None, None] * fields, axis=(0, 2, 3))
    mass_after = jnp.sum(area[:, None, None, None] * moved, axis=(0, 2, 3))
    return moved * (mass_before / mass_after)[None, :, None, None]
```

```python
import functools
import math

import jax
import jax.numpy as jnp
import numpy as np
from jax import lax
from jax.experimental import pallas as pl
from jax.experimental.pallas import tpu as pltpu
from jax.sharding import PartitionSpec as P

REACH = 4
LANES = 128
RING = 4
DEEP = 8
MESH = pl.DeviceIdType.MESH


def cubic(t):
    sixth = 1.0 / 6.0
    return (
        -t * (t - 1.0) * (t - 2.0) * sixth,
        (t + 1.0) * (t - 1.0) * (t - 2.0) * 0.5,
        -(t + 1.0) * t * (t - 2.0) * 0.5,
        (t + 1.0) * t * (t - 1.0) * sixth,
    )


def departure_of(row, first_row, rows, total_rows, departure_ref, extents_ref):
    low = first_row - extents_ref[0, 0] * rows + 1
    high = first_row + rows - 3 + extents_ref[0, 1] * rows
    inside = jnp.minimum(jnp.maximum(departure_ref[row], low), high)
    return jnp.minimum(jnp.maximum(inside, 1), total_rows - 3)


def exchange_kernel(bands, levs, lat_t_ref, lon_t_ref, departure_ref, extents_ref, area_ref, fields_ref,
                    out_ref, sums_ref, *scratch):
    rows, field_count, _, lon_count = fields_ref.shape
    held = scratch[0]
    window = scratch[1:1 + field_count]
    column = scratch[1 + field_count:1 + 2 * field_count]
    (real_meta, whole_meta, real_smem, whole_smem, part, met_one, met_two, met_three,
     load_sem, own_sem, smem_sem, meta_send, meta_recv, out_send, out_recv, halo_send, halo_recv,
     back_send, back_recv, one_send, one_recv, two_send, two_recv, three_send, three_recv,
     ) = scratch[1 + 2 * field_count:]
    band, lev = lax.axis_index("lat"), lax.axis_index("lev")
    group, member = band // RING, lax.rem(band, RING)
    groups = bands // RING
    crosses = groups // DEEP
    deep, cross = lax.rem(group, DEEP), group // DEEP
    first_row, total_rows = band * rows, bands * rows
    span = RING * rows
    piece = lon_count // RING

    def ring_member(step):
        return lax.rem(member + step, RING)

    def ring_peer(step):
        return group * RING + ring_member(step)

    def inside(distance):
        place = band + distance
        return jnp.logical_and(place >= 0, place < bands)

    near = [d for d in range(-REACH, REACH + 1) if d != 0]
    one_peers = [(dy, dl) for dy in range(RING) for dl in range(levs) if (dy, dl) != (0, 0)]

    def one_peer(dy, dl):
        return {"lat": ring_peer(dy), "lev": lax.rem(lev + dl, levs)}

    def two_peer(dx):
        return {"lat": (lax.rem(cross + dx, crosses) * DEEP + deep) * RING + member}

    def three_peer(dz):
        return {"lat": (cross * DEEP + lax.rem(deep + dz, DEEP)) * RING + member}

    barrier = pltpu.get_barrier_semaphore()

    def greet(peer):
        pl.semaphore_signal(barrier, inc=1, device_id=peer, device_id_type=MESH)

    for d in near:
        pl.when(inside(d))(functools.partial(greet, {"lat": band + d}))
    for dy, dl in one_peers:
        greet(one_peer(dy, dl))
    for dx in range(1, crosses):
        greet(two_peer(dx))
    for dz in range(1, DEEP):
        greet(three_peer(dz))

    load = pltpu.make_async_copy(fields_ref, held, load_sem)
    load.start()
    own_pieces = []
    for f in range(field_count):
        copy = pltpu.make_async_copy(
            fields_ref.at[:, f, :, pl.ds(pl.multiple_of(member * piece, LANES), piece)],
            window[f].at[pl.ds(span + member * rows, rows)],
            own_sem.at[0, f],
        )
        copy.start()
        own_pieces.append(copy)

    lane = lax.broadcasted_iota(jnp.int32, (1, LANES), 1)
    lat_t = jnp.zeros((1, LANES), jnp.float32)
    lon_t = jnp.zeros((1, LANES), jnp.float32)
    area = jnp.zeros((1, LANES), jnp.float32)
    start = jnp.zeros((1, LANES), jnp.int32)
    for row in range(rows):
        here = lane == row
        lat_t = jnp.where(here, lat_t_ref[row], lat_t)
        lon_t = jnp.where(here, lon_t_ref[row], lon_t)
        area = jnp.where(here, area_ref[first_row + row], area)
        departure = departure_of(row, first_row, rows, total_rows, departure_ref, extents_ref)
        start = jnp.where(here, departure - 1, start)
    lon_w = cubic(lon_t)
    for d in near:
        @pl.when(jnp.logical_not(inside(d)))
        def _(d=d):
            real_meta[REACH + d] = jnp.zeros(real_meta.shape[1:], jnp.float32)
            whole_meta[REACH + d] = jnp.zeros(whole_meta.shape[1:], jnp.int32)
    real_meta[REACH] = jnp.concatenate(
        [*cubic(lat_t), area * (lon_w[0] + lon_w[1] + lon_w[2] + lon_w[3]), jnp.zeros((3, LANES), jnp.float32)], axis=0
    )
    whole_meta[REACH] = jnp.broadcast_to(start, whole_meta.shape[1:])

    expected = len(one_peers) + (crosses - 1) + (DEEP - 1)
    for d in near:
        expected = expected + inside(d).astype(jnp.int32)
    pl.semaphore_wait(barrier, expected)

    def meta_copies(d):
        k = near.index(d)
        return [
            pltpu.make_async_remote_copy(
                src_ref=ref.at[REACH], dst_ref=ref.at[REACH - d],
                send_sem=meta_send.at[n, k], recv_sem=meta_recv.at[n, near.index(-d)],
                device_id={"lat": band + d}, device_id_type=MESH,
            )
            for n, ref in enumerate((real_meta, whole_meta))
        ]

    def meta_arrivals(d):
        k = near.index(d)
        return [
            pltpu.make_async_remote_copy(
                src_ref=ref.at[REACH + d], dst_ref=ref.at[REACH + d],
                send_sem=meta_send.at[n, k], recv_sem=meta_recv.at[n, k],
                device_id={"lat": band + d}, device_id_type=MESH,
            )
            for n, ref in enumerate((real_meta, whole_meta))
        ]

    for d in near:
        @pl.when(inside(d))
        def _(d=d):
            for copy in meta_copies(d):
                copy.start()

    def out_copy(f, dy):
        to = ring_member(dy)
        return pltpu.make_async_remote_copy(
            src_ref=fields_ref.at[:, f, :, pl.ds(pl.multiple_of(to * piece, LANES), piece)],
            dst_ref=window[f].at[pl.ds(span + member * rows, rows)],
            send_sem=out_send.at[f, dy - 1], recv_sem=out_recv.at[f, dy - 1],
            device_id={"lat": ring_peer(dy)}, device_id_type=MESH,
        )

    def out_arrival(f, dy):
        place = window[f].at[pl.ds(span + ring_member(RING - dy) * rows, rows)]
        return pltpu.make_async_remote_copy(
            src_ref=place, dst_ref=place, send_sem=out_send.at[f, dy - 1], recv_sem=out_recv.at[f, dy - 1],
            device_id={"lat": ring_peer(RING - dy)}, device_id_type=MESH,
        )

    has_side = (group < groups - 1, group > 0)

    def halo_copy(f, dy, side):
        who = ring_member(RING - dy)
        if dy == 0:
            source = fields_ref.at[:, f, :, pl.ds(pl.multiple_of(member * piece, LANES), piece)]
        else:
            source = window[f].at[pl.ds(span + who * rows, rows)]
        return pltpu.make_async_remote_copy(
            src_ref=source,
            dst_ref=window[f].at[pl.ds((0 if side == 0 else 2 * span) + who * rows, rows)],
            send_sem=halo_send.at[side, f, dy], recv_sem=halo_recv.at[side, f, dy],
            device_id={"lat": band + (RING if side == 0 else -RING)}, device_id_type=MESH,
        )

    def halo_arrival(f, dy, side):
        place = window[f].at[pl.ds((0 if side == 0 else 2 * span) + ring_member(RING - dy) * rows, rows)]
        return pltpu.make_async_remote_copy(
            src_ref=place, dst_ref=place, send_sem=halo_send.at[side, f, dy], recv_sem=halo_recv.at[side, f, dy],
            device_id={"lat": band + (-RING if side == 0 else RING)}, device_id_type=MESH,
        )

    def start_halo(f, dy):
        for side in range(2):
            pl.when(has_side[side])(lambda side=side: halo_copy(f, dy, side).start())

    def back_copy(f, dy):
        return pltpu.make_async_remote_copy(
            src_ref=column[f].at[pl.ds(dy * rows, rows)],
            dst_ref=out_ref.at[:, f, :, pl.ds(pl.multiple_of(member * piece, LANES), piece)],
            send_sem=back_send.at[f, dy - 1], recv_sem=back_recv.at[f, dy - 1],
            device_id={"lat": ring_peer(dy)}, device_id_type=MESH,
        )

    def back_arrival(f, dy):
        place = out_ref.at[:, f, :, pl.ds(pl.multiple_of(ring_member(RING - dy) * piece, LANES), piece)]
        return pltpu.make_async_remote_copy(
            src_ref=place, dst_ref=place, send_sem=back_send.at[f, dy - 1], recv_sem=back_recv.at[f, dy - 1],
            device_id={"lat": ring_peer(RING - dy)}, device_id_type=MESH,
        )

    def back_own(f):
        return pltpu.make_async_copy(
            column[f].at[pl.ds(0, rows)],
            out_ref.at[:, f, :, pl.ds(pl.multiple_of(member * piece, LANES), piece)],
            own_sem.at[1, f],
        )

    def small_copy(source, target, sends, arrivals, k, peer):
        return pltpu.make_async_remote_copy(
            src_ref=source, dst_ref=target.at[k], send_sem=sends.at[k], recv_sem=arrivals.at[k],
            device_id=peer, device_id_type=MESH,
        )

    ones = [small_copy(part.at[0], met_one, one_send, one_recv, k, one_peer(*p)) for k, p in enumerate(one_peers)]
    twos = [small_copy(part.at[1], met_two, two_send, two_recv, dx - 1, two_peer(dx)) for dx in range(1, crosses)]
    threes = [small_copy(part.at[2], met_three, three_send, three_recv, dz - 1, three_peer(dz)) for dz in range(1, DEEP)]

    order = (1, RING - 1, *range(2, RING - 1))
    for dy in order:
        out_copy(0, dy).start()
    start_halo(0, 0)
    start_halo(1, 0)

    for d in near:
        @pl.when(inside(d))
        def _(d=d):
            for copy in meta_arrivals(d):
                copy.wait_recv()
    group_slots = pl.ds(REACH - member, RING)
    to_smem = [
        pltpu.make_async_copy(real_meta.at[group_slots], real_smem, smem_sem.at[0]),
        pltpu.make_async_copy(whole_meta.at[group_slots], whole_smem, smem_sem.at[1]),
    ]
    for copy in to_smem:
        copy.start()
    load.wait()

    def add_row(row, totals):
        taken = jnp.zeros((2 * REACH + 1, LANES), jnp.float32)
        for a in range(4):
            hit = whole_meta[:, 0, :] + a == first_row + row
            taken = taken + jnp.where(hit, real_meta[:, a, :] * real_meta[:, 4, :], 0.0)
        taken = jnp.sum(jnp.sum(taken, axis=0, keepdims=True), axis=1, keepdims=True)
        row_area = area_ref[first_row + row]
        before, after = [], []
        for f in range(field_count):
            tile = held[row, f, :, 0:LANES]
            for t in range(1, lon_count // LANES):
                tile = tile + held[row, f, :, t * LANES:(t + 1) * LANES]
            total = jnp.sum(tile, axis=0, keepdims=True)
            before.append(totals[f] + row_area * total)
            after.append(totals[field_count + f] + taken * total)
        return tuple(before + after)

    zero = jnp.zeros((1, LANES), jnp.float32)
    totals = lax.fori_loop(0, rows, add_row, (zero,) * (2 * field_count))
    part[0] = jnp.concatenate([*totals, jnp.zeros((8 - 2 * field_count, LANES), jnp.float32)], axis=0)

    def gather_small(copies, target, level):
        for copy in copies:
            copy.wait_recv()
        total = part[level]
        for k in range(len(copies)):
            total = total + target[k]
        return total

    for copy in ones:
        copy.start()
    for f in range(1, field_count):
        for dy in order:
            out_copy(f, dy).start()
    for dy in order:
        out_arrival(0, dy).wait_recv()
        start_halo(0, dy)
    for f in range(2, field_count):
        start_halo(f, 0)
    part[1] = gather_small(ones, met_one, 0)
    for copy in twos:
        copy.start()
    for dy in order:
        out_arrival(1, dy).wait_recv()
        start_halo(1, dy)
    part[2] = gather_small(twos, met_two, 1)
    for copy in threes:
        copy.start()
    for f in range(2, field_count):
        for dy in order:
            out_arrival(f, dy).wait_recv()
            start_halo(f, dy)
    for copy in to_smem:
        copy.wait()
    for copy in own_pieces:
        copy.wait()

    base = (group - 1) * span

    def interpolate(f, dy):
        to = ring_member(dy)

        def one_row(row, carry):
            place = whole_smem[to, 0, row] - base
            weight = [real_smem[to, a, row] for a in range(4)]
            for t in range(piece // LANES):
                at = pl.ds(t * LANES, LANES)
                total = weight[0] * window[f][place, :, at]
                for a in range(1, 4):
                    total = total + weight[a] * window[f][place + a, :, at]
                column[f][dy * rows + row, :, at] = total
            return carry

        lax.fori_loop(0, rows, one_row, 0)

    for f in range(field_count):
        for dy in (0, *order):
            for side in range(2):
                pl.when(has_side[1 - side])(lambda dy=dy, side=side: halo_arrival(f, dy, side).wait_recv())
        for dy in (2, 1, RING - 1, 0):
            interpolate(f, dy)
        for dy in (2, 1, RING - 1):
            back_copy(f, dy).start()
        back_own(f).start()

    sums_ref[...] = gather_small(threes, met_three, 2)

    for f in range(field_count):
        for dy in order:
            back_arrival(f, dy).wait_recv()
    for d in near:
        @pl.when(inside(d))
        def _(d=d):
            for copy in meta_copies(d):
                copy.wait_send()
    for copy in ones + twos + threes:
        copy.wait_send()
    for f in range(field_count):
        back_own(f).wait()
        for dy in order:
            out_copy(f, dy).wait_send()
            back_copy(f, dy).wait_send()
        for dy in (0, *order):
            for side in range(2):
                pl.when(has_side[side])(lambda f=f, dy=dy, side=side: halo_copy(f, dy, side).wait_send())


def exchange(lat_t, lon_t, departure_row, extents, area, fields):
    bands, levs = lax.axis_size("lat"), lax.axis_size("lev")
    rows, field_count, levels, lon_count = fields.shape
    crosses = bands // RING // DEEP
    piece = lon_count // RING
    tile = (8, LANES)
    dma = pltpu.SemaphoreType.DMA
    ones = RING * levs - 1
    near = 2 * REACH
    return pl.pallas_call(
        functools.partial(exchange_kernel, bands, levs),
        out_shape=(
            jax.ShapeDtypeStruct(fields.shape, fields.dtype),
            jax.ShapeDtypeStruct(tile, jnp.float32),
        ),
        in_specs=[pl.BlockSpec(memory_space=pltpu.SMEM)] * 5 + [pl.BlockSpec(memory_space=pl.ANY)],
        out_specs=(pl.BlockSpec(memory_space=pl.ANY), pl.BlockSpec(memory_space=pltpu.VMEM)),
        scratch_shapes=[
            pltpu.VMEM(fields.shape, jnp.float32),
            *[pltpu.VMEM((3 * RING * rows, levels, piece), jnp.float32) for _ in range(field_count)],
            *[pltpu.VMEM((RING * rows, levels, piece), jnp.float32) for _ in range(field_count)],
            pltpu.VMEM((near + 1,) + tile, jnp.float32),
            pltpu.VMEM((near + 1,) + tile, jnp.int32),
            pltpu.SMEM((RING,) + tile, jnp.float32),
            pltpu.SMEM((RING,) + tile, jnp.int32),
            pltpu.VMEM((3,) + tile, jnp.float32),
            pltpu.VMEM((ones,) + tile, jnp.float32),
            pltpu.VMEM((max(crosses - 1, 1),) + tile, jnp.float32),
            pltpu.VMEM((DEEP - 1,) + tile, jnp.float32),
            dma,
            dma((2, field_count)),
            dma((2,)),
            dma((2, near)),
            dma((2, near)),
            dma((field_count, RING - 1)),
            dma((field_count, RING - 1)),
            dma((2, field_count, RING)),
            dma((2, field_count, RING)),
            dma((field_count, RING - 1)),
            dma((field_count, RING - 1)),
            dma((ones,)),
            dma((ones,)),
            dma((max(crosses - 1, 1),)),
            dma((max(crosses - 1, 1),)),
            dma((DEEP - 1,)),
            dma((DEEP - 1,)),
        ],
        compiler_params=pltpu.CompilerParams(collective_id=0, has_side_effects=True),
        name="exchange",
    )(lat_t, lon_t, departure_row, extents, area, fields)


def row_kernel(lon_t_ref, shift_ref, sums_ref, column_ref, out_ref, doubled, ratio):
    row = pl.program_id(0)
    _, field_count, levels, lon_count = column_ref.shape
    tiles = lon_count // LANES

    @pl.when(row == 0)
    def _():
        for f in range(field_count):
            before = jnp.sum(sums_ref[f:f + 1, :], axis=1, keepdims=True)
            after = jnp.sum(sums_ref[field_count + f:field_count + f + 1, :], axis=1, keepdims=True)
            ratio[f] = jnp.broadcast_to(before / after, ratio.shape[1:])

    lon_w = cubic(lon_t_ref[row])
    lane = lax.broadcasted_iota(jnp.int32, (levels, LANES), 1)
    first = lax.rem(shift_ref[row] - 1 + lon_count, lon_count)
    whole, rest = first // LANES, lax.rem(first, LANES)
    turn = lax.rem(LANES - rest, LANES)
    keep = lane < LANES - rest

    def ahead(pieces, step):
        turned = [pltpu.roll(piece, LANES - step, 1) for piece in pieces]
        return [jnp.where(lane < LANES - step, turned[t], turned[(t + 1) % tiles]) for t in range(tiles)]

    for f in range(field_count):
        lon = [weight * ratio[f] for weight in lon_w]
        column = [column_ref[0, f, :, t * LANES:(t + 1) * LANES] for t in range(tiles)]
        after = ahead(column, 1)
        later = ahead([lon[2] * column[t] + lon[3] * after[t] for t in range(tiles)], 2)
        for t in range(tiles):
            mixed = lon[0] * column[t] + lon[1] * after[t] + later[t]
            doubled[f, :, t * LANES:(t + 1) * LANES] = mixed
            doubled[f, :, lon_count + t * LANES:lon_count + (t + 1) * LANES] = mixed
        turned = []
        for t in range(tiles + 1):
            at = pl.multiple_of((whole + t) * LANES, LANES)
            turned.append(pltpu.roll(doubled[f, :, pl.ds(at, LANES)], turn, 1))
        for t in range(tiles):
            out_ref[0, f, :, t * LANES:(t + 1) * LANES] = jnp.where(keep, turned[t], turned[t + 1])


def rows_of(lon_t, shift, sums, column):
    rows, field_count, levels, lon_count = column.shape
    smem = pl.BlockSpec(memory_space=pltpu.SMEM)
    block = pl.BlockSpec((1, field_count, levels, lon_count), lambda r: (r, 0, 0, 0))
    return pl.pallas_call(
        row_kernel,
        grid=(rows,),
        out_shape=jax.ShapeDtypeStruct(column.shape, column.dtype),
        in_specs=[smem, smem, pl.BlockSpec(memory_space=pltpu.VMEM), block],
        out_specs=block,
        scratch_shapes=[
            pltpu.VMEM((field_count, levels, 2 * lon_count), jnp.float32),
            pltpu.VMEM((field_count, levels, LANES), jnp.float32),
        ],
        compiler_params=pltpu.CompilerParams(dimension_semantics=("arbitrary",)),
        name="rows",
    )(lon_t, shift, sums, column)


def per_device(fields, lat_fraction, lon_fraction, lon_shift, departure_row, extents):
    bands = lax.axis_size("lat")
    total_rows = bands * fields.shape[0]
    row_ids = np.arange(total_rows)
    area = jnp.asarray(np.cos(math.pi * (row_ids + 0.5) / total_rows - math.pi / 2.0), jnp.float32)
    column, sums = exchange(lat_fraction, lon_fraction, departure_row, extents, area, fields)
    return rows_of(lon_fraction, lon_shift, sums, column)


def solution(mesh):
    return jax.shard_map(
        per_device,
        mesh=mesh,
        in_specs=(
            P("lat", None, "lev", None),
            P("lat"),
            P("lat"),
            P("lat"),
            P("lat"),
            P("lat", None),
        ),
        out_specs=P("lat", None, "lev", None),
        check_vma=False,
    )
```

```python
import functools
import math

import jax
import jax.numpy as jnp
import numpy as np
from jax import lax
from jax.experimental import pallas as pl
from jax.experimental.pallas import tpu as pltpu
from jax.sharding import PartitionSpec as P

REACH = 4
LANES = 128
RING = 4
DEEP = 8
MESH = pl.DeviceIdType.MESH
CUTS = ((3, 2), (3, 2), (3, 2))
LEAD = 3
LATE = 4


def chunks_of(field_count, tiles):
    found = []
    for f in range(field_count):
        cuts = CUTS[f] if f < len(CUTS) and sum(CUTS[f]) == tiles else (tiles,)
        first = 0
        for width in cuts:
            found.append((f, first * LANES, width * LANES))
            first += width
    return found


def cubic(t):
    sixth = 1.0 / 6.0
    return (
        -t * (t - 1.0) * (t - 2.0) * sixth,
        (t + 1.0) * (t - 1.0) * (t - 2.0) * 0.5,
        -(t + 1.0) * t * (t - 2.0) * 0.5,
        (t + 1.0) * t * (t - 1.0) * sixth,
    )


def departure_of(row, first_row, rows, total_rows, departure_ref, extents_ref):
    low = first_row - extents_ref[0, 0] * rows + 1
    high = first_row + rows - 3 + extents_ref[0, 1] * rows
    inside = jnp.minimum(jnp.maximum(departure_ref[row], low), high)
    return jnp.minimum(jnp.maximum(inside, 1), total_rows - 3)


def exchange_kernel(bands, levs, lat_t_ref, lon_t_ref, departure_ref, extents_ref, area_ref, fields_ref,
                    out_ref, sums_ref, *scratch):
    rows, field_count, _, lon_count = fields_ref.shape
    piece = lon_count // RING
    chunks = chunks_of(field_count, piece // LANES)
    count = len(chunks)
    held = scratch[0]
    window = scratch[1:1 + count]
    column = scratch[1 + count:1 + 2 * count]
    (real_meta, whole_meta, real_smem, whole_smem, part, met_one, met_two, met_three,
     load_sem, own_sem, smem_sem, meta_send, meta_recv, out_send, out_recv, halo_send, halo_recv,
     back_send, back_recv, one_send, one_recv, two_send, two_recv, three_send, three_recv,
     round_sem) = scratch[1 + 2 * count:]
    band, lev = lax.axis_index("lat"), lax.axis_index("lev")
    group, member = band // RING, lax.rem(band, RING)
    groups = bands // RING
    crosses = groups // DEEP
    deep, cross = lax.rem(group, DEEP), group // DEEP
    first_row, total_rows = band * rows, bands * rows
    span = RING * rows

    def ring_member(step):
        return lax.rem(member + step, RING)

    def ring_peer(step):
        return group * RING + ring_member(step)

    def inside(distance):
        place = band + distance
        return jnp.logical_and(place >= 0, place < bands)

    near = [d for d in range(-REACH, REACH + 1) if d != 0]
    one_peers = [(dy, dl) for dy in range(RING) for dl in range(levs) if (dy, dl) != (0, 0)]

    def one_peer(dy, dl):
        return {"lat": ring_peer(dy), "lev": lax.rem(lev + dl, levs)}

    def two_peer(dx):
        return {"lat": (lax.rem(cross + dx, crosses) * DEEP + deep) * RING + member}

    def three_peer(dz):
        return {"lat": (cross * DEEP + lax.rem(deep + dz, DEEP)) * RING + member}

    barrier = pltpu.get_barrier_semaphore()

    def greet(peer):
        pl.semaphore_signal(barrier, inc=1, device_id=peer, device_id_type=MESH)

    for d in near:
        pl.when(inside(d))(functools.partial(greet, {"lat": band + d}))
    for dy, dl in one_peers:
        if dl:
            greet(one_peer(dy, dl))
    for step in (1, crosses - 1):
        greet(two_peer(step))
    for step in (1, DEEP - 1):
        greet(three_peer(step))

    load = pltpu.make_async_copy(fields_ref, held, load_sem)
    load.start()

    def cut(c, place):
        f, first, width = chunks[c]
        return (slice(None), f, slice(None), pl.ds(pl.multiple_of(place * piece + first, LANES), width))

    own_pieces = [
        pltpu.make_async_copy(
            fields_ref.at[cut(c, member)], window[c].at[pl.ds(span + member * rows, rows)], own_sem.at[0, c]
        )
        for c in range(count)
    ]
    for copy in own_pieces:
        copy.start()

    lane = lax.broadcasted_iota(jnp.int32, (1, LANES), 1)
    lat_t = jnp.zeros((1, LANES), jnp.float32)
    lon_t = jnp.zeros((1, LANES), jnp.float32)
    area = jnp.zeros((1, LANES), jnp.float32)
    start = jnp.zeros((1, LANES), jnp.int32)
    for row in range(rows):
        here = lane == row
        lat_t = jnp.where(here, lat_t_ref[row], lat_t)
        lon_t = jnp.where(here, lon_t_ref[row], lon_t)
        area = jnp.where(here, area_ref[first_row + row], area)
        departure = departure_of(row, first_row, rows, total_rows, departure_ref, extents_ref)
        start = jnp.where(here, departure - 1, start)
    lon_w = cubic(lon_t)
    for d in near:
        @pl.when(jnp.logical_not(inside(d)))
        def _(d=d):
            real_meta[REACH + d] = jnp.zeros(real_meta.shape[1:], jnp.float32)
            whole_meta[REACH + d] = jnp.zeros(whole_meta.shape[1:], jnp.int32)
    real_meta[REACH] = jnp.concatenate(
        [*cubic(lat_t), area * (lon_w[0] + lon_w[1] + lon_w[2] + lon_w[3]), jnp.zeros((3, LANES), jnp.float32)], axis=0
    )
    whole_meta[REACH] = jnp.broadcast_to(start, whole_meta.shape[1:])

    expected = sum(dl != 0 for _, dl in one_peers) + 4
    for d in near:
        expected = expected + inside(d).astype(jnp.int32)
    pl.semaphore_wait(barrier, expected)

    def tell(n):
        for step in (1, DEEP - 1):
            pl.semaphore_signal(round_sem.at[n], inc=1, device_id=three_peer(step), device_id_type=MESH)
        if n == 0:
            for step in (1, crosses - 1):
                pl.semaphore_signal(round_sem.at[n], inc=1, device_id=two_peer(step), device_id_type=MESH)

    def hear(n):
        pl.semaphore_wait(round_sem.at[n], 4 if n == 0 else 2)

    tell(0)

    def meta_copies(d):
        k = near.index(d)
        return [
            pltpu.make_async_remote_copy(
                src_ref=ref.at[REACH], dst_ref=ref.at[REACH - d],
                send_sem=meta_send.at[n, k], recv_sem=meta_recv.at[n, near.index(-d)],
                device_id={"lat": band + d}, device_id_type=MESH,
            )
            for n, ref in enumerate((real_meta, whole_meta))
        ]

    def meta_arrivals(d):
        k = near.index(d)
        return [
            pltpu.make_async_remote_copy(
                src_ref=ref.at[REACH + d], dst_ref=ref.at[REACH + d],
                send_sem=meta_send.at[n, k], recv_sem=meta_recv.at[n, k],
                device_id={"lat": band + d}, device_id_type=MESH,
            )
            for n, ref in enumerate((real_meta, whole_meta))
        ]

    for d in near:
        @pl.when(inside(d))
        def _(d=d):
            for copy in meta_copies(d):
                copy.start()

    def out_copy(c, dy):
        return pltpu.make_async_remote_copy(
            src_ref=fields_ref.at[cut(c, ring_member(dy))],
            dst_ref=window[c].at[pl.ds(span + member * rows, rows)],
            send_sem=out_send.at[c, dy - 1], recv_sem=out_recv.at[c, dy - 1],
            device_id={"lat": ring_peer(dy)}, device_id_type=MESH,
        )

    def out_arrival(c, dy):
        place = window[c].at[pl.ds(span + ring_member(RING - dy) * rows, rows)]
        return pltpu.make_async_remote_copy(
            src_ref=place, dst_ref=place, send_sem=out_send.at[c, dy - 1], recv_sem=out_recv.at[c, dy - 1],
            device_id={"lat": ring_peer(RING - dy)}, device_id_type=MESH,
        )

    has_side = (group < groups - 1, group > 0)

    def halo_place(c, dy, side):
        return window[c].at[pl.ds((0 if side == 0 else 2 * span) + ring_member(RING - dy) * rows, rows)]

    def halo_copy(c, dy, side):
        if dy == 0:
            source = fields_ref.at[cut(c, member)]
        else:
            source = window[c].at[pl.ds(span + ring_member(RING - dy) * rows, rows)]
        return pltpu.make_async_remote_copy(
            src_ref=source, dst_ref=halo_place(c, dy, side),
            send_sem=halo_send.at[side, c, dy], recv_sem=halo_recv.at[side, c, dy],
            device_id={"lat": band + (RING if side == 0 else -RING)}, device_id_type=MESH,
        )

    def halo_arrival(c, dy, side):
        place = halo_place(c, dy, side)
        return pltpu.make_async_remote_copy(
            src_ref=place, dst_ref=place, send_sem=halo_send.at[side, c, dy], recv_sem=halo_recv.at[side, c, dy],
            device_id={"lat": band + (-RING if side == 0 else RING)}, device_id_type=MESH,
        )

    def start_halo(c, dy):
        for side in range(2):
            pl.when(has_side[side])(lambda side=side: halo_copy(c, dy, side).start())

    def back_copy(c, dy):
        return pltpu.make_async_remote_copy(
            src_ref=column[c].at[pl.ds(dy * rows, rows)],
            dst_ref=out_ref.at[cut(c, member)],
            send_sem=back_send.at[c, dy - 1], recv_sem=back_recv.at[c, dy - 1],
            device_id={"lat": ring_peer(dy)}, device_id_type=MESH,
        )

    def back_arrival(c, dy):
        place = out_ref.at[cut(c, ring_member(RING - dy))]
        return pltpu.make_async_remote_copy(
            src_ref=place, dst_ref=place, send_sem=back_send.at[c, dy - 1], recv_sem=back_recv.at[c, dy - 1],
            device_id={"lat": ring_peer(RING - dy)}, device_id_type=MESH,
        )

    def back_own(c):
        return pltpu.make_async_copy(column[c].at[pl.ds(0, rows)], out_ref.at[cut(c, member)], own_sem.at[1, c])

    def small_copy(source, target, sends, arrivals, k, peer):
        return pltpu.make_async_remote_copy(
            src_ref=source, dst_ref=target.at[k], send_sem=sends.at[k], recv_sem=arrivals.at[k],
            device_id=peer, device_id_type=MESH,
        )

    ones = [small_copy(part.at[0], met_one, one_send, one_recv, k, one_peer(*p)) for k, p in enumerate(one_peers)]
    twos = [small_copy(part.at[1], met_two, two_send, two_recv, dx - 1, two_peer(dx)) for dx in range(1, crosses)]
    threes = [small_copy(part.at[2], met_three, three_send, three_recv, dz - 1, three_peer(dz)) for dz in range(1, DEEP)]

    order = (1, RING - 1, *range(2, RING - 1))
    slots = [(c, 0) for c in range(min(LEAD, count))]
    for c in range(count):
        slots += [(c, dy) for dy in order] + [(c + LEAD, 0)] * (c + LEAD < count)
    place_of = {slot: k for k, slot in enumerate(slots)}
    start_halo(*slots[0])
    for c in range(min(2, count)):
        for dy in order:
            out_copy(c, dy).start()
    for slot in slots[1:LEAD]:
        start_halo(*slot)

    for d in near:
        @pl.when(inside(d))
        def _(d=d):
            for copy in meta_arrivals(d):
                copy.wait_recv()
    group_slots = pl.ds(REACH - member, RING)
    to_smem = [
        pltpu.make_async_copy(real_meta.at[group_slots], real_smem, smem_sem.at[0]),
        pltpu.make_async_copy(whole_meta.at[group_slots], whole_smem, smem_sem.at[1]),
    ]
    for copy in to_smem:
        copy.start()
    load.wait()

    def add_row(row, totals):
        taken = jnp.zeros((2 * REACH + 1, LANES), jnp.float32)
        for a in range(4):
            hit = whole_meta[:, 0, :] + a == first_row + row
            taken = taken + jnp.where(hit, real_meta[:, a, :] * real_meta[:, 4, :], 0.0)
        taken = jnp.sum(jnp.sum(taken, axis=0, keepdims=True), axis=1, keepdims=True)
        row_area = area_ref[first_row + row]
        before, after = [], []
        for f in range(field_count):
            tile = held[row, f, :, 0:LANES]
            for t in range(1, lon_count // LANES):
                tile = tile + held[row, f, :, t * LANES:(t + 1) * LANES]
            total = jnp.sum(tile, axis=0, keepdims=True)
            before.append(totals[f] + row_area * total)
            after.append(totals[field_count + f] + taken * total)
        return tuple(before + after)

    zero = jnp.zeros((1, LANES), jnp.float32)
    totals = lax.fori_loop(0, rows, add_row, (zero,) * (2 * field_count))
    part[0] = jnp.concatenate([*totals, jnp.zeros((8 - 2 * field_count, LANES), jnp.float32)], axis=0)

    def gather_small(copies, target, level):
        for copy in copies:
            copy.wait_recv()
        total = part[level]
        for k in range(len(copies)):
            total = total + target[k]
        return total

    for copy in ones:
        copy.start()
    for c in range(min(2, count), count):
        for dy in order:
            out_copy(c, dy).start()

    base = (group - 1) * span

    def interpolate(c, dy):
        to = ring_member(dy)

        def one_row(row, carry):
            place = whole_smem[to, 0, row] - base
            weight = [real_smem[to, a, row] for a in range(4)]
            for t in range(chunks[c][2] // LANES):
                at = pl.ds(t * LANES, LANES)
                total = weight[0] * window[c][place, :, at]
                for a in range(1, 4):
                    total = total + weight[a] * window[c][place + a, :, at]
                column[c][dy * rows + row, :, at] = total
            return carry

        lax.fori_loop(0, rows, one_row, 0)

    def finish_chunk(c):
        if c == 0:
            for copy in to_smem:
                copy.wait()
        own_pieces[c].wait()
        for dy in (0, *order):
            for side in range(2):
                pl.when(has_side[1 - side])(lambda dy=dy, side=side: halo_arrival(c, dy, side).wait_recv())
        for dy in (2, 1, RING - 1, 0):
            interpolate(c, dy)
        for dy in (2, 1, RING - 1):
            back_copy(c, dy).start()
        back_own(c).start()

    def one_done():
        part[1] = gather_small(ones, met_one, 0)
        for copy in twos:
            copy.start()

    def two_done():
        part[2] = gather_small(twos, met_two, 1)
        hear(2)
        for copy in threes:
            copy.start()

    def pass_on(n):
        hear(n)
        tell(n + 1)

    tasks = {k: [] for k in range(len(slots) + LATE)}
    tasks[4].append(functools.partial(pass_on, 0))
    tasks[6].append(one_done)
    tasks[7].append(functools.partial(pass_on, 1))
    tasks[9].append(two_done)
    for c in range(count):
        tasks[place_of[c, order[-1]] + LATE].append(functools.partial(finish_chunk, c))
    for k in range(LEAD, len(slots) + LATE):
        if k < len(slots):
            c, dy = slots[k]
            if dy:
                out_arrival(c, dy).wait_recv()
            for side in range(2):
                pl.when(has_side[side])(lambda k=k, side=side: halo_copy(*slots[k - LEAD], side).wait_send())
            start_halo(c, dy)
        for task in tasks[k]:
            task()

    sums_ref[...] = gather_small(threes, met_three, 2)

    for c in range(count):
        for dy in order:
            back_arrival(c, dy).wait_recv()
    for d in near:
        @pl.when(inside(d))
        def _(d=d):
            for copy in meta_copies(d):
                copy.wait_send()
    for copy in ones + twos + threes:
        copy.wait_send()
    for c in range(count):
        back_own(c).wait()
        for dy in order:
            out_copy(c, dy).wait_send()
            back_copy(c, dy).wait_send()
    for slot in slots[-LEAD:]:
        for side in range(2):
            pl.when(has_side[side])(lambda slot=slot, side=side: halo_copy(*slot, side).wait_send())


def exchange(lat_t, lon_t, departure_row, extents, area, fields):
    bands, levs = lax.axis_size("lat"), lax.axis_size("lev")
    rows, field_count, levels, lon_count = fields.shape
    crosses = bands // RING // DEEP
    piece = lon_count // RING
    tile = (8, LANES)
    dma = pltpu.SemaphoreType.DMA
    ones = RING * levs - 1
    near = 2 * REACH
    chunks = chunks_of(field_count, piece // LANES)
    count = len(chunks)
    return pl.pallas_call(
        functools.partial(exchange_kernel, bands, levs),
        out_shape=(
            pltpu.VMEM(fields.shape, fields.dtype),
            pltpu.VMEM(tile, jnp.float32),
        ),
        in_specs=[pl.BlockSpec(memory_space=pltpu.SMEM)] * 5 + [pl.BlockSpec(memory_space=pl.ANY)],
        out_specs=(pl.BlockSpec(memory_space=pltpu.VMEM), pl.BlockSpec(memory_space=pltpu.VMEM)),
        scratch_shapes=[
            pltpu.VMEM(fields.shape, jnp.float32),
            *[pltpu.VMEM((3 * RING * rows, levels, width), jnp.float32) for _, _, width in chunks],
            *[pltpu.VMEM((RING * rows, levels, width), jnp.float32) for _, _, width in chunks],
            pltpu.VMEM((near + 1,) + tile, jnp.float32),
            pltpu.VMEM((near + 1,) + tile, jnp.int32),
            pltpu.SMEM((RING,) + tile, jnp.float32),
            pltpu.SMEM((RING,) + tile, jnp.int32),
            pltpu.VMEM((3,) + tile, jnp.float32),
            pltpu.VMEM((ones,) + tile, jnp.float32),
            pltpu.VMEM((max(crosses - 1, 1),) + tile, jnp.float32),
            pltpu.VMEM((DEEP - 1,) + tile, jnp.float32),
            dma,
            dma((2, count)),
            dma((2,)),
            dma((2, near)),
            dma((2, near)),
            dma((count, RING - 1)),
            dma((count, RING - 1)),
            dma((2, count, RING)),
            dma((2, count, RING)),
            dma((count, RING - 1)),
            dma((count, RING - 1)),
            dma((ones,)),
            dma((ones,)),
            dma((max(crosses - 1, 1),)),
            dma((max(crosses - 1, 1),)),
            dma((DEEP - 1,)),
            dma((DEEP - 1,)),
            pltpu.SemaphoreType.REGULAR((3,)),
        ],
        compiler_params=pltpu.CompilerParams(
            collective_id=0, has_side_effects=True, vmem_limit_bytes=60000 * 1024
        ),
        name="exchange",
    )(lat_t, lon_t, departure_row, extents, area, fields)


def row_kernel(lon_t_ref, shift_ref, sums_ref, column_ref, out_ref, doubled, held, sem):
    rows, field_count, levels, lon_count = column_ref.shape
    tiles = lon_count // LANES
    lane = lax.broadcasted_iota(jnp.int32, (levels, LANES), 1)
    ratio = []
    for f in range(field_count):
        before = jnp.sum(sums_ref[f:f + 1, :], axis=1, keepdims=True)
        after = jnp.sum(sums_ref[field_count + f:field_count + f + 1, :], axis=1, keepdims=True)
        ratio.append(before / after)

    def ahead(pieces, step):
        turned = [pltpu.roll(piece, LANES - step, 1) for piece in pieces]
        return [jnp.where(lane < LANES - step, turned[t], turned[(t + 1) % tiles]) for t in range(tiles)]

    def row_copy(row):
        return pltpu.make_async_copy(held.at[row], out_ref.at[row], sem.at[row])

    def one_row(row, carry):
        lon_w = cubic(lon_t_ref[row])
        first = lax.rem(shift_ref[row] - 1 + lon_count, lon_count)
        whole, rest = first // LANES, lax.rem(first, LANES)
        turn = lax.rem(LANES - rest, LANES)
        keep = lane < LANES - rest
        for f in range(field_count):
            lon = [weight * ratio[f] for weight in lon_w]
            column = [column_ref[row, f, :, t * LANES:(t + 1) * LANES] for t in range(tiles)]
            after = ahead(column, 1)
            later = ahead([lon[2] * column[t] + lon[3] * after[t] for t in range(tiles)], 2)
            for t in range(tiles):
                mixed = lon[0] * column[t] + lon[1] * after[t] + later[t]
                doubled[f, :, t * LANES:(t + 1) * LANES] = mixed
                doubled[f, :, lon_count + t * LANES:lon_count + (t + 1) * LANES] = mixed
        for f in range(field_count):
            turned = []
            for t in range(tiles + 1):
                at = pl.multiple_of((whole + t) * LANES, LANES)
                turned.append(pltpu.roll(doubled[f, :, pl.ds(at, LANES)], turn, 1))
            for t in range(tiles):
                held[row, f, :, t * LANES:(t + 1) * LANES] = jnp.where(keep, turned[t], turned[t + 1])
        row_copy(row).start()
        return carry

    lax.fori_loop(0, rows, one_row, 0)
    for row in range(rows):
        row_copy(row).wait()


def rows_of(lon_t, shift, sums, column):
    rows, field_count, levels, lon_count = column.shape
    smem = pl.BlockSpec(memory_space=pltpu.SMEM)
    vmem = pl.BlockSpec(memory_space=pltpu.VMEM)
    return pl.pallas_call(
        row_kernel,
        out_shape=jax.ShapeDtypeStruct(column.shape, column.dtype),
        in_specs=[smem, smem, vmem, vmem],
        out_specs=pl.BlockSpec(memory_space=pl.ANY),
        scratch_shapes=[
            pltpu.VMEM((field_count, levels, 2 * lon_count), jnp.float32),
            pltpu.VMEM(column.shape, jnp.float32),
            pltpu.SemaphoreType.DMA((rows,)),
        ],
        compiler_params=pltpu.CompilerParams(vmem_limit_bytes=16 * 1024 * 1024),
        name="rows",
    )(lon_t, shift, sums, column)


def per_device(fields, lat_fraction, lon_fraction, lon_shift, departure_row, extents):
    bands = lax.axis_size("lat")
    total_rows = bands * fields.shape[0]
    row_ids = np.arange(total_rows)
    area = jnp.asarray(np.cos(math.pi * (row_ids + 0.5) / total_rows - math.pi / 2.0), jnp.float32)
    column, sums = exchange(lat_fraction, lon_fraction, departure_row, extents, area, fields)
    return rows_of(lon_fraction, lon_shift, sums, column)


def solution(mesh):
    return jax.shard_map(
        per_device,
        mesh=mesh,
        in_specs=(
            P("lat", None, "lev", None),
            P("lat"),
            P("lat"),
            P("lat"),
            P("lat"),
            P("lat", None),
        ),
        out_specs=P("lat", None, "lev", None),
        check_vma=False,
    )
```

```python
import functools
import math

import jax
import jax.numpy as jnp
import numpy as np
from jax import lax
from jax.experimental import pallas as pl
from jax.experimental.pallas import tpu as pltpu
from jax.sharding import PartitionSpec as P

REACH = 4
LANES = 128
RING = 4
DEEP = 8
MESH = pl.DeviceIdType.MESH
CUTS = ((3, 2), (3, 2), (3, 2))
LEAD = 3
LATE = 3
TOGETHER = 2
AT_ONCE = 2


def chunks_of(field_count, tiles):
    found = []
    for f in range(field_count):
        cuts = CUTS[f] if f < len(CUTS) and sum(CUTS[f]) == tiles else (tiles,)
        first = 0
        for width in cuts:
            found.append((f, first * LANES, width * LANES))
            first += width
    return found


def cubic(t):
    sixth = 1.0 / 6.0
    return (
        -t * (t - 1.0) * (t - 2.0) * sixth,
        (t + 1.0) * (t - 1.0) * (t - 2.0) * 0.5,
        -(t + 1.0) * t * (t - 2.0) * 0.5,
        (t + 1.0) * t * (t - 1.0) * sixth,
    )


def departure_of(row, first_row, rows, total_rows, departure_ref, extents_ref):
    low = first_row - extents_ref[0, 0] * rows + 1
    high = first_row + rows - 3 + extents_ref[0, 1] * rows
    inside = jnp.minimum(jnp.maximum(departure_ref[row], low), high)
    return jnp.minimum(jnp.maximum(inside, 1), total_rows - 3)


def exchange_kernel(bands, levs, lat_t_ref, lon_t_ref, departure_ref, extents_ref, area_ref, fields_ref,
                    out_ref, *scratch):
    rows, field_count, _, lon_count = fields_ref.shape
    piece = lon_count // RING
    chunks = chunks_of(field_count, piece // LANES)
    count = len(chunks)
    held, landed = scratch[:2]
    window = scratch[2:2 + count]
    column = scratch[2 + count:2 + 2 * count]
    (real_meta, whole_meta, real_smem, whole_smem, part, met_one, met_two, met_three,
     load_sem, own_sem, smem_sem, meta_send, meta_recv, out_send, out_recv, halo_send, halo_recv,
     back_send, back_recv, one_send, one_recv, two_send, two_recv, three_send, three_recv,
     round_sem) = scratch[2 + 2 * count:]
    band, lev = lax.axis_index("lat"), lax.axis_index("lev")
    group, member = band // RING, lax.rem(band, RING)
    groups = bands // RING
    crosses = groups // DEEP
    deep, cross = lax.rem(group, DEEP), group // DEEP
    first_row, total_rows = band * rows, bands * rows
    span = RING * rows

    def ring_member(step):
        return lax.rem(member + step, RING)

    def ring_peer(step):
        return group * RING + ring_member(step)

    def inside(distance):
        place = band + distance
        return jnp.logical_and(place >= 0, place < bands)

    near = [d for d in range(-REACH, REACH + 1) if d != 0]
    one_peers = [(dy, dl) for dy in range(RING) for dl in range(levs) if (dy, dl) != (0, 0)]

    def one_peer(dy, dl):
        return {"lat": ring_peer(dy), "lev": lax.rem(lev + dl, levs)}

    def two_peer(dx):
        return {"lat": (lax.rem(cross + dx, crosses) * DEEP + deep) * RING + member}

    def three_peer(dz):
        return {"lat": (cross * DEEP + lax.rem(deep + dz, DEEP)) * RING + member}

    barrier = pltpu.get_barrier_semaphore()

    def greet(peer):
        pl.semaphore_signal(barrier, inc=1, device_id=peer, device_id_type=MESH)

    for d in near:
        pl.when(inside(d))(functools.partial(greet, {"lat": band + d}))
    for dy, dl in one_peers:
        if dl:
            greet(one_peer(dy, dl))
    for step in (1, crosses - 1):
        greet(two_peer(step))
    for step in (1, DEEP - 1):
        greet(three_peer(step))

    load = pltpu.make_async_copy(fields_ref, held, load_sem)
    load.start()

    def cut(c, place):
        f, first, width = chunks[c]
        return (slice(None), f, slice(None), pl.ds(pl.multiple_of(place * piece + first, LANES), width))

    own_pieces = [
        pltpu.make_async_copy(
            fields_ref.at[cut(c, member)], window[c].at[pl.ds(span + member * rows, rows)], own_sem.at[0, c]
        )
        for c in range(count)
    ]
    for copy in own_pieces:
        copy.start()

    lane = lax.broadcasted_iota(jnp.int32, (1, LANES), 1)
    lat_t = jnp.zeros((1, LANES), jnp.float32)
    lon_t = jnp.zeros((1, LANES), jnp.float32)
    area = jnp.zeros((1, LANES), jnp.float32)
    start = jnp.zeros((1, LANES), jnp.int32)
    for row in range(rows):
        here = lane == row
        lat_t = jnp.where(here, lat_t_ref[row], lat_t)
        lon_t = jnp.where(here, lon_t_ref[row], lon_t)
        area = jnp.where(here, area_ref[first_row + row], area)
        departure = departure_of(row, first_row, rows, total_rows, departure_ref, extents_ref)
        start = jnp.where(here, departure - 1, start)
    lon_w = cubic(lon_t)
    for d in near:
        @pl.when(jnp.logical_not(inside(d)))
        def _(d=d):
            real_meta[REACH + d] = jnp.zeros(real_meta.shape[1:], jnp.float32)
            whole_meta[REACH + d] = jnp.zeros(whole_meta.shape[1:], jnp.int32)
    real_meta[REACH] = jnp.concatenate(
        [*cubic(lat_t), area * (lon_w[0] + lon_w[1] + lon_w[2] + lon_w[3]), jnp.zeros((3, LANES), jnp.float32)], axis=0
    )
    whole_meta[REACH] = jnp.broadcast_to(start, whole_meta.shape[1:])

    expected = sum(dl != 0 for _, dl in one_peers) + 4
    for d in near:
        expected = expected + inside(d).astype(jnp.int32)
    pl.semaphore_wait(barrier, expected)

    def tell(n):
        for step in (1, DEEP - 1):
            pl.semaphore_signal(round_sem.at[n], inc=1, device_id=three_peer(step), device_id_type=MESH)
        if n == 0:
            for step in (1, crosses - 1):
                pl.semaphore_signal(round_sem.at[n], inc=1, device_id=two_peer(step), device_id_type=MESH)

    def hear(n):
        pl.semaphore_wait(round_sem.at[n], 4 if n == 0 else 2)

    tell(0)

    def meta_copies(d):
        k = near.index(d)
        return [
            pltpu.make_async_remote_copy(
                src_ref=ref.at[REACH], dst_ref=ref.at[REACH - d],
                send_sem=meta_send.at[n, k], recv_sem=meta_recv.at[n, near.index(-d)],
                device_id={"lat": band + d}, device_id_type=MESH,
            )
            for n, ref in enumerate((real_meta, whole_meta))
        ]

    def meta_arrivals(d):
        k = near.index(d)
        return [
            pltpu.make_async_remote_copy(
                src_ref=ref.at[REACH + d], dst_ref=ref.at[REACH + d],
                send_sem=meta_send.at[n, k], recv_sem=meta_recv.at[n, k],
                device_id={"lat": band + d}, device_id_type=MESH,
            )
            for n, ref in enumerate((real_meta, whole_meta))
        ]

    for d in near:
        @pl.when(inside(d))
        def _(d=d):
            for copy in meta_copies(d):
                copy.start()

    def out_copy(c, dy):
        return pltpu.make_async_remote_copy(
            src_ref=fields_ref.at[cut(c, ring_member(dy))],
            dst_ref=window[c].at[pl.ds(span + member * rows, rows)],
            send_sem=out_send.at[c, dy - 1], recv_sem=out_recv.at[c, dy - 1],
            device_id={"lat": ring_peer(dy)}, device_id_type=MESH,
        )

    def out_arrival(c, dy):
        place = window[c].at[pl.ds(span + ring_member(RING - dy) * rows, rows)]
        return pltpu.make_async_remote_copy(
            src_ref=place, dst_ref=place, send_sem=out_send.at[c, dy - 1], recv_sem=out_recv.at[c, dy - 1],
            device_id={"lat": ring_peer(RING - dy)}, device_id_type=MESH,
        )

    has_side = (group < groups - 1, group > 0)

    def halo_place(c, dy, side):
        return window[c].at[pl.ds((0 if side == 0 else 2 * span) + ring_member(RING - dy) * rows, rows)]

    def halo_copy(c, dy, side):
        if dy == 0:
            source = fields_ref.at[cut(c, member)]
        else:
            source = window[c].at[pl.ds(span + ring_member(RING - dy) * rows, rows)]
        return pltpu.make_async_remote_copy(
            src_ref=source, dst_ref=halo_place(c, dy, side),
            send_sem=halo_send.at[side, c, dy], recv_sem=halo_recv.at[side, c, dy],
            device_id={"lat": band + (RING if side == 0 else -RING)}, device_id_type=MESH,
        )

    def halo_arrival(c, dy, side):
        place = halo_place(c, dy, side)
        return pltpu.make_async_remote_copy(
            src_ref=place, dst_ref=place, send_sem=halo_send.at[side, c, dy], recv_sem=halo_recv.at[side, c, dy],
            device_id={"lat": band + (-RING if side == 0 else RING)}, device_id_type=MESH,
        )

    def start_halo(c, dy):
        for side in range(2):
            pl.when(has_side[side])(lambda side=side: halo_copy(c, dy, side).start())

    def back_copy(c, dy):
        return pltpu.make_async_remote_copy(
            src_ref=column[c].at[pl.ds(dy * rows, rows)],
            dst_ref=landed.at[cut(c, member)],
            send_sem=back_send.at[c, dy - 1], recv_sem=back_recv.at[c, dy - 1],
            device_id={"lat": ring_peer(dy)}, device_id_type=MESH,
        )

    def back_arrival(c, dy):
        place = landed.at[cut(c, ring_member(RING - dy))]
        return pltpu.make_async_remote_copy(
            src_ref=place, dst_ref=place, send_sem=back_send.at[c, dy - 1], recv_sem=back_recv.at[c, dy - 1],
            device_id={"lat": ring_peer(RING - dy)}, device_id_type=MESH,
        )

    def back_own(c):
        return pltpu.make_async_copy(column[c].at[pl.ds(0, rows)], landed.at[cut(c, member)], own_sem.at[1, c])

    def small_copy(source, target, sends, arrivals, k, peer):
        return pltpu.make_async_remote_copy(
            src_ref=source, dst_ref=target.at[k], send_sem=sends.at[k], recv_sem=arrivals.at[k],
            device_id=peer, device_id_type=MESH,
        )

    ones = [small_copy(part.at[0], met_one, one_send, one_recv, k, one_peer(*p)) for k, p in enumerate(one_peers)]
    twos = [small_copy(part.at[1], met_two, two_send, two_recv, dx - 1, two_peer(dx)) for dx in range(1, crosses)]
    threes = [small_copy(part.at[2], met_three, three_send, three_recv, dz - 1, three_peer(dz)) for dz in range(1, DEEP)]

    order = (1, RING - 1, *range(2, RING - 1))
    slots = [(c, 0) for c in range(min(LEAD, count))]
    for c in range(count):
        slots += [(c, dy) for dy in order] + [(c + LEAD, 0)] * (c + LEAD < count)
    place_of = {slot: k for k, slot in enumerate(slots)}
    start_halo(*slots[0])
    for c in range(min(2, count)):
        for dy in order:
            out_copy(c, dy).start()
    for slot in slots[1:LEAD]:
        start_halo(*slot)

    for d in near:
        @pl.when(inside(d))
        def _(d=d):
            for copy in meta_arrivals(d):
                copy.wait_recv()
    group_slots = pl.ds(REACH - member, RING)
    to_smem = [
        pltpu.make_async_copy(real_meta.at[group_slots], real_smem, smem_sem.at[0]),
        pltpu.make_async_copy(whole_meta.at[group_slots], whole_smem, smem_sem.at[1]),
    ]
    for copy in to_smem:
        copy.start()
    load.wait()

    def add_row(row, totals):
        taken = jnp.zeros((2 * REACH + 1, LANES), jnp.float32)
        for a in range(4):
            hit = whole_meta[:, 0, :] + a == first_row + row
            taken = taken + jnp.where(hit, real_meta[:, a, :] * real_meta[:, 4, :], 0.0)
        taken = jnp.sum(jnp.sum(taken, axis=0, keepdims=True), axis=1, keepdims=True)
        row_area = area_ref[first_row + row]
        before, after = [], []
        for f in range(field_count):
            tile = held[row, f, :, 0:LANES]
            for t in range(1, lon_count // LANES):
                tile = tile + held[row, f, :, t * LANES:(t + 1) * LANES]
            total = jnp.sum(tile, axis=0, keepdims=True)
            before.append(totals[f] + row_area * total)
            after.append(totals[field_count + f] + taken * total)
        return tuple(before + after)

    zero = jnp.zeros((1, LANES), jnp.float32)
    totals = lax.fori_loop(0, rows, add_row, (zero,) * (2 * field_count))
    part[0] = jnp.concatenate([*totals, jnp.zeros((8 - 2 * field_count, LANES), jnp.float32)], axis=0)

    def gather_small(copies, target, level):
        for copy in copies:
            copy.wait_recv()
        total = part[level]
        for k in range(len(copies)):
            total = total + target[k]
        return total

    for copy in ones:
        copy.start()
    for c in range(min(2, count), count):
        for dy in order:
            out_copy(c, dy).start()

    base = (group - 1) * span

    def interpolate(c, dy):
        to = ring_member(dy)

        def one_row(row, carry):
            place = whole_smem[to, 0, row] - base
            weight = [real_smem[to, a, row] for a in range(4)]
            for t in range(chunks[c][2] // LANES):
                at = pl.ds(t * LANES, LANES)
                total = weight[0] * window[c][place, :, at]
                for a in range(1, 4):
                    total = total + weight[a] * window[c][place + a, :, at]
                column[c][dy * rows + row, :, at] = total
            return carry

        lax.fori_loop(0, rows, one_row, 0)

    def finish_chunk(c):
        if c == 0:
            for copy in to_smem:
                copy.wait()
        own_pieces[c].wait()
        for dy in (0, *order):
            for side in range(2):
                pl.when(has_side[1 - side])(lambda dy=dy, side=side: halo_arrival(c, dy, side).wait_recv())
        for dy in (2, 1, RING - 1, 0):
            interpolate(c, dy)
        for dy in (2, 1, RING - 1):
            back_copy(c, dy).start()
        back_own(c).start()

    def one_done():
        part[1] = gather_small(ones, met_one, 0)
        for copy in twos:
            copy.start()

    def two_done():
        part[2] = gather_small(twos, met_two, 1)
        hear(2)
        for copy in threes:
            copy.start()

    def pass_on(n):
        hear(n)
        tell(n + 1)

    lanes = lax.broadcasted_iota(jnp.int32, fields_ref.shape[2:3] + (LANES,), 1)
    tiles = lon_count // LANES

    def shifted(pieces, step):
        turned = [pltpu.roll(piece, LANES - step, 1) for piece in pieces]
        return [jnp.where(lanes < LANES - step, turned[t], turned[(t + 1) % tiles]) for t in range(tiles)]

    def along(f, sums):
        for c in range(count):
            if chunks[c][0] == f:
                back_own(c).wait()
                for dy in order:
                    back_arrival(c, dy).wait_recv()
        before = jnp.sum(sums[f:f + 1], axis=1, keepdims=True)
        after = jnp.sum(sums[field_count + f:field_count + f + 1], axis=1, keepdims=True)
        ratio = before / after

        def some_rows(step, carry):
            for n in range(TOGETHER):
                row = step * TOGETHER + n
                lon = [weight * ratio for weight in cubic(lon_t_ref[row])]
                here = [landed[row, f, :, t * LANES:(t + 1) * LANES] for t in range(tiles)]
                after = shifted(here, 1)
                later = shifted([lon[2] * here[t] + lon[3] * after[t] for t in range(tiles)], 2)
                for t in range(tiles):
                    mixed = lon[0] * here[t] + lon[1] * after[t] + later[t]
                    out_ref[row, f, :, t * LANES:(t + 1) * LANES] = mixed
            return carry

        lax.fori_loop(0, rows // TOGETHER, some_rows, 0)

    sums = []
    tasks = {k: [] for k in range(len(slots) + LATE)}
    tasks[4].append(functools.partial(pass_on, 0))
    tasks[6].append(one_done)
    tasks[7].append(functools.partial(pass_on, 1))
    tasks[9].append(two_done)
    for c in range(count):
        tasks[place_of[c, order[-1]] + LATE].append(functools.partial(finish_chunk, c))
    tasks[place_of[count - 3, order[-1]] + LATE].append(
        lambda: sums.append(gather_small(threes, met_three, 2))
    )
    for f in range(field_count - 1):
        near_end = count - field_count + 1 + f
        tasks[place_of[near_end - 1, order[-1]] + LATE].append(functools.partial(lambda f: along(f, sums[0]), f))
    for k in range(LEAD, len(slots) + LATE):
        if k < len(slots):
            c, dy = slots[k]
            if dy:
                out_arrival(c, dy).wait_recv()
            for side in range(2):
                pl.when(has_side[side])(lambda k=k, side=side: halo_copy(*slots[k - LEAD], side).wait_send())
            start_halo(c, dy)
        for task in tasks[k]:
            task()

    along(field_count - 1, sums[0])
    for d in near:
        @pl.when(inside(d))
        def _(d=d):
            for copy in meta_copies(d):
                copy.wait_send()
    for copy in ones + twos + threes:
        copy.wait_send()
    for c in range(count):
        for dy in order:
            out_copy(c, dy).wait_send()
            back_copy(c, dy).wait_send()
    for slot in slots[-LEAD:]:
        for side in range(2):
            pl.when(has_side[side])(lambda slot=slot, side=side: halo_copy(*slot, side).wait_send())


def exchange(lat_t, lon_t, departure_row, extents, area, fields):
    bands, levs = lax.axis_size("lat"), lax.axis_size("lev")
    rows, field_count, levels, lon_count = fields.shape
    crosses = bands // RING // DEEP
    piece = lon_count // RING
    tile = (8, LANES)
    dma = pltpu.SemaphoreType.DMA
    ones = RING * levs - 1
    near = 2 * REACH
    chunks = chunks_of(field_count, piece // LANES)
    count = len(chunks)
    return pl.pallas_call(
        functools.partial(exchange_kernel, bands, levs),
        out_shape=pltpu.VMEM(fields.shape, fields.dtype),
        in_specs=[pl.BlockSpec(memory_space=pltpu.SMEM)] * 5 + [pl.BlockSpec(memory_space=pl.ANY)],
        out_specs=pl.BlockSpec(memory_space=pltpu.VMEM),
        scratch_shapes=[
            pltpu.VMEM(fields.shape, jnp.float32),
            pltpu.VMEM(fields.shape, jnp.float32),
            *[pltpu.VMEM((3 * RING * rows, levels, width), jnp.float32) for _, _, width in chunks],
            *[pltpu.VMEM((RING * rows, levels, width), jnp.float32) for _, _, width in chunks],
            pltpu.VMEM((near + 1,) + tile, jnp.float32),
            pltpu.VMEM((near + 1,) + tile, jnp.int32),
            pltpu.SMEM((RING,) + tile, jnp.float32),
            pltpu.SMEM((RING,) + tile, jnp.int32),
            pltpu.VMEM((3,) + tile, jnp.float32),
            pltpu.VMEM((ones,) + tile, jnp.float32),
            pltpu.VMEM((max(crosses - 1, 1),) + tile, jnp.float32),
            pltpu.VMEM((DEEP - 1,) + tile, jnp.float32),
            dma,
            dma((2, count)),
            dma((2,)),
            dma((2, near)),
            dma((2, near)),
            dma((count, RING - 1)),
            dma((count, RING - 1)),
            dma((2, count, RING)),
            dma((2, count, RING)),
            dma((count, RING - 1)),
            dma((count, RING - 1)),
            dma((ones,)),
            dma((ones,)),
            dma((max(crosses - 1, 1),)),
            dma((max(crosses - 1, 1),)),
            dma((DEEP - 1,)),
            dma((DEEP - 1,)),
            pltpu.SemaphoreType.REGULAR((3,)),
        ],
        compiler_params=pltpu.CompilerParams(
            collective_id=0, has_side_effects=True, vmem_limit_bytes=60000 * 1024
        ),
        name="exchange",
    )(lat_t, lon_t, departure_row, extents, area, fields)


def row_kernel(shift_ref, mixed_ref, out_ref, held, sem):
    rows, field_count, levels, lon_count = mixed_ref.shape
    tiles = lon_count // LANES
    lane = lax.broadcasted_iota(jnp.int32, (levels, LANES), 1)

    def row_copy(row):
        return pltpu.make_async_copy(held.at[row], out_ref.at[row], sem.at[row])

    def some_rows(step, carry):
        for n in range(AT_ONCE):
            row = step * AT_ONCE + n
            first = lax.rem(shift_ref[row] - 1 + lon_count, lon_count)
            whole, rest = first // LANES, lax.rem(first, LANES)
            turn = lax.rem(LANES - rest, LANES)
            keep = lane < LANES - rest
            places = [pl.multiple_of(lax.rem(whole + t, tiles) * LANES, LANES) for t in range(tiles)]
            for f in range(field_count):
                turned = [pltpu.roll(mixed_ref[row, f, :, pl.ds(at, LANES)], turn, 1) for at in places]
                for t in range(tiles):
                    held[row, f, :, t * LANES:(t + 1) * LANES] = jnp.where(keep, turned[t], turned[(t + 1) % tiles])
        for n in range(AT_ONCE):
            row_copy(step * AT_ONCE + n).start()
        return carry

    lax.fori_loop(0, rows // AT_ONCE, some_rows, 0)
    for row in range(rows):
        row_copy(row).wait()


def rows_of(shift, mixed):
    rows = mixed.shape[0]
    return pl.pallas_call(
        row_kernel,
        out_shape=jax.ShapeDtypeStruct(mixed.shape, mixed.dtype),
        in_specs=[pl.BlockSpec(memory_space=pltpu.SMEM), pl.BlockSpec(memory_space=pltpu.VMEM)],
        out_specs=pl.BlockSpec(memory_space=pl.ANY),
        scratch_shapes=[pltpu.VMEM(mixed.shape, jnp.float32), pltpu.SemaphoreType.DMA((rows,))],
        compiler_params=pltpu.CompilerParams(vmem_limit_bytes=16 * 1024 * 1024),
        name="rows",
    )(shift, mixed)


def per_device(fields, lat_fraction, lon_fraction, lon_shift, departure_row, extents):
    bands = lax.axis_size("lat")
    total_rows = bands * fields.shape[0]
    row_ids = np.arange(total_rows)
    area = jnp.asarray(np.cos(math.pi * (row_ids + 0.5) / total_rows - math.pi / 2.0), jnp.float32)
    mixed = exchange(lat_fraction, lon_fraction, departure_row, extents, area, fields)
    return rows_of(lon_shift, mixed)


def solution(mesh):
    return jax.shard_map(
        per_device,
        mesh=mesh,
        in_specs=(
            P("lat", None, "lev", None),
            P("lat"),
            P("lat"),
            P("lat"),
            P("lat"),
            P("lat", None),
        ),
        out_specs=P("lat", None, "lev", None),
        check_vma=False,
    )
```

```python
import functools
import math

import jax
import jax.numpy as jnp
import numpy as np
from jax import lax
from jax.experimental import pallas as pl
from jax.experimental.pallas import tpu as pltpu
from jax.sharding import PartitionSpec as P

REACH = 4
LANES = 128
RING = 4
DEEP = 8
MESH = pl.DeviceIdType.MESH
CUTS = ((3, 2), (3, 2), (3, 2))
LEAD = 3
HOPS = 2
RELAYED = (0, 1, RING - 1)
LATE = 3
TOGETHER = 2
AT_ONCE = 2


def chunks_of(field_count, tiles):
    found = []
    for f in range(field_count):
        cuts = CUTS[f] if f < len(CUTS) and sum(CUTS[f]) == tiles else (tiles,)
        first = 0
        for width in cuts:
            found.append((f, first * LANES, width * LANES))
            first += width
    return found


def cubic(t):
    sixth = 1.0 / 6.0
    return (
        -t * (t - 1.0) * (t - 2.0) * sixth,
        (t + 1.0) * (t - 1.0) * (t - 2.0) * 0.5,
        -(t + 1.0) * t * (t - 2.0) * 0.5,
        (t + 1.0) * t * (t - 1.0) * sixth,
    )


def departure_of(row, first_row, rows, total_rows, departure_ref, extents_ref):
    low = first_row - extents_ref[0, 0] * rows + 1
    high = first_row + rows - 3 + extents_ref[0, 1] * rows
    inside = jnp.minimum(jnp.maximum(departure_ref[row], low), high)
    return jnp.minimum(jnp.maximum(inside, 1), total_rows - 3)


def exchange_kernel(bands, levs, lat_t_ref, lon_t_ref, departure_ref, extents_ref, area_ref, fields_ref,
                    out_ref, *scratch):
    rows, field_count, _, lon_count = fields_ref.shape
    piece = lon_count // RING
    chunks = chunks_of(field_count, piece // LANES)
    count = len(chunks)
    held, landed = scratch[:2]
    window = scratch[2:2 + count]
    column = scratch[2 + count:2 + 2 * count]
    passing = scratch[2 + 2 * count:2 + 3 * count]
    (real_meta, whole_meta, real_smem, whole_smem, part, met_one, met_two, met_three,
     load_sem, own_sem, smem_sem, meta_send, meta_recv, out_send, out_recv, halo_send, halo_recv,
     back_send, back_recv, one_send, one_recv, two_send, two_recv, three_send, three_recv,
     round_sem, pass_send, pass_recv) = scratch[2 + 3 * count:]
    band, lev = lax.axis_index("lat"), lax.axis_index("lev")
    group, member = band // RING, lax.rem(band, RING)
    groups = bands // RING
    crosses = groups // DEEP
    deep, cross = lax.rem(group, DEEP), group // DEEP
    first_row, total_rows = band * rows, bands * rows
    span = RING * rows

    def ring_member(step):
        return lax.rem(member + step, RING)

    def ring_peer(step):
        return group * RING + ring_member(step)

    def inside(distance):
        place = band + distance
        return jnp.logical_and(place >= 0, place < bands)

    near = [d for d in range(-REACH, REACH + 1) if d != 0]
    one_peers = [(dy, dl) for dy in range(RING) for dl in range(levs) if (dy, dl) != (0, 0)]

    def one_peer(dy, dl):
        return {"lat": ring_peer(dy), "lev": lax.rem(lev + dl, levs)}

    def two_peer(dx):
        return {"lat": (lax.rem(cross + dx, crosses) * DEEP + deep) * RING + member}

    def three_peer(dz):
        return {"lat": (cross * DEEP + lax.rem(deep + dz, DEEP)) * RING + member}

    barrier = pltpu.get_barrier_semaphore()

    def greet(peer):
        pl.semaphore_signal(barrier, inc=1, device_id=peer, device_id_type=MESH)

    for d in near:
        pl.when(inside(d))(functools.partial(greet, {"lat": band + d}))
    for dy, dl in one_peers:
        if dl:
            greet(one_peer(dy, dl))
    for step in (1, crosses - 1):
        greet(two_peer(step))
    for step in (1, DEEP - 1):
        greet(three_peer(step))

    load = pltpu.make_async_copy(fields_ref, held, load_sem)
    load.start()

    def cut(c, place):
        f, first, width = chunks[c]
        return (slice(None), f, slice(None), pl.ds(pl.multiple_of(place * piece + first, LANES), width))

    own_pieces = [
        pltpu.make_async_copy(
            fields_ref.at[cut(c, member)], window[c].at[pl.ds(span + member * rows, rows)], own_sem.at[0, c]
        )
        for c in range(count)
    ]
    for copy in own_pieces:
        copy.start()

    lane = lax.broadcasted_iota(jnp.int32, (1, LANES), 1)
    lat_t = jnp.zeros((1, LANES), jnp.float32)
    lon_t = jnp.zeros((1, LANES), jnp.float32)
    area = jnp.zeros((1, LANES), jnp.float32)
    start = jnp.zeros((1, LANES), jnp.int32)
    for row in range(rows):
        here = lane == row
        lat_t = jnp.where(here, lat_t_ref[row], lat_t)
        lon_t = jnp.where(here, lon_t_ref[row], lon_t)
        area = jnp.where(here, area_ref[first_row + row], area)
        departure = departure_of(row, first_row, rows, total_rows, departure_ref, extents_ref)
        start = jnp.where(here, departure - 1, start)
    lon_w = cubic(lon_t)
    for d in near:
        @pl.when(jnp.logical_not(inside(d)))
        def _(d=d):
            real_meta[REACH + d] = jnp.zeros(real_meta.shape[1:], jnp.float32)
            whole_meta[REACH + d] = jnp.zeros(whole_meta.shape[1:], jnp.int32)
    real_meta[REACH] = jnp.concatenate(
        [*cubic(lat_t), area * (lon_w[0] + lon_w[1] + lon_w[2] + lon_w[3]), jnp.zeros((3, LANES), jnp.float32)], axis=0
    )
    whole_meta[REACH] = jnp.broadcast_to(start, whole_meta.shape[1:])

    expected = sum(dl != 0 for _, dl in one_peers) + 4
    for d in near:
        expected = expected + inside(d).astype(jnp.int32)
    pl.semaphore_wait(barrier, expected)

    def tell(n):
        for step in (1, DEEP - 1):
            pl.semaphore_signal(round_sem.at[n], inc=1, device_id=three_peer(step), device_id_type=MESH)
        if n == 0:
            for step in (1, crosses - 1):
                pl.semaphore_signal(round_sem.at[n], inc=1, device_id=two_peer(step), device_id_type=MESH)

    def hear(n):
        pl.semaphore_wait(round_sem.at[n], 4 if n == 0 else 2)

    tell(0)

    def meta_copies(d):
        k = near.index(d)
        return [
            pltpu.make_async_remote_copy(
                src_ref=ref.at[REACH], dst_ref=ref.at[REACH - d],
                send_sem=meta_send.at[n, k], recv_sem=meta_recv.at[n, near.index(-d)],
                device_id={"lat": band + d}, device_id_type=MESH,
            )
            for n, ref in enumerate((real_meta, whole_meta))
        ]

    def meta_arrivals(d):
        k = near.index(d)
        return [
            pltpu.make_async_remote_copy(
                src_ref=ref.at[REACH + d], dst_ref=ref.at[REACH + d],
                send_sem=meta_send.at[n, k], recv_sem=meta_recv.at[n, k],
                device_id={"lat": band + d}, device_id_type=MESH,
            )
            for n, ref in enumerate((real_meta, whole_meta))
        ]

    for d in near:
        @pl.when(inside(d))
        def _(d=d):
            for copy in meta_copies(d):
                copy.start()

    def out_copy(c, dy):
        return pltpu.make_async_remote_copy(
            src_ref=fields_ref.at[cut(c, ring_member(dy))],
            dst_ref=window[c].at[pl.ds(span + member * rows, rows)],
            send_sem=out_send.at[c, dy - 1], recv_sem=out_recv.at[c, dy - 1],
            device_id={"lat": ring_peer(dy)}, device_id_type=MESH,
        )

    def out_arrival(c, dy):
        place = window[c].at[pl.ds(span + ring_member(RING - dy) * rows, rows)]
        return pltpu.make_async_remote_copy(
            src_ref=place, dst_ref=place, send_sem=out_send.at[c, dy - 1], recv_sem=out_recv.at[c, dy - 1],
            device_id={"lat": ring_peer(RING - dy)}, device_id_type=MESH,
        )

    has_side = (group < groups - 1, group > 0)

    def halo_place(c, dy, side):
        return window[c].at[pl.ds((0 if side == 0 else 2 * span) + ring_member(RING - dy) * rows, rows)]

    def halo_source(c, dy):
        if dy == 0:
            return fields_ref.at[cut(c, member)]
        return window[c].at[pl.ds(span + ring_member(RING - dy) * rows, rows)]

    def halo_copy(c, dy, side):
        return pltpu.make_async_remote_copy(
            src_ref=halo_source(c, dy), dst_ref=halo_place(c, dy, side),
            send_sem=halo_send.at[side, c, dy], recv_sem=halo_recv.at[side, c, dy],
            device_id={"lat": band + (RING if side == 0 else -RING)}, device_id_type=MESH,
        )

    edge = (jnp.logical_and(has_side[0], deep == DEEP - 1), jnp.logical_and(has_side[1], deep == 0))
    inner = tuple(jnp.logical_and(h, jnp.logical_not(e)) for h, e in zip(has_side, edge))
    shared = (cross + 1, crosses - cross)
    serves = (
        (jnp.logical_and(deep == DEEP - 1, cross > 0), cross),
        (jnp.logical_and(deep == 0, cross < crosses - 1), crosses - 1 - cross),
    )

    def pass_place(c, rank):
        return passing[c].at[pl.ds(rank * rows, rows)]

    def to_relay(c, dy, side):
        rank = RELAYED.index(dy)
        return pltpu.make_async_remote_copy(
            src_ref=halo_source(c, dy), dst_ref=pass_place(c, rank),
            send_sem=halo_send.at[side, c, dy], recv_sem=pass_recv.at[c, rank],
            device_id=two_peer(1 if side == 0 else crosses - 1), device_id_type=MESH,
        )

    def from_relay(c, dy, side):
        rank = RELAYED.index(dy)
        return pltpu.make_async_remote_copy(
            src_ref=pass_place(c, rank), dst_ref=halo_place(c, dy, side),
            send_sem=pass_send.at[c, rank], recv_sem=halo_recv.at[side, c, dy],
            device_id=three_peer(1 if side == 0 else DEEP - 1), device_id_type=MESH,
        )

    def at_relay(c, dy):
        rank = RELAYED.index(dy)
        place = pass_place(c, rank)
        return pltpu.make_async_remote_copy(
            src_ref=place, dst_ref=place, send_sem=pass_send.at[c, rank], recv_sem=pass_recv.at[c, rank],
            device_id=two_peer(1), device_id_type=MESH,
        )

    def start_edge(c, dy):
        for side in range(2):
            if dy in RELAYED:
                relayed = RELAYED.index(dy) < shared[side]
                pl.when(jnp.logical_and(edge[side], relayed))(lambda side=side: to_relay(c, dy, side).start())
                pl.when(jnp.logical_and(edge[side], jnp.logical_not(relayed)))(
                    lambda side=side: halo_copy(c, dy, side).start()
                )
            else:
                pl.when(edge[side])(lambda side=side: halo_copy(c, dy, side).start())

    def pass_along(c, dy):
        for side in range(2):
            serving, limit = serves[side]

            @pl.when(jnp.logical_and(serving, RELAYED.index(dy) < limit))
            def _(side=side):
                at_relay(c, dy).wait_recv()
                from_relay(c, dy, side).start()

    def passed_along(c, dy):
        for side in range(2):
            serving, limit = serves[side]
            pl.when(jnp.logical_and(serving, RELAYED.index(dy) < limit))(
                lambda side=side: from_relay(c, dy, side).wait_send()
            )

    def halo_arrival(c, dy, side):
        place = halo_place(c, dy, side)
        return pltpu.make_async_remote_copy(
            src_ref=place, dst_ref=place, send_sem=halo_send.at[side, c, dy], recv_sem=halo_recv.at[side, c, dy],
            device_id={"lat": band + (-RING if side == 0 else RING)}, device_id_type=MESH,
        )

    def start_halo(c, dy):
        for side in range(2):
            pl.when(inner[side])(lambda side=side: halo_copy(c, dy, side).start())

    def back_copy(c, dy):
        return pltpu.make_async_remote_copy(
            src_ref=column[c].at[pl.ds(dy * rows, rows)],
            dst_ref=landed.at[cut(c, member)],
            send_sem=back_send.at[c, dy - 1], recv_sem=back_recv.at[c, dy - 1],
            device_id={"lat": ring_peer(dy)}, device_id_type=MESH,
        )

    def back_arrival(c, dy):
        place = landed.at[cut(c, ring_member(RING - dy))]
        return pltpu.make_async_remote_copy(
            src_ref=place, dst_ref=place, send_sem=back_send.at[c, dy - 1], recv_sem=back_recv.at[c, dy - 1],
            device_id={"lat": ring_peer(RING - dy)}, device_id_type=MESH,
        )

    def back_own(c):
        return pltpu.make_async_copy(column[c].at[pl.ds(0, rows)], landed.at[cut(c, member)], own_sem.at[1, c])

    def small_copy(source, target, sends, arrivals, k, peer):
        return pltpu.make_async_remote_copy(
            src_ref=source, dst_ref=target.at[k], send_sem=sends.at[k], recv_sem=arrivals.at[k],
            device_id=peer, device_id_type=MESH,
        )

    ones = [small_copy(part.at[0], met_one, one_send, one_recv, k, one_peer(*p)) for k, p in enumerate(one_peers)]
    twos = [small_copy(part.at[1], met_two, two_send, two_recv, dx - 1, two_peer(dx)) for dx in range(1, crosses)]
    threes = [small_copy(part.at[2], met_three, three_send, three_recv, dz - 1, three_peer(dz)) for dz in range(1, DEEP)]

    order = (1, RING - 1, *range(2, RING - 1))
    slots = [(c, 0) for c in range(min(LEAD, count))]
    for c in range(count):
        slots += [(c, dy) for dy in order] + [(c + LEAD, 0)] * (c + LEAD < count)
    place_of = {slot: k for k, slot in enumerate(slots)}
    start_halo(*slots[0])
    start_edge(*slots[0])
    for c in range(min(2, count)):
        for dy in order:
            out_copy(c, dy).start()
    for slot in slots[1:LEAD]:
        start_halo(*slot)
        start_edge(*slot)

    for d in near:
        @pl.when(inside(d))
        def _(d=d):
            for copy in meta_arrivals(d):
                copy.wait_recv()
    group_slots = pl.ds(REACH - member, RING)
    to_smem = [
        pltpu.make_async_copy(real_meta.at[group_slots], real_smem, smem_sem.at[0]),
        pltpu.make_async_copy(whole_meta.at[group_slots], whole_smem, smem_sem.at[1]),
    ]
    for copy in to_smem:
        copy.start()
    load.wait()

    def add_row(row, totals):
        taken = jnp.zeros((2 * REACH + 1, LANES), jnp.float32)
        for a in range(4):
            hit = whole_meta[:, 0, :] + a == first_row + row
            taken = taken + jnp.where(hit, real_meta[:, a, :] * real_meta[:, 4, :], 0.0)
        taken = jnp.sum(jnp.sum(taken, axis=0, keepdims=True), axis=1, keepdims=True)
        row_area = area_ref[first_row + row]
        before, after = [], []
        for f in range(field_count):
            tile = held[row, f, :, 0:LANES]
            for t in range(1, lon_count // LANES):
                tile = tile + held[row, f, :, t * LANES:(t + 1) * LANES]
            total = jnp.sum(tile, axis=0, keepdims=True)
            before.append(totals[f] + row_area * total)
            after.append(totals[field_count + f] + taken * total)
        return tuple(before + after)

    zero = jnp.zeros((1, LANES), jnp.float32)
    totals = lax.fori_loop(0, rows, add_row, (zero,) * (2 * field_count))
    part[0] = jnp.concatenate([*totals, jnp.zeros((8 - 2 * field_count, LANES), jnp.float32)], axis=0)

    def gather_small(copies, target, level):
        for copy in copies:
            copy.wait_recv()
        total = part[level]
        for k in range(len(copies)):
            total = total + target[k]
        return total

    for copy in ones:
        copy.start()
    for c in range(min(2, count), count):
        for dy in order:
            out_copy(c, dy).start()

    base = (group - 1) * span

    def interpolate(c, dy):
        to = ring_member(dy)

        def one_row(row, carry):
            place = whole_smem[to, 0, row] - base
            weight = [real_smem[to, a, row] for a in range(4)]
            for t in range(chunks[c][2] // LANES):
                at = pl.ds(t * LANES, LANES)
                total = weight[0] * window[c][place, :, at]
                for a in range(1, 4):
                    total = total + weight[a] * window[c][place + a, :, at]
                column[c][dy * rows + row, :, at] = total
            return carry

        lax.fori_loop(0, rows, one_row, 0)

    def finish_chunk(c):
        if c == 0:
            for copy in to_smem:
                copy.wait()
        own_pieces[c].wait()
        for dy in (0, *order):
            for side in range(2):
                pl.when(has_side[1 - side])(lambda dy=dy, side=side: halo_arrival(c, dy, side).wait_recv())
        for dy in (2, 1, RING - 1, 0):
            interpolate(c, dy)
        for dy in (2, 1, RING - 1):
            back_copy(c, dy).start()
        back_own(c).start()

    def one_done():
        part[1] = gather_small(ones, met_one, 0)
        for copy in twos:
            copy.start()

    def two_done():
        part[2] = gather_small(twos, met_two, 1)
        hear(2)
        for copy in threes:
            copy.start()

    def pass_on(n):
        hear(n)
        tell(n + 1)

    lanes = lax.broadcasted_iota(jnp.int32, fields_ref.shape[2:3] + (LANES,), 1)
    tiles = lon_count // LANES

    def shifted(pieces, step):
        turned = [pltpu.roll(piece, LANES - step, 1) for piece in pieces]
        return [jnp.where(lanes < LANES - step, turned[t], turned[(t + 1) % tiles]) for t in range(tiles)]

    def along(f, sums):
        for c in range(count):
            if chunks[c][0] == f:
                back_own(c).wait()
                for dy in order:
                    back_arrival(c, dy).wait_recv()
        before = jnp.sum(sums[f:f + 1], axis=1, keepdims=True)
        after = jnp.sum(sums[field_count + f:field_count + f + 1], axis=1, keepdims=True)
        ratio = before / after

        def some_rows(step, carry):
            for n in range(TOGETHER):
                row = step * TOGETHER + n
                lon = [weight * ratio for weight in cubic(lon_t_ref[row])]
                here = [landed[row, f, :, t * LANES:(t + 1) * LANES] for t in range(tiles)]
                after = shifted(here, 1)
                later = shifted([lon[2] * here[t] + lon[3] * after[t] for t in range(tiles)], 2)
                for t in range(tiles):
                    mixed = lon[0] * here[t] + lon[1] * after[t] + later[t]
                    out_ref[row, f, :, t * LANES:(t + 1) * LANES] = mixed
            return carry

        lax.fori_loop(0, rows // TOGETHER, some_rows, 0)

    sums = []
    tasks = {k: [] for k in range(len(slots) + LATE)}
    tasks[4].append(functools.partial(pass_on, 0))
    tasks[6].append(one_done)
    tasks[7].append(functools.partial(pass_on, 1))
    tasks[9].append(two_done)
    for c in range(count):
        tasks[place_of[c, order[-1]] + LATE].append(functools.partial(finish_chunk, c))
    tasks[place_of[count - 3, order[-1]] + LATE].append(
        lambda: sums.append(gather_small(threes, met_three, 2))
    )
    for f in range(field_count - 1):
        near_end = count - field_count + 1 + f
        tasks[place_of[near_end - 1, order[-1]] + LATE].append(functools.partial(lambda f: along(f, sums[0]), f))
    sent_at = {slot: k + 1 for k, slot in enumerate(slots[:LEAD])}
    arrived = set()

    def await_arrival(slot):
        if slot[1] and slot not in arrived:
            arrived.add(slot)
            out_arrival(*slot).wait_recv()

    reached = LEAD
    for k in range(LEAD, len(slots) + LATE):
        if k < len(slots):
            await_arrival(slots[k])
            for side in range(2):
                pl.when(inner[side])(lambda k=k, side=side: halo_copy(*slots[k - LEAD], side).wait_send())
            start_halo(*slots[k])
            until = min(len(slots), LEAD + -(-(k - LEAD + 1) * RING // (RING - 1)))
            for slot in slots[reached:until]:
                await_arrival(slot)
                start_edge(*slot)
                sent_at[slot] = k
            reached = until
        for slot in slots:
            if slot[1] in RELAYED and sent_at.get(slot, k) + HOPS == k:
                pass_along(*slot)
        for task in tasks[k]:
            task()

    along(field_count - 1, sums[0])
    for d in near:
        @pl.when(inside(d))
        def _(d=d):
            for copy in meta_copies(d):
                copy.wait_send()
    for copy in ones + twos + threes:
        copy.wait_send()
    for c in range(count):
        for dy in order:
            out_copy(c, dy).wait_send()
            back_copy(c, dy).wait_send()
    for k, slot in enumerate(slots):
        for side in range(2):
            if k >= len(slots) - LEAD:
                pl.when(inner[side])(lambda slot=slot, side=side: halo_copy(*slot, side).wait_send())
            pl.when(edge[side])(lambda slot=slot, side=side: halo_copy(*slot, side).wait_send())
        if slot[1] in RELAYED:
            passed_along(*slot)


def exchange(lat_t, lon_t, departure_row, extents, area, fields):
    bands, levs = lax.axis_size("lat"), lax.axis_size("lev")
    rows, field_count, levels, lon_count = fields.shape
    crosses = bands // RING // DEEP
    piece = lon_count // RING
    tile = (8, LANES)
    dma = pltpu.SemaphoreType.DMA
    ones = RING * levs - 1
    near = 2 * REACH
    chunks = chunks_of(field_count, piece // LANES)
    count = len(chunks)
    return pl.pallas_call(
        functools.partial(exchange_kernel, bands, levs),
        out_shape=pltpu.VMEM(fields.shape, fields.dtype),
        in_specs=[pl.BlockSpec(memory_space=pltpu.SMEM)] * 5 + [pl.BlockSpec(memory_space=pl.ANY)],
        out_specs=pl.BlockSpec(memory_space=pltpu.VMEM),
        scratch_shapes=[
            pltpu.VMEM(fields.shape, jnp.float32),
            pltpu.VMEM(fields.shape, jnp.float32),
            *[pltpu.VMEM((3 * RING * rows, levels, width), jnp.float32) for _, _, width in chunks],
            *[pltpu.VMEM((RING * rows, levels, width), jnp.float32) for _, _, width in chunks],
            *[pltpu.VMEM((len(RELAYED) * rows, levels, width), jnp.float32) for _, _, width in chunks],
            pltpu.VMEM((near + 1,) + tile, jnp.float32),
            pltpu.VMEM((near + 1,) + tile, jnp.int32),
            pltpu.SMEM((RING,) + tile, jnp.float32),
            pltpu.SMEM((RING,) + tile, jnp.int32),
            pltpu.VMEM((3,) + tile, jnp.float32),
            pltpu.VMEM((ones,) + tile, jnp.float32),
            pltpu.VMEM((max(crosses - 1, 1),) + tile, jnp.float32),
            pltpu.VMEM((DEEP - 1,) + tile, jnp.float32),
            dma,
            dma((2, count)),
            dma((2,)),
            dma((2, near)),
            dma((2, near)),
            dma((count, RING - 1)),
            dma((count, RING - 1)),
            dma((2, count, RING)),
            dma((2, count, RING)),
            dma((count, RING - 1)),
            dma((count, RING - 1)),
            dma((ones,)),
            dma((ones,)),
            dma((max(crosses - 1, 1),)),
            dma((max(crosses - 1, 1),)),
            dma((DEEP - 1,)),
            dma((DEEP - 1,)),
            pltpu.SemaphoreType.REGULAR((3,)),
            dma((count, len(RELAYED))),
            dma((count, len(RELAYED))),
        ],
        compiler_params=pltpu.CompilerParams(
            collective_id=0, has_side_effects=True, vmem_limit_bytes=60000 * 1024
        ),
        name="exchange",
    )(lat_t, lon_t, departure_row, extents, area, fields)


def row_kernel(shift_ref, mixed_ref, out_ref, held, sem):
    rows, field_count, levels, lon_count = mixed_ref.shape
    tiles = lon_count // LANES
    lane = lax.broadcasted_iota(jnp.int32, (levels, LANES), 1)

    def row_copy(row):
        return pltpu.make_async_copy(held.at[row], out_ref.at[row], sem.at[row])

    def some_rows(step, carry):
        for n in range(AT_ONCE):
            row = step * AT_ONCE + n
            first = lax.rem(shift_ref[row] - 1 + lon_count, lon_count)
            whole, rest = first // LANES, lax.rem(first, LANES)
            turn = lax.rem(LANES - rest, LANES)
            keep = lane < LANES - rest
            places = [pl.multiple_of(lax.rem(whole + t, tiles) * LANES, LANES) for t in range(tiles)]
            for f in range(field_count):
                turned = [pltpu.roll(mixed_ref[row, f, :, pl.ds(at, LANES)], turn, 1) for at in places]
                for t in range(tiles):
                    held[row, f, :, t * LANES:(t + 1) * LANES] = jnp.where(keep, turned[t], turned[(t + 1) % tiles])
        for n in range(AT_ONCE):
            row_copy(step * AT_ONCE + n).start()
        return carry

    lax.fori_loop(0, rows // AT_ONCE, some_rows, 0)
    for row in range(rows):
        row_copy(row).wait()


def rows_of(shift, mixed):
    rows = mixed.shape[0]
    return pl.pallas_call(
        row_kernel,
        out_shape=jax.ShapeDtypeStruct(mixed.shape, mixed.dtype),
        in_specs=[pl.BlockSpec(memory_space=pltpu.SMEM), pl.BlockSpec(memory_space=pltpu.VMEM)],
        out_specs=pl.BlockSpec(memory_space=pl.ANY),
        scratch_shapes=[pltpu.VMEM(mixed.shape, jnp.float32), pltpu.SemaphoreType.DMA((rows,))],
        compiler_params=pltpu.CompilerParams(vmem_limit_bytes=16 * 1024 * 1024),
        name="rows",
    )(shift, mixed)


def per_device(fields, lat_fraction, lon_fraction, lon_shift, departure_row, extents):
    bands = lax.axis_size("lat")
    total_rows = bands * fields.shape[0]
    row_ids = np.arange(total_rows)
    area = jnp.asarray(np.cos(math.pi * (row_ids + 0.5) / total_rows - math.pi / 2.0), jnp.float32)
    mixed = exchange(lat_fraction, lon_fraction, departure_row, extents, area, fields)
    return rows_of(lon_shift, mixed)


def solution(mesh):
    return jax.shard_map(
        per_device,
        mesh=mesh,
        in_specs=(
            P("lat", None, "lev", None),
            P("lat"),
            P("lat"),
            P("lat"),
            P("lat"),
            P("lat", None),
        ),
        out_specs=P("lat", None, "lev", None),
        check_vma=False,
    )
```

```python
import functools
import math

import jax
import jax.numpy as jnp
import numpy as np
from jax import lax
from jax.experimental import pallas as pl
from jax.experimental.pallas import tpu as pltpu
from jax.sharding import PartitionSpec as P

REACH = 4
LANES = 128
RING = 4
DEEP = 8
MESH = pl.DeviceIdType.MESH
CUTS = ((3, 2), (3, 2), (3, 2))
LEAD = 3
HOPS = 2
RELAYED = (0, 1, RING - 1)
LATE = 3
TOGETHER = 2


def chunks_of(field_count, tiles):
    found = []
    for f in range(field_count):
        cuts = CUTS[f] if f < len(CUTS) and sum(CUTS[f]) == tiles else (tiles,)
        first = 0
        for width in cuts:
            found.append((f, first * LANES, width * LANES))
            first += width
    return found


def cubic(t):
    sixth = 1.0 / 6.0
    return (
        -t * (t - 1.0) * (t - 2.0) * sixth,
        (t + 1.0) * (t - 1.0) * (t - 2.0) * 0.5,
        -(t + 1.0) * t * (t - 2.0) * 0.5,
        (t + 1.0) * t * (t - 1.0) * sixth,
    )


def departure_of(row, first_row, rows, total_rows, departure_ref, extents_ref):
    low = first_row - extents_ref[0, 0] * rows + 1
    high = first_row + rows - 3 + extents_ref[0, 1] * rows
    inside = jnp.minimum(jnp.maximum(departure_ref[row], low), high)
    return jnp.minimum(jnp.maximum(inside, 1), total_rows - 3)


def exchange_kernel(bands, levs, lat_t_ref, lon_t_ref, shift_ref, departure_ref, extents_ref, area_ref, fields_ref,
                    out_ref, *scratch):
    rows, field_count, _, lon_count = fields_ref.shape
    piece = lon_count // RING
    chunks = chunks_of(field_count, piece // LANES)
    count = len(chunks)
    held, landed = scratch[:2]
    window = scratch[2:2 + count]
    column = scratch[2 + count:2 + 2 * count]
    passing = scratch[2 + 2 * count:2 + 3 * count]
    (real_meta, whole_meta, real_smem, whole_smem, part, met_one, met_two, met_three,
     load_sem, own_sem, smem_sem, meta_send, meta_recv, out_send, out_recv, halo_send, halo_recv,
     back_send, back_recv, one_send, one_recv, two_send, two_recv, three_send, three_recv,
     round_sem, pass_send, pass_recv) = scratch[2 + 3 * count:]
    band, lev = lax.axis_index("lat"), lax.axis_index("lev")
    group, member = band // RING, lax.rem(band, RING)
    groups = bands // RING
    crosses = groups // DEEP
    deep, cross = lax.rem(group, DEEP), group // DEEP
    first_row, total_rows = band * rows, bands * rows
    span = RING * rows

    def ring_member(step):
        return lax.rem(member + step, RING)

    def ring_peer(step):
        return group * RING + ring_member(step)

    def inside(distance):
        place = band + distance
        return jnp.logical_and(place >= 0, place < bands)

    near = [d for d in range(-REACH, REACH + 1) if d != 0]
    one_peers = [(dy, dl) for dy in range(RING) for dl in range(levs) if (dy, dl) != (0, 0)]

    def one_peer(dy, dl):
        return {"lat": ring_peer(dy), "lev": lax.rem(lev + dl, levs)}

    def two_peer(dx):
        return {"lat": (lax.rem(cross + dx, crosses) * DEEP + deep) * RING + member}

    def three_peer(dz):
        return {"lat": (cross * DEEP + lax.rem(deep + dz, DEEP)) * RING + member}

    barrier = pltpu.get_barrier_semaphore()

    def greet(peer):
        pl.semaphore_signal(barrier, inc=1, device_id=peer, device_id_type=MESH)

    for d in near:
        pl.when(inside(d))(functools.partial(greet, {"lat": band + d}))
    for dy, dl in one_peers:
        if dl:
            greet(one_peer(dy, dl))
    for step in (1, crosses - 1):
        greet(two_peer(step))
    for step in (1, DEEP - 1):
        greet(three_peer(step))

    load = pltpu.make_async_copy(fields_ref, held, load_sem)
    load.start()

    def cut(c, place):
        f, first, width = chunks[c]
        return (slice(None), f, slice(None), pl.ds(pl.multiple_of(place * piece + first, LANES), width))

    own_pieces = [
        pltpu.make_async_copy(
            fields_ref.at[cut(c, member)], window[c].at[pl.ds(span + member * rows, rows)], own_sem.at[0, c]
        )
        for c in range(count)
    ]
    for copy in own_pieces:
        copy.start()

    lane = lax.broadcasted_iota(jnp.int32, (1, LANES), 1)
    lat_t = jnp.zeros((1, LANES), jnp.float32)
    lon_t = jnp.zeros((1, LANES), jnp.float32)
    area = jnp.zeros((1, LANES), jnp.float32)
    start = jnp.zeros((1, LANES), jnp.int32)
    for row in range(rows):
        here = lane == row
        lat_t = jnp.where(here, lat_t_ref[row], lat_t)
        lon_t = jnp.where(here, lon_t_ref[row], lon_t)
        area = jnp.where(here, area_ref[first_row + row], area)
        departure = departure_of(row, first_row, rows, total_rows, departure_ref, extents_ref)
        start = jnp.where(here, departure - 1, start)
    lon_w = cubic(lon_t)
    for d in near:
        @pl.when(jnp.logical_not(inside(d)))
        def _(d=d):
            real_meta[REACH + d] = jnp.zeros(real_meta.shape[1:], jnp.float32)
            whole_meta[REACH + d] = jnp.zeros(whole_meta.shape[1:], jnp.int32)
    real_meta[REACH] = jnp.concatenate(
        [*cubic(lat_t), area * (lon_w[0] + lon_w[1] + lon_w[2] + lon_w[3]), jnp.zeros((3, LANES), jnp.float32)], axis=0
    )
    whole_meta[REACH] = jnp.broadcast_to(start, whole_meta.shape[1:])

    expected = sum(dl != 0 for _, dl in one_peers) + 4
    for d in near:
        expected = expected + inside(d).astype(jnp.int32)
    pl.semaphore_wait(barrier, expected)

    def tell(n):
        for step in (1, DEEP - 1):
            pl.semaphore_signal(round_sem.at[n], inc=1, device_id=three_peer(step), device_id_type=MESH)
        if n == 0:
            for step in (1, crosses - 1):
                pl.semaphore_signal(round_sem.at[n], inc=1, device_id=two_peer(step), device_id_type=MESH)

    def hear(n):
        pl.semaphore_wait(round_sem.at[n], 4 if n == 0 else 2)

    tell(0)

    def meta_copies(d):
        k = near.index(d)
        return [
            pltpu.make_async_remote_copy(
                src_ref=ref.at[REACH], dst_ref=ref.at[REACH - d],
                send_sem=meta_send.at[n, k], recv_sem=meta_recv.at[n, near.index(-d)],
                device_id={"lat": band + d}, device_id_type=MESH,
            )
            for n, ref in enumerate((real_meta, whole_meta))
        ]

    def meta_arrivals(d):
        k = near.index(d)
        return [
            pltpu.make_async_remote_copy(
                src_ref=ref.at[REACH + d], dst_ref=ref.at[REACH + d],
                send_sem=meta_send.at[n, k], recv_sem=meta_recv.at[n, k],
                device_id={"lat": band + d}, device_id_type=MESH,
            )
            for n, ref in enumerate((real_meta, whole_meta))
        ]

    for d in near:
        @pl.when(inside(d))
        def _(d=d):
            for copy in meta_copies(d):
                copy.start()

    def out_copy(c, dy):
        return pltpu.make_async_remote_copy(
            src_ref=fields_ref.at[cut(c, ring_member(dy))],
            dst_ref=window[c].at[pl.ds(span + member * rows, rows)],
            send_sem=out_send.at[c, dy - 1], recv_sem=out_recv.at[c, dy - 1],
            device_id={"lat": ring_peer(dy)}, device_id_type=MESH,
        )

    def out_arrival(c, dy):
        place = window[c].at[pl.ds(span + ring_member(RING - dy) * rows, rows)]
        return pltpu.make_async_remote_copy(
            src_ref=place, dst_ref=place, send_sem=out_send.at[c, dy - 1], recv_sem=out_recv.at[c, dy - 1],
            device_id={"lat": ring_peer(RING - dy)}, device_id_type=MESH,
        )

    has_side = (group < groups - 1, group > 0)

    def halo_place(c, dy, side):
        return window[c].at[pl.ds((0 if side == 0 else 2 * span) + ring_member(RING - dy) * rows, rows)]

    def halo_source(c, dy):
        if dy == 0:
            return fields_ref.at[cut(c, member)]
        return window[c].at[pl.ds(span + ring_member(RING - dy) * rows, rows)]

    def halo_copy(c, dy, side):
        return pltpu.make_async_remote_copy(
            src_ref=halo_source(c, dy), dst_ref=halo_place(c, dy, side),
            send_sem=halo_send.at[side, c, dy], recv_sem=halo_recv.at[side, c, dy],
            device_id={"lat": band + (RING if side == 0 else -RING)}, device_id_type=MESH,
        )

    edge = (jnp.logical_and(has_side[0], deep == DEEP - 1), jnp.logical_and(has_side[1], deep == 0))
    inner = tuple(jnp.logical_and(h, jnp.logical_not(e)) for h, e in zip(has_side, edge))
    shared = (cross + 1, crosses - cross)
    serves = (
        (jnp.logical_and(deep == DEEP - 1, cross > 0), cross),
        (jnp.logical_and(deep == 0, cross < crosses - 1), crosses - 1 - cross),
    )

    def pass_place(c, rank):
        return passing[c].at[pl.ds(rank * rows, rows)]

    def to_relay(c, dy, side):
        rank = RELAYED.index(dy)
        return pltpu.make_async_remote_copy(
            src_ref=halo_source(c, dy), dst_ref=pass_place(c, rank),
            send_sem=halo_send.at[side, c, dy], recv_sem=pass_recv.at[c, rank],
            device_id=two_peer(1 if side == 0 else crosses - 1), device_id_type=MESH,
        )

    def from_relay(c, dy, side):
        rank = RELAYED.index(dy)
        return pltpu.make_async_remote_copy(
            src_ref=pass_place(c, rank), dst_ref=halo_place(c, dy, side),
            send_sem=pass_send.at[c, rank], recv_sem=halo_recv.at[side, c, dy],
            device_id=three_peer(1 if side == 0 else DEEP - 1), device_id_type=MESH,
        )

    def at_relay(c, dy):
        rank = RELAYED.index(dy)
        place = pass_place(c, rank)
        return pltpu.make_async_remote_copy(
            src_ref=place, dst_ref=place, send_sem=pass_send.at[c, rank], recv_sem=pass_recv.at[c, rank],
            device_id=two_peer(1), device_id_type=MESH,
        )

    def start_edge(c, dy):
        for side in range(2):
            if dy in RELAYED:
                relayed = RELAYED.index(dy) < shared[side]
                pl.when(jnp.logical_and(edge[side], relayed))(lambda side=side: to_relay(c, dy, side).start())
                pl.when(jnp.logical_and(edge[side], jnp.logical_not(relayed)))(
                    lambda side=side: halo_copy(c, dy, side).start()
                )
            else:
                pl.when(edge[side])(lambda side=side: halo_copy(c, dy, side).start())

    def pass_along(c, dy):
        for side in range(2):
            serving, limit = serves[side]

            @pl.when(jnp.logical_and(serving, RELAYED.index(dy) < limit))
            def _(side=side):
                at_relay(c, dy).wait_recv()
                from_relay(c, dy, side).start()

    def passed_along(c, dy):
        for side in range(2):
            serving, limit = serves[side]
            pl.when(jnp.logical_and(serving, RELAYED.index(dy) < limit))(
                lambda side=side: from_relay(c, dy, side).wait_send()
            )

    def halo_arrival(c, dy, side):
        place = halo_place(c, dy, side)
        return pltpu.make_async_remote_copy(
            src_ref=place, dst_ref=place, send_sem=halo_send.at[side, c, dy], recv_sem=halo_recv.at[side, c, dy],
            device_id={"lat": band + (-RING if side == 0 else RING)}, device_id_type=MESH,
        )

    def start_halo(c, dy):
        for side in range(2):
            pl.when(inner[side])(lambda side=side: halo_copy(c, dy, side).start())

    def back_copy(c, dy):
        return pltpu.make_async_remote_copy(
            src_ref=column[c].at[pl.ds(dy * rows, rows)],
            dst_ref=landed.at[cut(c, member)],
            send_sem=back_send.at[c, dy - 1], recv_sem=back_recv.at[c, dy - 1],
            device_id={"lat": ring_peer(dy)}, device_id_type=MESH,
        )

    def back_arrival(c, dy):
        place = landed.at[cut(c, ring_member(RING - dy))]
        return pltpu.make_async_remote_copy(
            src_ref=place, dst_ref=place, send_sem=back_send.at[c, dy - 1], recv_sem=back_recv.at[c, dy - 1],
            device_id={"lat": ring_peer(RING - dy)}, device_id_type=MESH,
        )

    def back_own(c):
        return pltpu.make_async_copy(column[c].at[pl.ds(0, rows)], landed.at[cut(c, member)], own_sem.at[1, c])

    def small_copy(source, target, sends, arrivals, k, peer):
        return pltpu.make_async_remote_copy(
            src_ref=source, dst_ref=target.at[k], send_sem=sends.at[k], recv_sem=arrivals.at[k],
            device_id=peer, device_id_type=MESH,
        )

    ones = [small_copy(part.at[0], met_one, one_send, one_recv, k, one_peer(*p)) for k, p in enumerate(one_peers)]
    twos = [small_copy(part.at[1], met_two, two_send, two_recv, dx - 1, two_peer(dx)) for dx in range(1, crosses)]
    threes = [small_copy(part.at[2], met_three, three_send, three_recv, dz - 1, three_peer(dz)) for dz in range(1, DEEP)]

    order = (1, RING - 1, *range(2, RING - 1))
    slots = [(c, 0) for c in range(min(LEAD, count))]
    for c in range(count):
        slots += [(c, dy) for dy in order] + [(c + LEAD, 0)] * (c + LEAD < count)
    place_of = {slot: k for k, slot in enumerate(slots)}
    start_halo(*slots[0])
    start_edge(*slots[0])
    for c in range(min(2, count)):
        for dy in order:
            out_copy(c, dy).start()
    for slot in slots[1:LEAD]:
        start_halo(*slot)
        start_edge(*slot)

    for d in near:
        @pl.when(inside(d))
        def _(d=d):
            for copy in meta_arrivals(d):
                copy.wait_recv()
    group_slots = pl.ds(REACH - member, RING)
    to_smem = [
        pltpu.make_async_copy(real_meta.at[group_slots], real_smem, smem_sem.at[0]),
        pltpu.make_async_copy(whole_meta.at[group_slots], whole_smem, smem_sem.at[1]),
    ]
    for copy in to_smem:
        copy.start()
    load.wait()

    def add_row(row, totals):
        taken = jnp.zeros((2 * REACH + 1, LANES), jnp.float32)
        for a in range(4):
            hit = whole_meta[:, 0, :] + a == first_row + row
            taken = taken + jnp.where(hit, real_meta[:, a, :] * real_meta[:, 4, :], 0.0)
        taken = jnp.sum(jnp.sum(taken, axis=0, keepdims=True), axis=1, keepdims=True)
        row_area = area_ref[first_row + row]
        before, after = [], []
        for f in range(field_count):
            tile = held[row, f, :, 0:LANES]
            for t in range(1, lon_count // LANES):
                tile = tile + held[row, f, :, t * LANES:(t + 1) * LANES]
            total = jnp.sum(tile, axis=0, keepdims=True)
            before.append(totals[f] + row_area * total)
            after.append(totals[field_count + f] + taken * total)
        return tuple(before + after)

    zero = jnp.zeros((1, LANES), jnp.float32)
    totals = lax.fori_loop(0, rows, add_row, (zero,) * (2 * field_count))
    part[0] = jnp.concatenate([*totals, jnp.zeros((8 - 2 * field_count, LANES), jnp.float32)], axis=0)

    def gather_small(copies, target, level):
        for copy in copies:
            copy.wait_recv()
        total = part[level]
        for k in range(len(copies)):
            total = total + target[k]
        return total

    for copy in ones:
        copy.start()
    for c in range(min(2, count), count):
        for dy in order:
            out_copy(c, dy).start()

    base = (group - 1) * span

    def interpolate(c, dy):
        to = ring_member(dy)

        def one_row(row, carry):
            place = whole_smem[to, 0, row] - base
            weight = [real_smem[to, a, row] for a in range(4)]
            for t in range(chunks[c][2] // LANES):
                at = pl.ds(t * LANES, LANES)
                total = weight[0] * window[c][place, :, at]
                for a in range(1, 4):
                    total = total + weight[a] * window[c][place + a, :, at]
                column[c][dy * rows + row, :, at] = total
            return carry

        lax.fori_loop(0, rows, one_row, 0)

    def finish_chunk(c):
        if c == 0:
            for copy in to_smem:
                copy.wait()
        own_pieces[c].wait()
        for dy in (0, *order):
            for side in range(2):
                pl.when(has_side[1 - side])(lambda dy=dy, side=side: halo_arrival(c, dy, side).wait_recv())
        for dy in (2, 1, RING - 1, 0):
            interpolate(c, dy)
        for dy in (2, 1, RING - 1):
            back_copy(c, dy).start()
        back_own(c).start()

    def one_done():
        part[1] = gather_small(ones, met_one, 0)
        for copy in twos:
            copy.start()

    def two_done():
        part[2] = gather_small(twos, met_two, 1)
        hear(2)
        for copy in threes:
            copy.start()

    def pass_on(n):
        hear(n)
        tell(n + 1)

    lanes = lax.broadcasted_iota(jnp.int32, fields_ref.shape[2:3] + (LANES,), 1)
    tiles = lon_count // LANES

    def shifted(pieces, step):
        turned = [pltpu.roll(piece, LANES - step, 1) for piece in pieces]
        return [jnp.where(lanes < LANES - step, turned[t], turned[(t + 1) % tiles]) for t in range(tiles)]

    def along(f, sums):
        for c in range(count):
            if chunks[c][0] == f:
                back_own(c).wait()
                for dy in order:
                    back_arrival(c, dy).wait_recv()
        before = jnp.sum(sums[f:f + 1], axis=1, keepdims=True)
        after = jnp.sum(sums[field_count + f:field_count + f + 1], axis=1, keepdims=True)
        ratio = before / after

        def some_rows(step, carry):
            for n in range(TOGETHER):
                row = step * TOGETHER + n
                lon = [weight * ratio for weight in cubic(lon_t_ref[row])]
                here = [landed[row, f, :, t * LANES:(t + 1) * LANES] for t in range(tiles)]
                after = shifted(here, 1)
                later = shifted([lon[2] * here[t] + lon[3] * after[t] for t in range(tiles)], 2)
                moved = []
                for t in range(tiles):
                    mixed = lon[0] * here[t] + lon[1] * after[t] + later[t]
                    moved.append(mixed)
                first = lax.rem(shift_ref[row] - 1 + lon_count, lon_count)
                ahead = jnp.full(lanes.shape, first, jnp.int32)
                step_by = LANES
                while step_by < lon_count:
                    jump = (ahead & step_by) != 0
                    moved = [jnp.where(jump, moved[(t + step_by // LANES) % tiles], moved[t]) for t in range(tiles)]
                    step_by *= 2
                rest = ahead & (LANES - 1)
                pick = (lanes + rest) & (LANES - 1)
                moved = [jnp.take_along_axis(part_of, pick, axis=1) for part_of in moved]
                keep = lanes + rest < LANES
                for t in range(tiles):
                    out_ref[row, f, :, t * LANES:(t + 1) * LANES] = jnp.where(keep, moved[t], moved[(t + 1) % tiles])
            return carry

        lax.fori_loop(0, rows // TOGETHER, some_rows, 0)

    sums = []
    tasks = {k: [] for k in range(len(slots) + LATE)}
    tasks[4].append(functools.partial(pass_on, 0))
    tasks[6].append(one_done)
    tasks[7].append(functools.partial(pass_on, 1))
    tasks[9].append(two_done)
    for c in range(count):
        tasks[place_of[c, order[-1]] + LATE].append(functools.partial(finish_chunk, c))
    tasks[place_of[count - 3, order[-1]] + LATE].append(
        lambda: sums.append(gather_small(threes, met_three, 2))
    )
    for f in range(field_count - 1):
        near_end = count - field_count + 1 + f
        tasks[place_of[near_end - 1, order[-1]] + LATE].append(functools.partial(lambda f: along(f, sums[0]), f))
    sent_at = {slot: k + 1 for k, slot in enumerate(slots[:LEAD])}
    arrived = set()

    def await_arrival(slot):
        if slot[1] and slot not in arrived:
            arrived.add(slot)
            out_arrival(*slot).wait_recv()

    reached = LEAD
    for k in range(LEAD, len(slots) + LATE):
        if k < len(slots):
            await_arrival(slots[k])
            for side in range(2):
                pl.when(inner[side])(lambda k=k, side=side: halo_copy(*slots[k - LEAD], side).wait_send())
            start_halo(*slots[k])
            until = min(len(slots), LEAD + -(-(k - LEAD + 1) * RING // (RING - 1)))
            for slot in slots[reached:until]:
                await_arrival(slot)
                start_edge(*slot)
                sent_at[slot] = k
            reached = until
        for slot in slots:
            if slot[1] in RELAYED and sent_at.get(slot, k) + HOPS == k:
                pass_along(*slot)
        for task in tasks[k]:
            task()

    along(field_count - 1, sums[0])
    for d in near:
        @pl.when(inside(d))
        def _(d=d):
            for copy in meta_copies(d):
                copy.wait_send()
    for copy in ones + twos + threes:
        copy.wait_send()
    for c in range(count):
        for dy in order:
            out_copy(c, dy).wait_send()
            back_copy(c, dy).wait_send()
    for k, slot in enumerate(slots):
        for side in range(2):
            if k >= len(slots) - LEAD:
                pl.when(inner[side])(lambda slot=slot, side=side: halo_copy(*slot, side).wait_send())
            pl.when(edge[side])(lambda slot=slot, side=side: halo_copy(*slot, side).wait_send())
        if slot[1] in RELAYED:
            passed_along(*slot)


def exchange(lat_t, lon_t, shift, departure_row, extents, area, fields):
    bands, levs = lax.axis_size("lat"), lax.axis_size("lev")
    rows, field_count, levels, lon_count = fields.shape
    crosses = bands // RING // DEEP
    piece = lon_count // RING
    tile = (8, LANES)
    dma = pltpu.SemaphoreType.DMA
    ones = RING * levs - 1
    near = 2 * REACH
    chunks = chunks_of(field_count, piece // LANES)
    count = len(chunks)
    return pl.pallas_call(
        functools.partial(exchange_kernel, bands, levs),
        out_shape=pltpu.VMEM(fields.shape, fields.dtype),
        in_specs=[pl.BlockSpec(memory_space=pltpu.SMEM)] * 6 + [pl.BlockSpec(memory_space=pl.ANY)],
        out_specs=pl.BlockSpec(memory_space=pltpu.VMEM),
        scratch_shapes=[
            pltpu.VMEM(fields.shape, jnp.float32),
            pltpu.VMEM(fields.shape, jnp.float32),
            *[pltpu.VMEM((3 * RING * rows, levels, width), jnp.float32) for _, _, width in chunks],
            *[pltpu.VMEM((RING * rows, levels, width), jnp.float32) for _, _, width in chunks],
            *[pltpu.VMEM((len(RELAYED) * rows, levels, width), jnp.float32) for _, _, width in chunks],
            pltpu.VMEM((near + 1,) + tile, jnp.float32),
            pltpu.VMEM((near + 1,) + tile, jnp.int32),
            pltpu.SMEM((RING,) + tile, jnp.float32),
            pltpu.SMEM((RING,) + tile, jnp.int32),
            pltpu.VMEM((3,) + tile, jnp.float32),
            pltpu.VMEM((ones,) + tile, jnp.float32),
            pltpu.VMEM((max(crosses - 1, 1),) + tile, jnp.float32),
            pltpu.VMEM((DEEP - 1,) + tile, jnp.float32),
            dma,
            dma((2, count)),
            dma((2,)),
            dma((2, near)),
            dma((2, near)),
            dma((count, RING - 1)),
            dma((count, RING - 1)),
            dma((2, count, RING)),
            dma((2, count, RING)),
            dma((count, RING - 1)),
            dma((count, RING - 1)),
            dma((ones,)),
            dma((ones,)),
            dma((max(crosses - 1, 1),)),
            dma((max(crosses - 1, 1),)),
            dma((DEEP - 1,)),
            dma((DEEP - 1,)),
            pltpu.SemaphoreType.REGULAR((3,)),
            dma((count, len(RELAYED))),
            dma((count, len(RELAYED))),
        ],
        compiler_params=pltpu.CompilerParams(
            collective_id=0, has_side_effects=True, vmem_limit_bytes=60000 * 1024
        ),
        name="exchange",
    )(lat_t, lon_t, shift, departure_row, extents, area, fields)


def per_device(fields, lat_fraction, lon_fraction, lon_shift, departure_row, extents):
    bands = lax.axis_size("lat")
    total_rows = bands * fields.shape[0]
    row_ids = np.arange(total_rows)
    area = jnp.asarray(np.cos(math.pi * (row_ids + 0.5) / total_rows - math.pi / 2.0), jnp.float32)
    return exchange(lat_fraction, lon_fraction, lon_shift, departure_row, extents, area, fields)


def solution(mesh):
    return jax.shard_map(
        per_device,
        mesh=mesh,
        in_specs=(
            P("lat", None, "lev", None),
            P("lat"),
            P("lat"),
            P("lat"),
            P("lat"),
            P("lat", None),
        ),
        out_specs=P("lat", None, "lev", None),
        check_vma=False,
    )
```

```python
import functools
import math

import jax
import jax.numpy as jnp
import numpy as np
from jax import lax
from jax.experimental import pallas as pl
from jax.experimental.pallas import tpu as pltpu
from jax.sharding import PartitionSpec as P

REACH = 4
LANES = 128
RING = 4
DEEP = 8
MESH = pl.DeviceIdType.MESH
CUTS = ((5,), (3, 2), (3, 2))
LEAD = 3
HOPS = 2
RELAYED = (0, 1, RING - 1)
LATE = 3
EARLIER = 0
TOGETHER = 2
TAIL = 2


def chunks_of(field_count, tiles):
    found = []
    for f in range(field_count):
        cuts = CUTS[f] if f < len(CUTS) and sum(CUTS[f]) == tiles else (tiles,)
        first = 0
        for width in cuts:
            found.append((f, first * LANES, width * LANES))
            first += width
    return found


def cubic(t):
    sixth = 1.0 / 6.0
    return (
        -t * (t - 1.0) * (t - 2.0) * sixth,
        (t + 1.0) * (t - 1.0) * (t - 2.0) * 0.5,
        -(t + 1.0) * t * (t - 2.0) * 0.5,
        (t + 1.0) * t * (t - 1.0) * sixth,
    )


def departure_of(row, first_row, rows, total_rows, departure_ref, extents_ref):
    low = first_row - extents_ref[0, 0] * rows + 1
    high = first_row + rows - 3 + extents_ref[0, 1] * rows
    inside = jnp.minimum(jnp.maximum(departure_ref[row], low), high)
    return jnp.minimum(jnp.maximum(inside, 1), total_rows - 3)


def exchange_kernel(bands, levs, lat_t_ref, lon_t_ref, shift_ref, departure_ref, extents_ref, area_ref, fields_ref,
                    out_ref, *scratch):
    rows, field_count, _, lon_count = fields_ref.shape
    piece = lon_count // RING
    chunks = chunks_of(field_count, piece // LANES)
    count = len(chunks)
    held, landed = scratch[:2]
    window = scratch[2:2 + count]
    column = scratch[2 + count:2 + 2 * count]
    passing = scratch[2 + 2 * count:2 + 3 * count]
    (real_meta, whole_meta, real_smem, whole_smem, part, met_one, met_two, met_three,
     load_sem, own_sem, smem_sem, meta_send, meta_recv, out_send, out_recv, halo_send, halo_recv,
     back_send, back_recv, one_send, one_recv, two_send, two_recv, three_send, three_recv,
     round_sem, pass_send, pass_recv) = scratch[2 + 3 * count:]
    band, lev = lax.axis_index("lat"), lax.axis_index("lev")
    group, member = band // RING, lax.rem(band, RING)
    groups = bands // RING
    crosses = groups // DEEP
    deep, cross = lax.rem(group, DEEP), group // DEEP
    first_row, total_rows = band * rows, bands * rows
    span = RING * rows

    def ring_member(step):
        return lax.rem(member + step, RING)

    def ring_peer(step):
        return group * RING + ring_member(step)

    def inside(distance):
        place = band + distance
        return jnp.logical_and(place >= 0, place < bands)

    near = [d for d in range(-REACH, REACH + 1) if d != 0]
    one_peers = [(dy, dl) for dy in range(RING) for dl in range(levs) if (dy, dl) != (0, 0)]

    def one_peer(dy, dl):
        return {"lat": ring_peer(dy), "lev": lax.rem(lev + dl, levs)}

    def two_peer(dx):
        return {"lat": (lax.rem(cross + dx, crosses) * DEEP + deep) * RING + member}

    def three_peer(dz):
        return {"lat": (cross * DEEP + lax.rem(deep + dz, DEEP)) * RING + member}

    barrier = pltpu.get_barrier_semaphore()

    def greet(peer):
        pl.semaphore_signal(barrier, inc=1, device_id=peer, device_id_type=MESH)

    for d in near:
        pl.when(inside(d))(functools.partial(greet, {"lat": band + d}))
    for dy, dl in one_peers:
        if dl:
            greet(one_peer(dy, dl))
    for step in (1, crosses - 1):
        greet(two_peer(step))
    for step in (1, DEEP - 1):
        greet(three_peer(step))

    load = pltpu.make_async_copy(fields_ref, held, load_sem)
    load.start()

    def cut(c, place):
        f, first, width = chunks[c]
        return (slice(None), f, slice(None), pl.ds(pl.multiple_of(place * piece + first, LANES), width))

    own_pieces = [
        pltpu.make_async_copy(
            fields_ref.at[cut(c, member)], window[c].at[pl.ds(span + member * rows, rows)], own_sem.at[0, c]
        )
        for c in range(count)
    ]
    for copy in own_pieces:
        copy.start()

    lane = lax.broadcasted_iota(jnp.int32, (1, LANES), 1)
    lat_t = jnp.zeros((1, LANES), jnp.float32)
    lon_t = jnp.zeros((1, LANES), jnp.float32)
    area = jnp.zeros((1, LANES), jnp.float32)
    start = jnp.zeros((1, LANES), jnp.int32)
    for row in range(rows):
        here = lane == row
        lat_t = jnp.where(here, lat_t_ref[row], lat_t)
        lon_t = jnp.where(here, lon_t_ref[row], lon_t)
        area = jnp.where(here, area_ref[first_row + row], area)
        departure = departure_of(row, first_row, rows, total_rows, departure_ref, extents_ref)
        start = jnp.where(here, departure - 1, start)
    lon_w = cubic(lon_t)
    for d in near:
        @pl.when(jnp.logical_not(inside(d)))
        def _(d=d):
            real_meta[REACH + d] = jnp.zeros(real_meta.shape[1:], jnp.float32)
            whole_meta[REACH + d] = jnp.zeros(whole_meta.shape[1:], jnp.int32)
    real_meta[REACH] = jnp.concatenate(
        [*cubic(lat_t), area * (lon_w[0] + lon_w[1] + lon_w[2] + lon_w[3]), jnp.zeros((3, LANES), jnp.float32)], axis=0
    )
    whole_meta[REACH] = jnp.broadcast_to(start, whole_meta.shape[1:])

    expected = sum(dl != 0 for _, dl in one_peers) + 4
    for d in near:
        expected = expected + inside(d).astype(jnp.int32)
    pl.semaphore_wait(barrier, expected)

    def tell(n):
        for step in (1, DEEP - 1):
            pl.semaphore_signal(round_sem.at[n], inc=1, device_id=three_peer(step), device_id_type=MESH)
        if n == 0:
            for step in (1, crosses - 1):
                pl.semaphore_signal(round_sem.at[n], inc=1, device_id=two_peer(step), device_id_type=MESH)

    def hear(n):
        pl.semaphore_wait(round_sem.at[n], 4 if n == 0 else 2)

    tell(0)

    def meta_copies(d):
        k = near.index(d)
        return [
            pltpu.make_async_remote_copy(
                src_ref=ref.at[REACH], dst_ref=ref.at[REACH - d],
                send_sem=meta_send.at[n, k], recv_sem=meta_recv.at[n, near.index(-d)],
                device_id={"lat": band + d}, device_id_type=MESH,
            )
            for n, ref in enumerate((real_meta, whole_meta))
        ]

    def meta_arrivals(d):
        k = near.index(d)
        return [
            pltpu.make_async_remote_copy(
                src_ref=ref.at[REACH + d], dst_ref=ref.at[REACH + d],
                send_sem=meta_send.at[n, k], recv_sem=meta_recv.at[n, k],
                device_id={"lat": band + d}, device_id_type=MESH,
            )
            for n, ref in enumerate((real_meta, whole_meta))
        ]

    for d in near:
        @pl.when(inside(d))
        def _(d=d):
            for copy in meta_copies(d):
                copy.start()

    def out_copy(c, dy):
        return pltpu.make_async_remote_copy(
            src_ref=fields_ref.at[cut(c, ring_member(dy))],
            dst_ref=window[c].at[pl.ds(span + member * rows, rows)],
            send_sem=out_send.at[c, dy - 1], recv_sem=out_recv.at[c, dy - 1],
            device_id={"lat": ring_peer(dy)}, device_id_type=MESH,
        )

    def out_arrival(c, dy):
        place = window[c].at[pl.ds(span + ring_member(RING - dy) * rows, rows)]
        return pltpu.make_async_remote_copy(
            src_ref=place, dst_ref=place, send_sem=out_send.at[c, dy - 1], recv_sem=out_recv.at[c, dy - 1],
            device_id={"lat": ring_peer(RING - dy)}, device_id_type=MESH,
        )

    has_side = (group < groups - 1, group > 0)

    def halo_place(c, dy, side):
        return window[c].at[pl.ds((0 if side == 0 else 2 * span) + ring_member(RING - dy) * rows, rows)]

    def halo_source(c, dy):
        if dy == 0:
            return fields_ref.at[cut(c, member)]
        return window[c].at[pl.ds(span + ring_member(RING - dy) * rows, rows)]

    def halo_copy(c, dy, side):
        return pltpu.make_async_remote_copy(
            src_ref=halo_source(c, dy), dst_ref=halo_place(c, dy, side),
            send_sem=halo_send.at[side, c, dy], recv_sem=halo_recv.at[side, c, dy],
            device_id={"lat": band + (RING if side == 0 else -RING)}, device_id_type=MESH,
        )

    edge = (jnp.logical_and(has_side[0], deep == DEEP - 1), jnp.logical_and(has_side[1], deep == 0))
    inner = tuple(jnp.logical_and(h, jnp.logical_not(e)) for h, e in zip(has_side, edge))
    shared = (cross + 1, crosses - cross)
    serves = (
        (jnp.logical_and(deep == DEEP - 1, cross > 0), cross),
        (jnp.logical_and(deep == 0, cross < crosses - 1), crosses - 1 - cross),
    )

    def pass_place(c, rank):
        return passing[c].at[pl.ds(rank * rows, rows)]

    def to_relay(c, dy, side):
        rank = RELAYED.index(dy)
        return pltpu.make_async_remote_copy(
            src_ref=halo_source(c, dy), dst_ref=pass_place(c, rank),
            send_sem=halo_send.at[side, c, dy], recv_sem=pass_recv.at[c, rank],
            device_id=two_peer(1 if side == 0 else crosses - 1), device_id_type=MESH,
        )

    def from_relay(c, dy, side):
        rank = RELAYED.index(dy)
        return pltpu.make_async_remote_copy(
            src_ref=pass_place(c, rank), dst_ref=halo_place(c, dy, side),
            send_sem=pass_send.at[c, rank], recv_sem=halo_recv.at[side, c, dy],
            device_id=three_peer(1 if side == 0 else DEEP - 1), device_id_type=MESH,
        )

    def at_relay(c, dy):
        rank = RELAYED.index(dy)
        place = pass_place(c, rank)
        return pltpu.make_async_remote_copy(
            src_ref=place, dst_ref=place, send_sem=pass_send.at[c, rank], recv_sem=pass_recv.at[c, rank],
            device_id=two_peer(1), device_id_type=MESH,
        )

    def start_edge(c, dy):
        for side in range(2):
            if dy in RELAYED:
                relayed = RELAYED.index(dy) < shared[side]
                pl.when(jnp.logical_and(edge[side], relayed))(lambda side=side: to_relay(c, dy, side).start())
                pl.when(jnp.logical_and(edge[side], jnp.logical_not(relayed)))(
                    lambda side=side: halo_copy(c, dy, side).start()
                )
            else:
                pl.when(edge[side])(lambda side=side: halo_copy(c, dy, side).start())

    def pass_along(c, dy):
        for side in range(2):
            serving, limit = serves[side]

            @pl.when(jnp.logical_and(serving, RELAYED.index(dy) < limit))
            def _(side=side):
                at_relay(c, dy).wait_recv()
                from_relay(c, dy, side).start()

    def passed_along(c, dy):
        for side in range(2):
            serving, limit = serves[side]
            pl.when(jnp.logical_and(serving, RELAYED.index(dy) < limit))(
                lambda side=side: from_relay(c, dy, side).wait_send()
            )

    def halo_arrival(c, dy, side):
        place = halo_place(c, dy, side)
        return pltpu.make_async_remote_copy(
            src_ref=place, dst_ref=place, send_sem=halo_send.at[side, c, dy], recv_sem=halo_recv.at[side, c, dy],
            device_id={"lat": band + (-RING if side == 0 else RING)}, device_id_type=MESH,
        )

    def start_halo(c, dy):
        for side in range(2):
            pl.when(inner[side])(lambda side=side: halo_copy(c, dy, side).start())

    def groups_of(c):
        parts = TAIL if c == count - 1 and rows % TAIL == 0 else 1
        return [(n, n * rows // parts, rows // parts) for n in range(parts)]

    def landing(c, place, first, height):
        f, begin, width = chunks[c]
        at = pl.ds(pl.multiple_of(place * piece + begin, LANES), width)
        return landed.at[pl.ds(first, height), f, :, at]

    def back_copy(c, dy, n, first, height):
        return pltpu.make_async_remote_copy(
            src_ref=column[c].at[pl.ds(dy * rows + first, height)], dst_ref=landing(c, member, first, height),
            send_sem=back_send.at[c, dy - 1, n], recv_sem=back_recv.at[c, dy - 1, n],
            device_id={"lat": ring_peer(dy)}, device_id_type=MESH,
        )

    def back_arrival(c, dy, n, first, height):
        place = landing(c, ring_member(RING - dy), first, height)
        return pltpu.make_async_remote_copy(
            src_ref=place, dst_ref=place, send_sem=back_send.at[c, dy - 1, n], recv_sem=back_recv.at[c, dy - 1, n],
            device_id={"lat": ring_peer(RING - dy)}, device_id_type=MESH,
        )

    def back_own(c):
        return pltpu.make_async_copy(column[c].at[pl.ds(0, rows)], landing(c, member, 0, rows), own_sem.at[1, c])

    def small_copy(source, target, sends, arrivals, k, peer):
        return pltpu.make_async_remote_copy(
            src_ref=source, dst_ref=target.at[k], send_sem=sends.at[k], recv_sem=arrivals.at[k],
            device_id=peer, device_id_type=MESH,
        )

    ones = [small_copy(part.at[0], met_one, one_send, one_recv, k, one_peer(*p)) for k, p in enumerate(one_peers)]
    twos = [small_copy(part.at[1], met_two, two_send, two_recv, dx - 1, two_peer(dx)) for dx in range(1, crosses)]
    threes = [small_copy(part.at[2], met_three, three_send, three_recv, dz - 1, three_peer(dz)) for dz in range(1, DEEP)]

    order = (1, RING - 1, *range(2, RING - 1))
    slots = [(c, 0) for c in range(min(LEAD, count))]
    for c in range(count):
        slots += [(c, dy) for dy in order] + [(c + LEAD, 0)] * (c + LEAD < count)
    place_of = {slot: k for k, slot in enumerate(slots)}
    start_halo(*slots[0])
    start_edge(*slots[0])
    for c in range(min(2, count)):
        for dy in order:
            out_copy(c, dy).start()
    for slot in slots[1:LEAD]:
        start_halo(*slot)
        start_edge(*slot)

    for d in near:
        @pl.when(inside(d))
        def _(d=d):
            for copy in meta_arrivals(d):
                copy.wait_recv()
    group_slots = pl.ds(REACH - member, RING)
    to_smem = [
        pltpu.make_async_copy(real_meta.at[group_slots], real_smem, smem_sem.at[0]),
        pltpu.make_async_copy(whole_meta.at[group_slots], whole_smem, smem_sem.at[1]),
    ]
    for copy in to_smem:
        copy.start()
    load.wait()

    def add_row(row, totals):
        taken = jnp.zeros((2 * REACH + 1, LANES), jnp.float32)
        for a in range(4):
            hit = whole_meta[:, 0, :] + a == first_row + row
            taken = taken + jnp.where(hit, real_meta[:, a, :] * real_meta[:, 4, :], 0.0)
        taken = jnp.sum(jnp.sum(taken, axis=0, keepdims=True), axis=1, keepdims=True)
        row_area = area_ref[first_row + row]
        before, after = [], []
        for f in range(field_count):
            tile = held[row, f, :, 0:LANES]
            for t in range(1, lon_count // LANES):
                tile = tile + held[row, f, :, t * LANES:(t + 1) * LANES]
            total = jnp.sum(tile, axis=0, keepdims=True)
            before.append(totals[f] + row_area * total)
            after.append(totals[field_count + f] + taken * total)
        return tuple(before + after)

    zero = jnp.zeros((1, LANES), jnp.float32)
    totals = lax.fori_loop(0, rows, add_row, (zero,) * (2 * field_count))
    part[0] = jnp.concatenate([*totals, jnp.zeros((8 - 2 * field_count, LANES), jnp.float32)], axis=0)

    def gather_small(copies, target, level):
        for copy in copies:
            copy.wait_recv()
        total = part[level]
        for k in range(len(copies)):
            total = total + target[k]
        return total

    for copy in ones:
        copy.start()
    for c in range(min(2, count), count):
        for dy in order:
            out_copy(c, dy).start()

    base = (group - 1) * span

    def interpolate(c, dy, first, height):
        to = ring_member(dy)

        def one_row(row, carry):
            place = whole_smem[to, 0, row] - base
            weight = [real_smem[to, a, row] for a in range(4)]
            for t in range(chunks[c][2] // LANES):
                at = pl.ds(t * LANES, LANES)
                total = weight[0] * window[c][place, :, at]
                for a in range(1, 4):
                    total = total + weight[a] * window[c][place + a, :, at]
                column[c][dy * rows + row, :, at] = total
            return carry

        lax.fori_loop(first, first + height, one_row, 0)

    def finish_chunk(c):
        if c == 0:
            for copy in to_smem:
                copy.wait()
        own_pieces[c].wait()
        for dy in (0, *order):
            for side in range(2):
                pl.when(has_side[1 - side])(lambda dy=dy, side=side: halo_arrival(c, dy, side).wait_recv())
        for n, first, height in groups_of(c):
            for dy in (2, 1, RING - 1, 0):
                interpolate(c, dy, first, height)
            for dy in (2, 1, RING - 1):
                back_copy(c, dy, n, first, height).start()
        back_own(c).start()

    def one_done():
        part[1] = gather_small(ones, met_one, 0)
        for copy in twos:
            copy.start()

    def two_done():
        part[2] = gather_small(twos, met_two, 1)
        hear(2)
        for copy in threes:
            copy.start()

    def pass_on(n):
        hear(n)
        tell(n + 1)

    lanes = lax.broadcasted_iota(jnp.int32, fields_ref.shape[2:3] + (LANES,), 1)
    tiles = lon_count // LANES

    def shifted(pieces, step):
        turned = [pltpu.roll(piece, LANES - step, 1) for piece in pieces]
        return [jnp.where(lanes < LANES - step, turned[t], turned[(t + 1) % tiles]) for t in range(tiles)]

    def along(f, sums):
        before = jnp.sum(sums[f:f + 1], axis=1, keepdims=True)
        after = jnp.sum(sums[field_count + f:field_count + f + 1], axis=1, keepdims=True)
        ratio = before / after

        def some_rows(together, step, carry):
            for n in range(together):
                row = step * together + n
                lon = [weight * ratio for weight in cubic(lon_t_ref[row])]
                here = [landed[row, f, :, t * LANES:(t + 1) * LANES] for t in range(tiles)]
                after = shifted(here, 1)
                later = shifted([lon[2] * here[t] + lon[3] * after[t] for t in range(tiles)], 2)
                moved = []
                for t in range(tiles):
                    mixed = lon[0] * here[t] + lon[1] * after[t] + later[t]
                    moved.append(mixed)
                first = lax.rem(shift_ref[row] - 1 + lon_count, lon_count)
                ahead = jnp.full(lanes.shape, first, jnp.int32)
                step_by = LANES
                while step_by < lon_count:
                    jump = (ahead & step_by) != 0
                    moved = [jnp.where(jump, moved[(t + step_by // LANES) % tiles], moved[t]) for t in range(tiles)]
                    step_by *= 2
                rest = ahead & (LANES - 1)
                pick = (lanes + rest) & (LANES - 1)
                moved = [jnp.take_along_axis(part_of, pick, axis=1) for part_of in moved]
                keep = lanes + rest < LANES
                for t in range(tiles):
                    out_ref[row, f, :, t * LANES:(t + 1) * LANES] = jnp.where(keep, moved[t], moved[(t + 1) % tiles])
            return carry

        mine = [c for c in range(count) if chunks[c][0] == f]
        for c in mine:
            back_own(c).wait()
            if c != mine[-1]:
                for dy in order:
                    for group_of in groups_of(c):
                        back_arrival(c, dy, *group_of).wait_recv()
        for group_of in groups_of(mine[-1]):
            for dy in order:
                back_arrival(mine[-1], dy, *group_of).wait_recv()
            _, first_of, height = group_of
            together = TOGETHER if height % TOGETHER == 0 and first_of % TOGETHER == 0 else height
            lax.fori_loop(
                first_of // together, (first_of + height) // together, functools.partial(some_rows, together), 0
            )

    sums = []
    tasks = {k: [] for k in range(len(slots) + LATE)}
    tasks[4].append(functools.partial(pass_on, 0))
    tasks[6].append(one_done)
    tasks[7].append(functools.partial(pass_on, 1))
    tasks[9].append(two_done)
    for c in range(count):
        tasks[place_of[c, order[-1]] + LATE].append(functools.partial(finish_chunk, c))
    tasks[place_of[count - 3 - EARLIER, order[-1]] + LATE].append(
        lambda: sums.append(gather_small(threes, met_three, 2))
    )
    for f in range(field_count - 1):
        near_end = count - field_count + 1 + f - EARLIER
        tasks[place_of[near_end - 1, order[-1]] + LATE].append(functools.partial(lambda f: along(f, sums[0]), f))
    sent_at = {slot: k + 1 for k, slot in enumerate(slots[:LEAD])}
    arrived = set()

    def await_arrival(slot):
        if slot[1] and slot not in arrived:
            arrived.add(slot)
            out_arrival(*slot).wait_recv()

    reached = LEAD
    for k in range(LEAD, len(slots) + LATE):
        if k < len(slots):
            await_arrival(slots[k])
            for side in range(2):
                pl.when(inner[side])(lambda k=k, side=side: halo_copy(*slots[k - LEAD], side).wait_send())
            start_halo(*slots[k])
            until = min(len(slots), LEAD + -(-(k - LEAD + 1) * RING // (RING - 1)))
            for slot in slots[reached:until]:
                await_arrival(slot)
                start_edge(*slot)
                sent_at[slot] = k
            reached = until
        for slot in slots:
            if slot[1] in RELAYED and slot in sent_at and max(sent_at[slot] + HOPS, LEAD) == k:
                pass_along(*slot)
        for task in tasks[k]:
            task()

    along(field_count - 1, sums[0])
    for d in near:
        @pl.when(inside(d))
        def _(d=d):
            for copy in meta_copies(d):
                copy.wait_send()
    for copy in ones + twos + threes:
        copy.wait_send()
    for c in range(count):
        for dy in order:
            out_copy(c, dy).wait_send()
            for group_of in groups_of(c):
                back_copy(c, dy, *group_of).wait_send()
    for k, slot in enumerate(slots):
        for side in range(2):
            if k >= len(slots) - LEAD:
                pl.when(inner[side])(lambda slot=slot, side=side: halo_copy(*slot, side).wait_send())
            pl.when(edge[side])(lambda slot=slot, side=side: halo_copy(*slot, side).wait_send())
        if slot[1] in RELAYED:
            passed_along(*slot)


def exchange(lat_t, lon_t, shift, departure_row, extents, area, fields):
    bands, levs = lax.axis_size("lat"), lax.axis_size("lev")
    rows, field_count, levels, lon_count = fields.shape
    crosses = bands // RING // DEEP
    piece = lon_count // RING
    tile = (8, LANES)
    dma = pltpu.SemaphoreType.DMA
    ones = RING * levs - 1
    near = 2 * REACH
    chunks = chunks_of(field_count, piece // LANES)
    count = len(chunks)
    return pl.pallas_call(
        functools.partial(exchange_kernel, bands, levs),
        out_shape=pltpu.VMEM(fields.shape, fields.dtype),
        in_specs=[pl.BlockSpec(memory_space=pltpu.SMEM)] * 6 + [pl.BlockSpec(memory_space=pl.ANY)],
        out_specs=pl.BlockSpec(memory_space=pltpu.VMEM),
        scratch_shapes=[
            pltpu.VMEM(fields.shape, jnp.float32),
            pltpu.VMEM(fields.shape, jnp.float32),
            *[pltpu.VMEM((3 * RING * rows, levels, width), jnp.float32) for _, _, width in chunks],
            *[pltpu.VMEM((RING * rows, levels, width), jnp.float32) for _, _, width in chunks],
            *[pltpu.VMEM((len(RELAYED) * rows, levels, width), jnp.float32) for _, _, width in chunks],
            pltpu.VMEM((near + 1,) + tile, jnp.float32),
            pltpu.VMEM((near + 1,) + tile, jnp.int32),
            pltpu.SMEM((RING,) + tile, jnp.float32),
            pltpu.SMEM((RING,) + tile, jnp.int32),
            pltpu.VMEM((3,) + tile, jnp.float32),
            pltpu.VMEM((ones,) + tile, jnp.float32),
            pltpu.VMEM((max(crosses - 1, 1),) + tile, jnp.float32),
            pltpu.VMEM((DEEP - 1,) + tile, jnp.float32),
            dma,
            dma((2, count)),
            dma((2,)),
            dma((2, near)),
            dma((2, near)),
            dma((count, RING - 1)),
            dma((count, RING - 1)),
            dma((2, count, RING)),
            dma((2, count, RING)),
            dma((count, RING - 1, TAIL)),
            dma((count, RING - 1, TAIL)),
            dma((ones,)),
            dma((ones,)),
            dma((max(crosses - 1, 1),)),
            dma((max(crosses - 1, 1),)),
            dma((DEEP - 1,)),
            dma((DEEP - 1,)),
            pltpu.SemaphoreType.REGULAR((3,)),
            dma((count, len(RELAYED))),
            dma((count, len(RELAYED))),
        ],
        compiler_params=pltpu.CompilerParams(
            collective_id=0, has_side_effects=True, vmem_limit_bytes=60000 * 1024
        ),
        name="exchange",
    )(lat_t, lon_t, shift, departure_row, extents, area, fields)


def per_device(fields, lat_fraction, lon_fraction, lon_shift, departure_row, extents):
    bands = lax.axis_size("lat")
    total_rows = bands * fields.shape[0]
    row_ids = np.arange(total_rows)
    area = jnp.asarray(np.cos(math.pi * (row_ids + 0.5) / total_rows - math.pi / 2.0), jnp.float32)
    return exchange(lat_fraction, lon_fraction, lon_shift, departure_row, extents, area, fields)


def solution(mesh):
    return jax.shard_map(
        per_device,
        mesh=mesh,
        in_specs=(
            P("lat", None, "lev", None),
            P("lat"),
            P("lat"),
            P("lat"),
            P("lat"),
            P("lat", None),
        ),
        out_specs=P("lat", None, "lev", None),
        check_vma=False,
    )
```

```python
import functools
import math

import jax
import jax.numpy as jnp
import numpy as np
from jax import lax
from jax.experimental import pallas as pl
from jax.experimental.pallas import tpu as pltpu
from jax.sharding import PartitionSpec as P

REACH = 4
LANES = 128
RING = 4
DEEP = 8
MESH = pl.DeviceIdType.MESH
CUTS = ((5,), (3, 2), (3, 2))
LEAD = 3
HOPS = 2
RELAYED = (0, 1, RING - 1)
LATE = 4
EARLIER = 0
TOGETHER = 2
TAIL = 2


def chunks_of(field_count, tiles):
    found = []
    for f in range(field_count):
        cuts = CUTS[f] if f < len(CUTS) and sum(CUTS[f]) == tiles else (tiles,)
        first = 0
        for width in cuts:
            found.append((f, first * LANES, width * LANES))
            first += width
    return found


def cubic(t):
    sixth = 1.0 / 6.0
    return (
        -t * (t - 1.0) * (t - 2.0) * sixth,
        (t + 1.0) * (t - 1.0) * (t - 2.0) * 0.5,
        -(t + 1.0) * t * (t - 2.0) * 0.5,
        (t + 1.0) * t * (t - 1.0) * sixth,
    )


def departure_of(row, first_row, rows, total_rows, departure_ref, extents_ref):
    low = first_row - extents_ref[0, 0] * rows + 1
    high = first_row + rows - 3 + extents_ref[0, 1] * rows
    inside = jnp.minimum(jnp.maximum(departure_ref[row], low), high)
    return jnp.minimum(jnp.maximum(inside, 1), total_rows - 3)


def exchange_kernel(bands, levs, lat_t_ref, lon_t_ref, shift_ref, departure_ref, extents_ref, area_ref, fields_ref,
                    out_ref, *scratch):
    rows, field_count, _, lon_count = fields_ref.shape
    piece = lon_count // RING
    chunks = chunks_of(field_count, piece // LANES)
    count = len(chunks)
    held, landed = scratch[:2]
    window = scratch[2:2 + count]
    column = scratch[2 + count:2 + 2 * count]
    passing = scratch[2 + 2 * count:2 + 3 * count]
    (real_meta, whole_meta, real_smem, whole_smem, part, met_one, met_two, met_three,
     load_sem, own_sem, smem_sem, meta_send, meta_recv, out_send, out_recv, halo_send, halo_recv,
     back_send, back_recv, one_send, one_recv, two_send, two_recv, three_send, three_recv,
     round_sem, pass_send, pass_recv) = scratch[2 + 3 * count:]
    band, lev = lax.axis_index("lat"), lax.axis_index("lev")
    group, member = band // RING, lax.rem(band, RING)
    groups = bands // RING
    crosses = groups // DEEP
    deep, cross = lax.rem(group, DEEP), group // DEEP
    first_row, total_rows = band * rows, bands * rows
    span = RING * rows

    def ring_member(step):
        return lax.rem(member + step, RING)

    def ring_peer(step):
        return group * RING + ring_member(step)

    def inside(distance):
        place = band + distance
        return jnp.logical_and(place >= 0, place < bands)

    near = [d for d in range(-REACH, REACH + 1) if d != 0]
    one_peers = [(dy, dl) for dy in range(RING) for dl in range(levs) if (dy, dl) != (0, 0)]

    def one_peer(dy, dl):
        return {"lat": ring_peer(dy), "lev": lax.rem(lev + dl, levs)}

    def two_peer(dx):
        return {"lat": (lax.rem(cross + dx, crosses) * DEEP + deep) * RING + member}

    def three_peer(dz):
        return {"lat": (cross * DEEP + lax.rem(deep + dz, DEEP)) * RING + member}

    barrier = pltpu.get_barrier_semaphore()

    def greet(peer):
        pl.semaphore_signal(barrier, inc=1, device_id=peer, device_id_type=MESH)

    bottom, top = deep == 0, deep == DEEP - 1

    def late(d):
        return jnp.logical_and(inside(d), jnp.logical_and(bottom, member + d < 0))

    def early(d):
        return jnp.logical_and(inside(d), jnp.logical_and(top, member + d >= RING))

    def prompt(d):
        return jnp.logical_and(inside(d), jnp.logical_not(late(d) if d < 0 else early(d)))

    for d in near:
        pl.when(prompt(d))(functools.partial(greet, {"lat": band + d}))
    for dy, dl in one_peers:
        if dl:
            greet(one_peer(dy, dl))
    for step in (1, crosses - 1):
        greet(two_peer(step))
    pl.when(jnp.logical_not(top))(lambda: greet(three_peer(1)))
    pl.when(jnp.logical_not(bottom))(lambda: greet(three_peer(DEEP - 1)))

    load = pltpu.make_async_copy(fields_ref, held, load_sem)
    load.start()

    def cut(c, place):
        f, first, width = chunks[c]
        return (slice(None), f, slice(None), pl.ds(pl.multiple_of(place * piece + first, LANES), width))

    own_pieces = [
        pltpu.make_async_copy(
            fields_ref.at[cut(c, member)], window[c].at[pl.ds(span + member * rows, rows)], own_sem.at[0, c]
        )
        for c in range(count)
    ]
    for copy in own_pieces:
        copy.start()

    lane = lax.broadcasted_iota(jnp.int32, (1, LANES), 1)
    lat_t = jnp.zeros((1, LANES), jnp.float32)
    lon_t = jnp.zeros((1, LANES), jnp.float32)
    area = jnp.zeros((1, LANES), jnp.float32)
    start = jnp.zeros((1, LANES), jnp.int32)
    for row in range(rows):
        here = lane == row
        lat_t = jnp.where(here, lat_t_ref[row], lat_t)
        lon_t = jnp.where(here, lon_t_ref[row], lon_t)
        area = jnp.where(here, area_ref[first_row + row], area)
        departure = departure_of(row, first_row, rows, total_rows, departure_ref, extents_ref)
        start = jnp.where(here, departure - 1, start)
    lon_w = cubic(lon_t)
    for d in near:
        @pl.when(jnp.logical_not(inside(d)))
        def _(d=d):
            real_meta[REACH + d] = jnp.zeros(real_meta.shape[1:], jnp.float32)
            whole_meta[REACH + d] = jnp.zeros(whole_meta.shape[1:], jnp.int32)
    real_meta[REACH] = jnp.concatenate(
        [*cubic(lat_t), area * (lon_w[0] + lon_w[1] + lon_w[2] + lon_w[3]), jnp.zeros((3, LANES), jnp.float32)], axis=0
    )
    whole_meta[REACH] = jnp.broadcast_to(start, whole_meta.shape[1:])

    expected = sum(dl != 0 for _, dl in one_peers) + 3 + jnp.logical_not(bottom).astype(jnp.int32)
    awaited = 1
    for d in near:
        if d < 0:
            expected = expected + (inside(d).astype(jnp.int32) - late(d).astype(jnp.int32))
            awaited = awaited + late(d).astype(jnp.int32)
        else:
            expected = expected + inside(d).astype(jnp.int32)
    pl.semaphore_wait(barrier, expected)

    def signal_round(n, peer):
        pl.semaphore_signal(round_sem.at[n], inc=1, device_id=peer, device_id_type=MESH)

    for d in near:
        if d < 0:
            pl.when(late(d))(functools.partial(greet, {"lat": band + d}))
        else:
            pl.when(early(d))(functools.partial(signal_round, 3, {"lat": band + d}))
    pl.when(bottom)(lambda: greet(three_peer(DEEP - 1)))
    pl.when(top)(lambda: signal_round(3, three_peer(1)))

    def tell(n):
        if n:
            signal_round(n, three_peer(DEEP - 1))
        signal_round(n, three_peer(1))
        if n == 0:
            for step in (1, crosses - 1):
                signal_round(n, two_peer(step))

    def hear(n):
        pl.semaphore_wait(round_sem.at[n], 4 if n == 0 else 2)

    tell(0)

    def meta_copies(d):
        k = near.index(d)
        return [
            pltpu.make_async_remote_copy(
                src_ref=ref.at[REACH], dst_ref=ref.at[REACH - d],
                send_sem=meta_send.at[n, k], recv_sem=meta_recv.at[n, near.index(-d)],
                device_id={"lat": band + d}, device_id_type=MESH,
            )
            for n, ref in enumerate((real_meta, whole_meta))
        ]

    def meta_arrivals(d):
        k = near.index(d)
        return [
            pltpu.make_async_remote_copy(
                src_ref=ref.at[REACH + d], dst_ref=ref.at[REACH + d],
                send_sem=meta_send.at[n, k], recv_sem=meta_recv.at[n, k],
                device_id={"lat": band + d}, device_id_type=MESH,
            )
            for n, ref in enumerate((real_meta, whole_meta))
        ]

    def send_meta(d):
        for copy in meta_copies(d):
            copy.start()

    for d in near:
        pl.when(jnp.logical_and(inside(d), jnp.logical_not(late(d))) if d < 0 else inside(d))(
            functools.partial(send_meta, d)
        )

    def out_copy(c, dy):
        return pltpu.make_async_remote_copy(
            src_ref=fields_ref.at[cut(c, ring_member(dy))],
            dst_ref=window[c].at[pl.ds(span + member * rows, rows)],
            send_sem=out_send.at[c, dy - 1], recv_sem=out_recv.at[c, dy - 1],
            device_id={"lat": ring_peer(dy)}, device_id_type=MESH,
        )

    def out_arrival(c, dy):
        place = window[c].at[pl.ds(span + ring_member(RING - dy) * rows, rows)]
        return pltpu.make_async_remote_copy(
            src_ref=place, dst_ref=place, send_sem=out_send.at[c, dy - 1], recv_sem=out_recv.at[c, dy - 1],
            device_id={"lat": ring_peer(RING - dy)}, device_id_type=MESH,
        )

    has_side = (group < groups - 1, group > 0)

    def halo_place(c, dy, side):
        return window[c].at[pl.ds((0 if side == 0 else 2 * span) + ring_member(RING - dy) * rows, rows)]

    def halo_source(c, dy):
        if dy == 0:
            return fields_ref.at[cut(c, member)]
        return window[c].at[pl.ds(span + ring_member(RING - dy) * rows, rows)]

    def halo_copy(c, dy, side):
        return pltpu.make_async_remote_copy(
            src_ref=halo_source(c, dy), dst_ref=halo_place(c, dy, side),
            send_sem=halo_send.at[side, c, dy], recv_sem=halo_recv.at[side, c, dy],
            device_id={"lat": band + (RING if side == 0 else -RING)}, device_id_type=MESH,
        )

    edge = (jnp.logical_and(has_side[0], deep == DEEP - 1), jnp.logical_and(has_side[1], deep == 0))
    inner = tuple(jnp.logical_and(h, jnp.logical_not(e)) for h, e in zip(has_side, edge))
    shared = (cross + 1, crosses - cross)
    serves = (
        (jnp.logical_and(deep == DEEP - 1, cross > 0), cross),
        (jnp.logical_and(deep == 0, cross < crosses - 1), crosses - 1 - cross),
    )

    def pass_place(c, rank):
        return passing[c].at[pl.ds(rank * rows, rows)]

    def to_relay(c, dy, side):
        rank = RELAYED.index(dy)
        return pltpu.make_async_remote_copy(
            src_ref=halo_source(c, dy), dst_ref=pass_place(c, rank),
            send_sem=halo_send.at[side, c, dy], recv_sem=pass_recv.at[c, rank],
            device_id=two_peer(1 if side == 0 else crosses - 1), device_id_type=MESH,
        )

    def from_relay(c, dy, side):
        rank = RELAYED.index(dy)
        return pltpu.make_async_remote_copy(
            src_ref=pass_place(c, rank), dst_ref=halo_place(c, dy, side),
            send_sem=pass_send.at[c, rank], recv_sem=halo_recv.at[side, c, dy],
            device_id=three_peer(1 if side == 0 else DEEP - 1), device_id_type=MESH,
        )

    def at_relay(c, dy):
        rank = RELAYED.index(dy)
        place = pass_place(c, rank)
        return pltpu.make_async_remote_copy(
            src_ref=place, dst_ref=place, send_sem=pass_send.at[c, rank], recv_sem=pass_recv.at[c, rank],
            device_id=two_peer(1), device_id_type=MESH,
        )

    def start_edge(c, dy):
        for side in range(2):
            if dy in RELAYED:
                relayed = RELAYED.index(dy) < shared[side]
                pl.when(jnp.logical_and(edge[side], relayed))(lambda side=side: to_relay(c, dy, side).start())
                pl.when(jnp.logical_and(edge[side], jnp.logical_not(relayed)))(
                    lambda side=side: halo_copy(c, dy, side).start()
                )
            else:
                pl.when(edge[side])(lambda side=side: halo_copy(c, dy, side).start())

    def pass_along(c, dy):
        for side in range(2):
            serving, limit = serves[side]

            @pl.when(jnp.logical_and(serving, RELAYED.index(dy) < limit))
            def _(side=side):
                at_relay(c, dy).wait_recv()
                from_relay(c, dy, side).start()

    def passed_along(c, dy):
        for side in range(2):
            serving, limit = serves[side]
            pl.when(jnp.logical_and(serving, RELAYED.index(dy) < limit))(
                lambda side=side: from_relay(c, dy, side).wait_send()
            )

    def halo_arrival(c, dy, side):
        place = halo_place(c, dy, side)
        return pltpu.make_async_remote_copy(
            src_ref=place, dst_ref=place, send_sem=halo_send.at[side, c, dy], recv_sem=halo_recv.at[side, c, dy],
            device_id={"lat": band + (-RING if side == 0 else RING)}, device_id_type=MESH,
        )

    def start_halo(c, dy):
        for side in range(2):
            pl.when(inner[side])(lambda side=side: halo_copy(c, dy, side).start())

    def groups_of(c):
        parts = TAIL if c == count - 1 and rows % TAIL == 0 else 1
        return [(n, n * rows // parts, rows // parts) for n in range(parts)]

    def landing(c, place, first, height):
        f, begin, width = chunks[c]
        at = pl.ds(pl.multiple_of(place * piece + begin, LANES), width)
        return landed.at[pl.ds(first, height), f, :, at]

    def back_copy(c, dy, n, first, height):
        return pltpu.make_async_remote_copy(
            src_ref=column[c].at[pl.ds(dy * rows + first, height)], dst_ref=landing(c, member, first, height),
            send_sem=back_send.at[c, dy - 1, n], recv_sem=back_recv.at[c, dy - 1, n],
            device_id={"lat": ring_peer(dy)}, device_id_type=MESH,
        )

    def back_arrival(c, dy, n, first, height):
        place = landing(c, ring_member(RING - dy), first, height)
        return pltpu.make_async_remote_copy(
            src_ref=place, dst_ref=place, send_sem=back_send.at[c, dy - 1, n], recv_sem=back_recv.at[c, dy - 1, n],
            device_id={"lat": ring_peer(RING - dy)}, device_id_type=MESH,
        )

    def back_own(c):
        return pltpu.make_async_copy(column[c].at[pl.ds(0, rows)], landing(c, member, 0, rows), own_sem.at[1, c])

    def small_copy(source, target, sends, arrivals, k, peer):
        return pltpu.make_async_remote_copy(
            src_ref=source, dst_ref=target.at[k], send_sem=sends.at[k], recv_sem=arrivals.at[k],
            device_id=peer, device_id_type=MESH,
        )

    ones = [small_copy(part.at[0], met_one, one_send, one_recv, k, one_peer(*p)) for k, p in enumerate(one_peers)]
    twos = [small_copy(part.at[1], met_two, two_send, two_recv, dx - 1, two_peer(dx)) for dx in range(1, crosses)]
    threes = [small_copy(part.at[2], met_three, three_send, three_recv, dz - 1, three_peer(dz)) for dz in range(1, DEEP)]

    order = (1, RING - 1, *range(2, RING - 1))
    slots = [(c, 0) for c in range(min(LEAD, count))]
    for c in range(count):
        slots += [(c, dy) for dy in order] + [(c + LEAD, 0)] * (c + LEAD < count)
    place_of = {slot: k for k, slot in enumerate(slots)}
    start_halo(*slots[0])
    pl.when(top)(lambda: start_edge(*slots[0]))
    for c in range(min(2, count)):
        for dy in order:
            out_copy(c, dy).start()
    for slot in slots[1:LEAD]:
        start_halo(*slot)
        pl.when(top)(lambda slot=slot: start_edge(*slot))

    @pl.when(bottom)
    def _():
        pl.semaphore_wait(round_sem.at[3], awaited)
        for d in near:
            if d < 0:
                pl.when(late(d))(functools.partial(send_meta, d))
        for slot in slots[:LEAD]:
            start_edge(*slot)

    signal_round(0, three_peer(DEEP - 1))

    for d in near:
        @pl.when(inside(d))
        def _(d=d):
            for copy in meta_arrivals(d):
                copy.wait_recv()
    group_slots = pl.ds(REACH - member, RING)
    to_smem = [
        pltpu.make_async_copy(real_meta.at[group_slots], real_smem, smem_sem.at[0]),
        pltpu.make_async_copy(whole_meta.at[group_slots], whole_smem, smem_sem.at[1]),
    ]
    for copy in to_smem:
        copy.start()
    load.wait()

    def add_row(row, totals):
        taken = jnp.zeros((2 * REACH + 1, LANES), jnp.float32)
        for a in range(4):
            hit = whole_meta[:, 0, :] + a == first_row + row
            taken = taken + jnp.where(hit, real_meta[:, a, :] * real_meta[:, 4, :], 0.0)
        taken = jnp.sum(jnp.sum(taken, axis=0, keepdims=True), axis=1, keepdims=True)
        row_area = area_ref[first_row + row]
        before, after = [], []
        for f in range(field_count):
            tile = held[row, f, :, 0:LANES]
            for t in range(1, lon_count // LANES):
                tile = tile + held[row, f, :, t * LANES:(t + 1) * LANES]
            total = jnp.sum(tile, axis=0, keepdims=True)
            before.append(totals[f] + row_area * total)
            after.append(totals[field_count + f] + taken * total)
        return tuple(before + after)

    zero = jnp.zeros((1, LANES), jnp.float32)
    totals = lax.fori_loop(0, rows, add_row, (zero,) * (2 * field_count))
    part[0] = jnp.concatenate([*totals, jnp.zeros((8 - 2 * field_count, LANES), jnp.float32)], axis=0)

    def gather_small(copies, target, level):
        for copy in copies:
            copy.wait_recv()
        total = part[level]
        for k in range(len(copies)):
            total = total + target[k]
        return total

    for copy in ones:
        copy.start()
    for c in range(min(2, count), count):
        for dy in order:
            out_copy(c, dy).start()

    base = (group - 1) * span

    def interpolate(c, dy, first, height):
        to = ring_member(dy)

        def one_row(row, carry):
            place = whole_smem[to, 0, row] - base
            weight = [real_smem[to, a, row] for a in range(4)]
            for t in range(chunks[c][2] // LANES):
                at = pl.ds(t * LANES, LANES)
                total = weight[0] * window[c][place, :, at]
                for a in range(1, 4):
                    total = total + weight[a] * window[c][place + a, :, at]
                column[c][dy * rows + row, :, at] = total
            return carry

        lax.fori_loop(first, first + height, one_row, 0)

    def finish_chunk(c):
        if c == 0:
            for copy in to_smem:
                copy.wait()
        own_pieces[c].wait()
        for dy in (0, *order):
            for side in range(2):
                pl.when(has_side[1 - side])(lambda dy=dy, side=side: halo_arrival(c, dy, side).wait_recv())
        for n, first, height in groups_of(c):
            for dy in (2, 1, RING - 1, 0):
                interpolate(c, dy, first, height)
            for dy in (2, 1, RING - 1):
                back_copy(c, dy, n, first, height).start()
        back_own(c).start()

    def one_done():
        part[1] = gather_small(ones, met_one, 0)
        for copy in twos:
            copy.start()

    def two_done():
        part[2] = gather_small(twos, met_two, 1)
        hear(2)
        for copy in threes:
            copy.start()

    def pass_on(n):
        hear(n)
        tell(n + 1)

    lanes = lax.broadcasted_iota(jnp.int32, fields_ref.shape[2:3] + (LANES,), 1)
    tiles = lon_count // LANES

    def shifted(pieces, step):
        turned = [pltpu.roll(piece, LANES - step, 1) for piece in pieces]
        return [jnp.where(lanes < LANES - step, turned[t], turned[(t + 1) % tiles]) for t in range(tiles)]

    def along(f, sums):
        before = jnp.sum(sums[f:f + 1], axis=1, keepdims=True)
        after = jnp.sum(sums[field_count + f:field_count + f + 1], axis=1, keepdims=True)
        ratio = before / after

        def some_rows(together, step, carry):
            for n in range(together):
                row = step * together + n
                lon = [weight * ratio for weight in cubic(lon_t_ref[row])]
                here = [landed[row, f, :, t * LANES:(t + 1) * LANES] for t in range(tiles)]
                after = shifted(here, 1)
                later = shifted([lon[2] * here[t] + lon[3] * after[t] for t in range(tiles)], 2)
                moved = []
                for t in range(tiles):
                    mixed = lon[0] * here[t] + lon[1] * after[t] + later[t]
                    moved.append(mixed)
                first = lax.rem(shift_ref[row] - 1 + lon_count, lon_count)
                ahead = jnp.full(lanes.shape, first, jnp.int32)
                step_by = LANES
                while step_by < lon_count:
                    jump = (ahead & step_by) != 0
                    moved = [jnp.where(jump, moved[(t + step_by // LANES) % tiles], moved[t]) for t in range(tiles)]
                    step_by *= 2
                rest = ahead & (LANES - 1)
                pick = (lanes + rest) & (LANES - 1)
                moved = [jnp.take_along_axis(part_of, pick, axis=1) for part_of in moved]
                keep = lanes + rest < LANES
                for t in range(tiles):
                    out_ref[row, f, :, t * LANES:(t + 1) * LANES] = jnp.where(keep, moved[t], moved[(t + 1) % tiles])
            return carry

        mine = [c for c in range(count) if chunks[c][0] == f]
        for c in mine:
            back_own(c).wait()
            if c != mine[-1]:
                for dy in order:
                    for group_of in groups_of(c):
                        back_arrival(c, dy, *group_of).wait_recv()
        for group_of in groups_of(mine[-1]):
            for dy in order:
                back_arrival(mine[-1], dy, *group_of).wait_recv()
            _, first_of, height = group_of
            together = TOGETHER if height % TOGETHER == 0 and first_of % TOGETHER == 0 else height
            lax.fori_loop(
                first_of // together, (first_of + height) // together, functools.partial(some_rows, together), 0
            )

    sums = []
    tasks = {k: [] for k in range(len(slots) + LATE)}
    tasks[4].append(functools.partial(pass_on, 0))
    tasks[6].append(one_done)
    tasks[7].append(functools.partial(pass_on, 1))
    tasks[9].append(two_done)
    for c in range(count):
        tasks[place_of[c, order[-1]] + LATE].append(functools.partial(finish_chunk, c))
    tasks[place_of[count - 3 - EARLIER, order[-1]] + LATE].append(
        lambda: sums.append(gather_small(threes, met_three, 2))
    )
    for f in range(field_count - 1):
        near_end = count - field_count + 1 + f - EARLIER
        tasks[place_of[near_end - 1, order[-1]] + LATE].append(functools.partial(lambda f: along(f, sums[0]), f))
    sent_at = {slot: k + 1 for k, slot in enumerate(slots[:LEAD])}
    arrived = set()

    def await_arrival(slot):
        if slot[1] and slot not in arrived:
            arrived.add(slot)
            out_arrival(*slot).wait_recv()

    reached = LEAD
    for k in range(LEAD, len(slots) + LATE):
        if k < len(slots):
            await_arrival(slots[k])
            for side in range(2):
                pl.when(inner[side])(lambda k=k, side=side: halo_copy(*slots[k - LEAD], side).wait_send())
            start_halo(*slots[k])
            until = min(len(slots), LEAD + -(-(k - LEAD + 1) * RING // (RING - 1)))
            for slot in slots[reached:until]:
                await_arrival(slot)
                start_edge(*slot)
                sent_at[slot] = k
            reached = until
        for slot in slots:
            if slot[1] in RELAYED and slot in sent_at and max(sent_at[slot] + HOPS, LEAD) == k:
                pass_along(*slot)
        for task in tasks[k]:
            task()

    along(field_count - 1, sums[0])
    for d in near:
        @pl.when(inside(d))
        def _(d=d):
            for copy in meta_copies(d):
                copy.wait_send()
    for copy in ones + twos + threes:
        copy.wait_send()
    for c in range(count):
        for dy in order:
            out_copy(c, dy).wait_send()
            for group_of in groups_of(c):
                back_copy(c, dy, *group_of).wait_send()
    for k, slot in enumerate(slots):
        for side in range(2):
            if k >= len(slots) - LEAD:
                pl.when(inner[side])(lambda slot=slot, side=side: halo_copy(*slot, side).wait_send())
            pl.when(edge[side])(lambda slot=slot, side=side: halo_copy(*slot, side).wait_send())
        if slot[1] in RELAYED:
            passed_along(*slot)


def exchange(lat_t, lon_t, shift, departure_row, extents, area, fields):
    bands, levs = lax.axis_size("lat"), lax.axis_size("lev")
    rows, field_count, levels, lon_count = fields.shape
    crosses = bands // RING // DEEP
    piece = lon_count // RING
    tile = (8, LANES)
    dma = pltpu.SemaphoreType.DMA
    ones = RING * levs - 1
    near = 2 * REACH
    chunks = chunks_of(field_count, piece // LANES)
    count = len(chunks)
    return pl.pallas_call(
        functools.partial(exchange_kernel, bands, levs),
        out_shape=pltpu.VMEM(fields.shape, fields.dtype),
        in_specs=[pl.BlockSpec(memory_space=pltpu.SMEM)] * 6 + [pl.BlockSpec(memory_space=pl.ANY)],
        out_specs=pl.BlockSpec(memory_space=pltpu.VMEM),
        scratch_shapes=[
            pltpu.VMEM(fields.shape, jnp.float32),
            pltpu.VMEM(fields.shape, jnp.float32),
            *[pltpu.VMEM((3 * RING * rows, levels, width), jnp.float32) for _, _, width in chunks],
            *[pltpu.VMEM((RING * rows, levels, width), jnp.float32) for _, _, width in chunks],
            *[pltpu.VMEM((len(RELAYED) * rows, levels, width), jnp.float32) for _, _, width in chunks],
            pltpu.VMEM((near + 1,) + tile, jnp.float32),
            pltpu.VMEM((near + 1,) + tile, jnp.int32),
            pltpu.SMEM((RING,) + tile, jnp.float32),
            pltpu.SMEM((RING,) + tile, jnp.int32),
            pltpu.VMEM((3,) + tile, jnp.float32),
            pltpu.VMEM((ones,) + tile, jnp.float32),
            pltpu.VMEM((max(crosses - 1, 1),) + tile, jnp.float32),
            pltpu.VMEM((DEEP - 1,) + tile, jnp.float32),
            dma,
            dma((2, count)),
            dma((2,)),
            dma((2, near)),
            dma((2, near)),
            dma((count, RING - 1)),
            dma((count, RING - 1)),
            dma((2, count, RING)),
            dma((2, count, RING)),
            dma((count, RING - 1, TAIL)),
            dma((count, RING - 1, TAIL)),
            dma((ones,)),
            dma((ones,)),
            dma((max(crosses - 1, 1),)),
            dma((max(crosses - 1, 1),)),
            dma((DEEP - 1,)),
            dma((DEEP - 1,)),
            pltpu.SemaphoreType.REGULAR((4,)),
            dma((count, len(RELAYED))),
            dma((count, len(RELAYED))),
        ],
        compiler_params=pltpu.CompilerParams(
            collective_id=0, has_side_effects=True, vmem_limit_bytes=60000 * 1024
        ),
        name="exchange",
    )(lat_t, lon_t, shift, departure_row, extents, area, fields)


def per_device(fields, lat_fraction, lon_fraction, lon_shift, departure_row, extents):
    bands = lax.axis_size("lat")
    total_rows = bands * fields.shape[0]
    row_ids = np.arange(total_rows)
    area = jnp.asarray(np.cos(math.pi * (row_ids + 0.5) / total_rows - math.pi / 2.0), jnp.float32)
    return exchange(lat_fraction, lon_fraction, lon_shift, departure_row, extents, area, fields)


def solution(mesh):
    return jax.shard_map(
        per_device,
        mesh=mesh,
        in_specs=(
            P("lat", None, "lev", None),
            P("lat"),
            P("lat"),
            P("lat"),
            P("lat"),
            P("lat", None),
        ),
        out_specs=P("lat", None, "lev", None),
        check_vma=False,
    )
```

```python
import functools
import math

import jax
import jax.numpy as jnp
import numpy as np
from jax import lax
from jax.experimental import pallas as pl
from jax.experimental.pallas import tpu as pltpu
from jax.sharding import PartitionSpec as P

REACH = 4
LANES = 128
RING = 4
DEEP = 8
MESH = pl.DeviceIdType.MESH
CUTS = ((5,), (3, 2), (3, 2))
LEAD = 3
HOPS = 2
RELAYED = (0, 1, RING - 1)
LATE = 4
EARLIER = 0
TOGETHER = 2
TAIL = 2


def chunks_of(field_count, tiles):
    found = []
    for f in range(field_count):
        cuts = CUTS[f] if f < len(CUTS) and sum(CUTS[f]) == tiles else (tiles,)
        first = 0
        for width in cuts:
            found.append((f, first * LANES, width * LANES))
            first += width
    return found


def cubic(t):
    sixth = 1.0 / 6.0
    return (
        -t * (t - 1.0) * (t - 2.0) * sixth,
        (t + 1.0) * (t - 1.0) * (t - 2.0) * 0.5,
        -(t + 1.0) * t * (t - 2.0) * 0.5,
        (t + 1.0) * t * (t - 1.0) * sixth,
    )


def departure_of(row, first_row, rows, total_rows, departure_ref, extents_ref):
    low = first_row - extents_ref[0, 0] * rows + 1
    high = first_row + rows - 3 + extents_ref[0, 1] * rows
    inside = jnp.minimum(jnp.maximum(departure_ref[row], low), high)
    return jnp.minimum(jnp.maximum(inside, 1), total_rows - 3)


def exchange_kernel(bands, levs, lat_t_ref, lon_t_ref, shift_ref, departure_ref, extents_ref, area_ref, fields_ref,
                    out_ref, *scratch):
    rows, field_count, _, lon_count = fields_ref.shape
    piece = lon_count // RING
    chunks = chunks_of(field_count, piece // LANES)
    count = len(chunks)
    held, landed = scratch[:2]
    window = scratch[2:2 + count]
    column = scratch[2 + count:2 + 2 * count]
    passing = scratch[2 + 2 * count:2 + 3 * count]
    (real_meta, whole_meta, real_smem, whole_smem, part, met_one, met_two, met_three,
     load_sem, own_sem, smem_sem, meta_send, meta_recv, out_send, out_recv, halo_send, halo_recv,
     back_send, back_recv, one_send, one_recv, two_send, two_recv, three_send, three_recv,
     round_sem, pass_send, pass_recv) = scratch[2 + 3 * count:]
    band, lev = lax.axis_index("lat"), lax.axis_index("lev")
    group, member = band // RING, lax.rem(band, RING)
    groups = bands // RING
    crosses = groups // DEEP
    deep, cross = lax.rem(group, DEEP), group // DEEP
    first_row, total_rows = band * rows, bands * rows
    span = RING * rows

    def ring_member(step):
        return lax.rem(member + step, RING)

    def ring_peer(step):
        return group * RING + ring_member(step)

    def inside(distance):
        place = band + distance
        return jnp.logical_and(place >= 0, place < bands)

    near = [d for d in range(-REACH, REACH + 1) if d != 0]
    one_peers = [(dy, dl) for dy in range(RING) for dl in range(levs) if (dy, dl) != (0, 0)]

    def one_peer(dy, dl):
        return {"lat": ring_peer(dy), "lev": lax.rem(lev + dl, levs)}

    def two_peer(dx):
        return {"lat": (lax.rem(cross + dx, crosses) * DEEP + deep) * RING + member}

    def three_peer(dz):
        return {"lat": (cross * DEEP + lax.rem(deep + dz, DEEP)) * RING + member}

    barrier = pltpu.get_barrier_semaphore()

    def greet(peer):
        pl.semaphore_signal(barrier, inc=1, device_id=peer, device_id_type=MESH)

    bottom, top = deep == 0, deep == DEEP - 1

    def late(d):
        return jnp.logical_and(inside(d), jnp.logical_and(bottom, member + d < 0))

    def early(d):
        return jnp.logical_and(inside(d), jnp.logical_and(top, member + d >= RING))

    def prompt(d):
        return jnp.logical_and(inside(d), jnp.logical_not(late(d) if d < 0 else early(d)))

    for d in near:
        pl.when(prompt(d))(functools.partial(greet, {"lat": band + d}))
    for dy, dl in one_peers:
        if dl:
            greet(one_peer(dy, dl))
    for step in (1, crosses - 1):
        greet(two_peer(step))
    pl.when(jnp.logical_not(top))(lambda: greet(three_peer(1)))
    pl.when(jnp.logical_not(bottom))(lambda: greet(three_peer(DEEP - 1)))

    load = pltpu.make_async_copy(fields_ref, held, load_sem)
    load.start()

    def cut(c, place):
        f, first, width = chunks[c]
        return (slice(None), f, slice(None), pl.ds(pl.multiple_of(place * piece + first, LANES), width))

    own_pieces = [
        pltpu.make_async_copy(
            fields_ref.at[cut(c, member)], window[c].at[pl.ds(span + member * rows, rows)], own_sem.at[0, c]
        )
        for c in range(count)
    ]
    for copy in own_pieces:
        copy.start()

    lane = lax.broadcasted_iota(jnp.int32, (1, LANES), 1)
    lat_t = jnp.zeros((1, LANES), jnp.float32)
    lon_t = jnp.zeros((1, LANES), jnp.float32)
    area = jnp.zeros((1, LANES), jnp.float32)
    start = jnp.zeros((1, LANES), jnp.int32)
    for row in range(rows):
        here = lane == row
        lat_t = jnp.where(here, lat_t_ref[row], lat_t)
        lon_t = jnp.where(here, lon_t_ref[row], lon_t)
        area = jnp.where(here, area_ref[first_row + row], area)
        departure = departure_of(row, first_row, rows, total_rows, departure_ref, extents_ref)
        start = jnp.where(here, departure - 1, start)
    lon_w = cubic(lon_t)
    for d in near:
        @pl.when(jnp.logical_not(inside(d)))
        def _(d=d):
            real_meta[REACH + d] = jnp.zeros(real_meta.shape[1:], jnp.float32)
            whole_meta[REACH + d] = jnp.zeros(whole_meta.shape[1:], jnp.int32)
    real_meta[REACH] = jnp.concatenate(
        [*cubic(lat_t), area * (lon_w[0] + lon_w[1] + lon_w[2] + lon_w[3]), jnp.zeros((3, LANES), jnp.float32)], axis=0
    )
    whole_meta[REACH] = jnp.broadcast_to(start, whole_meta.shape[1:])

    expected = sum(dl != 0 for _, dl in one_peers) + 3 + jnp.logical_not(bottom).astype(jnp.int32)
    awaited = 1
    for d in near:
        if d < 0:
            expected = expected + (inside(d).astype(jnp.int32) - late(d).astype(jnp.int32))
            awaited = awaited + late(d).astype(jnp.int32)
        else:
            expected = expected + inside(d).astype(jnp.int32)
    pl.semaphore_wait(barrier, expected)

    def signal_round(n, peer):
        pl.semaphore_signal(round_sem.at[n], inc=1, device_id=peer, device_id_type=MESH)

    for d in near:
        if d < 0:
            pl.when(late(d))(functools.partial(greet, {"lat": band + d}))
        else:
            pl.when(early(d))(functools.partial(signal_round, 3, {"lat": band + d}))
    pl.when(bottom)(lambda: greet(three_peer(DEEP - 1)))
    pl.when(top)(lambda: signal_round(3, three_peer(1)))

    def tell(n):
        if n:
            signal_round(n, three_peer(DEEP - 1))
        signal_round(n, three_peer(1))
        if n == 0:
            for step in (1, crosses - 1):
                signal_round(n, two_peer(step))

    def hear(n):
        pl.semaphore_wait(round_sem.at[n], 4 if n == 0 else 2)

    tell(0)

    def meta_copies(d):
        k = near.index(d)
        return [
            pltpu.make_async_remote_copy(
                src_ref=ref.at[REACH], dst_ref=ref.at[REACH - d],
                send_sem=meta_send.at[n, k], recv_sem=meta_recv.at[n, near.index(-d)],
                device_id={"lat": band + d}, device_id_type=MESH,
            )
            for n, ref in enumerate((real_meta, whole_meta))
        ]

    def meta_arrivals(d):
        k = near.index(d)
        return [
            pltpu.make_async_remote_copy(
                src_ref=ref.at[REACH + d], dst_ref=ref.at[REACH + d],
                send_sem=meta_send.at[n, k], recv_sem=meta_recv.at[n, k],
                device_id={"lat": band + d}, device_id_type=MESH,
            )
            for n, ref in enumerate((real_meta, whole_meta))
        ]

    def send_meta(d):
        for copy in meta_copies(d):
            copy.start()

    for d in near:
        pl.when(jnp.logical_and(inside(d), jnp.logical_not(late(d))) if d < 0 else inside(d))(
            functools.partial(send_meta, d)
        )

    def out_copy(c, dy):
        return pltpu.make_async_remote_copy(
            src_ref=fields_ref.at[cut(c, ring_member(dy))],
            dst_ref=window[c].at[pl.ds(span + member * rows, rows)],
            send_sem=out_send.at[c, dy - 1], recv_sem=out_recv.at[c, dy - 1],
            device_id={"lat": ring_peer(dy)}, device_id_type=MESH,
        )

    def out_arrival(c, dy):
        place = window[c].at[pl.ds(span + ring_member(RING - dy) * rows, rows)]
        return pltpu.make_async_remote_copy(
            src_ref=place, dst_ref=place, send_sem=out_send.at[c, dy - 1], recv_sem=out_recv.at[c, dy - 1],
            device_id={"lat": ring_peer(RING - dy)}, device_id_type=MESH,
        )

    has_side = (group < groups - 1, group > 0)

    def halo_place(c, dy, side):
        return window[c].at[pl.ds((0 if side == 0 else 2 * span) + ring_member(RING - dy) * rows, rows)]

    def halo_source(c, dy):
        if dy == 0:
            return fields_ref.at[cut(c, member)]
        return window[c].at[pl.ds(span + ring_member(RING - dy) * rows, rows)]

    def halo_copy(c, dy, side):
        return pltpu.make_async_remote_copy(
            src_ref=halo_source(c, dy), dst_ref=halo_place(c, dy, side),
            send_sem=halo_send.at[side, c, dy], recv_sem=halo_recv.at[side, c, dy],
            device_id={"lat": band + (RING if side == 0 else -RING)}, device_id_type=MESH,
        )

    edge = (jnp.logical_and(has_side[0], deep == DEEP - 1), jnp.logical_and(has_side[1], deep == 0))
    inner = tuple(jnp.logical_and(h, jnp.logical_not(e)) for h, e in zip(has_side, edge))
    shared = (cross + 1, crosses - cross)
    serves = (
        (jnp.logical_and(deep == DEEP - 1, cross > 0), cross),
        (jnp.logical_and(deep == 0, cross < crosses - 1), crosses - 1 - cross),
    )

    def pass_place(c, rank):
        return passing[c].at[pl.ds(rank * rows, rows)]

    def to_relay(c, dy, side):
        rank = RELAYED.index(dy)
        return pltpu.make_async_remote_copy(
            src_ref=halo_source(c, dy), dst_ref=pass_place(c, rank),
            send_sem=halo_send.at[side, c, dy], recv_sem=pass_recv.at[c, rank],
            device_id=two_peer(1 if side == 0 else crosses - 1), device_id_type=MESH,
        )

    def from_relay(c, dy, side):
        rank = RELAYED.index(dy)
        return pltpu.make_async_remote_copy(
            src_ref=pass_place(c, rank), dst_ref=halo_place(c, dy, side),
            send_sem=pass_send.at[c, rank], recv_sem=halo_recv.at[side, c, dy],
            device_id=three_peer(1 if side == 0 else DEEP - 1), device_id_type=MESH,
        )

    def at_relay(c, dy):
        rank = RELAYED.index(dy)
        place = pass_place(c, rank)
        return pltpu.make_async_remote_copy(
            src_ref=place, dst_ref=place, send_sem=pass_send.at[c, rank], recv_sem=pass_recv.at[c, rank],
            device_id=two_peer(1), device_id_type=MESH,
        )

    def start_edge(c, dy):
        for side in range(2):
            if dy in RELAYED:
                relayed = RELAYED.index(dy) < shared[side]
                pl.when(jnp.logical_and(edge[side], relayed))(lambda side=side: to_relay(c, dy, side).start())
                pl.when(jnp.logical_and(edge[side], jnp.logical_not(relayed)))(
                    lambda side=side: halo_copy(c, dy, side).start()
                )
            else:
                pl.when(edge[side])(lambda side=side: halo_copy(c, dy, side).start())

    def pass_along(c, dy):
        for side in range(2):
            serving, limit = serves[side]

            @pl.when(jnp.logical_and(serving, RELAYED.index(dy) < limit))
            def _(side=side):
                at_relay(c, dy).wait_recv()
                from_relay(c, dy, side).start()

    def passed_along(c, dy):
        for side in range(2):
            serving, limit = serves[side]
            pl.when(jnp.logical_and(serving, RELAYED.index(dy) < limit))(
                lambda side=side: from_relay(c, dy, side).wait_send()
            )

    def halo_arrival(c, dy, side):
        place = halo_place(c, dy, side)
        return pltpu.make_async_remote_copy(
            src_ref=place, dst_ref=place, send_sem=halo_send.at[side, c, dy], recv_sem=halo_recv.at[side, c, dy],
            device_id={"lat": band + (-RING if side == 0 else RING)}, device_id_type=MESH,
        )

    def start_halo(c, dy):
        for side in range(2):
            pl.when(inner[side])(lambda side=side: halo_copy(c, dy, side).start())

    def groups_of(c):
        parts = TAIL if c == count - 1 and rows % TAIL == 0 else 1
        return [(n, n * rows // parts, rows // parts) for n in range(parts)]

    def landing(c, place, first, height):
        f, begin, width = chunks[c]
        at = pl.ds(pl.multiple_of(place * piece + begin, LANES), width)
        return landed.at[pl.ds(first, height), f, :, at]

    def back_copy(c, dy, n, first, height):
        return pltpu.make_async_remote_copy(
            src_ref=column[c].at[pl.ds(dy * rows + first, height)], dst_ref=landing(c, member, first, height),
            send_sem=back_send.at[c, dy - 1, n], recv_sem=back_recv.at[c, dy - 1, n],
            device_id={"lat": ring_peer(dy)}, device_id_type=MESH,
        )

    def back_arrival(c, dy, n, first, height):
        place = landing(c, ring_member(RING - dy), first, height)
        return pltpu.make_async_remote_copy(
            src_ref=place, dst_ref=place, send_sem=back_send.at[c, dy - 1, n], recv_sem=back_recv.at[c, dy - 1, n],
            device_id={"lat": ring_peer(RING - dy)}, device_id_type=MESH,
        )

    def back_own(c):
        return pltpu.make_async_copy(column[c].at[pl.ds(0, rows)], landing(c, member, 0, rows), own_sem.at[1, c])

    def small_copy(source, target, sends, arrivals, k, peer):
        return pltpu.make_async_remote_copy(
            src_ref=source, dst_ref=target.at[k], send_sem=sends.at[k], recv_sem=arrivals.at[k],
            device_id=peer, device_id_type=MESH,
        )

    ones = [small_copy(part.at[0], met_one, one_send, one_recv, k, one_peer(*p)) for k, p in enumerate(one_peers)]
    twos = [small_copy(part.at[1], met_two, two_send, two_recv, dx - 1, two_peer(dx)) for dx in range(1, crosses)]
    threes = [small_copy(part.at[2], met_three, three_send, three_recv, dz - 1, three_peer(dz)) for dz in range(1, DEEP)]

    order = (1, RING - 1, *range(2, RING - 1))
    slots = [(c, 0) for c in range(min(LEAD, count))]
    for c in range(count):
        slots += [(c, dy) for dy in order] + [(c + LEAD, 0)] * (c + LEAD < count)
    place_of = {slot: k for k, slot in enumerate(slots)}
    start_halo(*slots[0])
    pl.when(top)(lambda: start_edge(*slots[0]))
    for c in range(min(2, count)):
        for dy in order:
            out_copy(c, dy).start()
    for slot in slots[1:LEAD]:
        start_halo(*slot)
        pl.when(top)(lambda slot=slot: start_edge(*slot))

    @pl.when(bottom)
    def _():
        pl.semaphore_wait(round_sem.at[3], awaited)
        for d in near:
            if d < 0:
                pl.when(late(d))(functools.partial(send_meta, d))
        for slot in slots[:LEAD]:
            start_edge(*slot)

    signal_round(0, three_peer(DEEP - 1))

    for d in near:
        @pl.when(inside(d))
        def _(d=d):
            for copy in meta_arrivals(d):
                copy.wait_recv()
    group_slots = pl.ds(REACH - member, RING)
    to_smem = [
        pltpu.make_async_copy(real_meta.at[group_slots], real_smem, smem_sem.at[0]),
        pltpu.make_async_copy(whole_meta.at[group_slots], whole_smem, smem_sem.at[1]),
    ]
    for copy in to_smem:
        copy.start()
    load.wait()

    def add_row(row, totals):
        taken = jnp.zeros((2 * REACH + 1, LANES), jnp.float32)
        for a in range(4):
            hit = whole_meta[:, 0, :] + a == first_row + row
            taken = taken + jnp.where(hit, real_meta[:, a, :] * real_meta[:, 4, :], 0.0)
        taken = jnp.sum(jnp.sum(taken, axis=0, keepdims=True), axis=1, keepdims=True)
        row_area = area_ref[first_row + row]
        before, after = [], []
        for f in range(field_count):
            tile = held[row, f, :, 0:LANES]
            for t in range(1, lon_count // LANES):
                tile = tile + held[row, f, :, t * LANES:(t + 1) * LANES]
            total = jnp.sum(tile, axis=0, keepdims=True)
            before.append(totals[f] + row_area * total)
            after.append(totals[field_count + f] + taken * total)
        return tuple(before + after)

    zero = jnp.zeros((1, LANES), jnp.float32)
    totals = lax.fori_loop(0, rows, add_row, (zero,) * (2 * field_count))
    part[0] = jnp.concatenate([*totals, jnp.zeros((8 - 2 * field_count, LANES), jnp.float32)], axis=0)

    def gather_small(copies, target, level):
        for copy in copies:
            copy.wait_recv()
        total = part[level]
        for k in range(len(copies)):
            total = total + target[k]
        return total

    for copy in ones:
        copy.start()
    for c in range(min(2, count), count):
        for dy in order:
            out_copy(c, dy).start()

    base = (group - 1) * span

    def interpolate(c, dy, first, height):
        to = ring_member(dy)

        def one_row(row, carry):
            place = whole_smem[to, 0, row] - base
            weight = [real_smem[to, a, row] for a in range(4)]
            for t in range(chunks[c][2] // LANES):
                at = pl.ds(t * LANES, LANES)
                total = weight[0] * window[c][place, :, at]
                for a in range(1, 4):
                    total = total + weight[a] * window[c][place + a, :, at]
                column[c][dy * rows + row, :, at] = total
            return carry

        lax.fori_loop(first, first + height, one_row, 0)

    def finish_chunk(c):
        if c == 0:
            for copy in to_smem:
                copy.wait()
        own_pieces[c].wait()
        for dy in (0, *order):
            for side in range(2):
                pl.when(has_side[1 - side])(lambda dy=dy, side=side: halo_arrival(c, dy, side).wait_recv())
        for n, first, height in groups_of(c):
            for dy in (2, 1, RING - 1, 0):
                interpolate(c, dy, first, height)
            for dy in (2, 1, RING - 1):
                back_copy(c, dy, n, first, height).start()
        back_own(c).start()

    def one_done():
        part[1] = gather_small(ones, met_one, 0)
        for copy in twos:
            copy.start()

    def two_done():
        part[2] = gather_small(twos, met_two, 1)
        hear(2)
        for copy in threes:
            copy.start()

    def pass_on(n):
        hear(n)
        tell(n + 1)

    lanes = lax.broadcasted_iota(jnp.int32, fields_ref.shape[2:3] + (LANES,), 1)
    tiles = lon_count // LANES

    def shifted(pieces, step):
        turned = [pltpu.roll(piece, LANES - step, 1) for piece in pieces]
        return [jnp.where(lanes < LANES - step, turned[t], turned[(t + 1) % tiles]) for t in range(tiles)]

    def along(f, sums):
        before = jnp.sum(sums[f:f + 1], axis=1, keepdims=True)
        after = jnp.sum(sums[field_count + f:field_count + f + 1], axis=1, keepdims=True)
        ratio = before / after

        def some_rows(together, step, carry):
            for n in range(together):
                row = step * together + n
                lon = [weight * ratio for weight in cubic(lon_t_ref[row])]
                here = [landed[row, f, :, t * LANES:(t + 1) * LANES] for t in range(tiles)]
                after = shifted(here, 1)
                later = shifted([lon[2] * here[t] + lon[3] * after[t] for t in range(tiles)], 2)
                moved = []
                for t in range(tiles):
                    mixed = lon[0] * here[t] + lon[1] * after[t] + later[t]
                    moved.append(mixed)
                first = lax.rem(shift_ref[row] - 1 + lon_count, lon_count)
                ahead = jnp.full(lanes.shape, first, jnp.int32)
                step_by = LANES
                while step_by < lon_count:
                    jump = (ahead & step_by) != 0
                    moved = [jnp.where(jump, moved[(t + step_by // LANES) % tiles], moved[t]) for t in range(tiles)]
                    step_by *= 2
                rest = ahead & (LANES - 1)
                pick = (lanes + rest) & (LANES - 1)
                moved = [jnp.take_along_axis(part_of, pick, axis=1) for part_of in moved]
                keep = lanes + rest < LANES
                for t in range(tiles):
                    out_ref[row, f, :, t * LANES:(t + 1) * LANES] = jnp.where(keep, moved[t], moved[(t + 1) % tiles])
            return carry

        mine = [c for c in range(count) if chunks[c][0] == f]
        for c in mine:
            back_own(c).wait()
            if c != mine[-1]:
                for dy in order:
                    for group_of in groups_of(c):
                        back_arrival(c, dy, *group_of).wait_recv()
        for group_of in groups_of(mine[-1]):
            for dy in order:
                back_arrival(mine[-1], dy, *group_of).wait_recv()
            _, first_of, height = group_of
            together = TOGETHER if height % TOGETHER == 0 and first_of % TOGETHER == 0 else height
            lax.fori_loop(
                first_of // together, (first_of + height) // together, functools.partial(some_rows, together), 0
            )

    sums = []
    tasks = {k: [] for k in range(len(slots) + LATE)}
    tasks[4].append(functools.partial(pass_on, 0))
    tasks[6].append(one_done)
    tasks[7].append(functools.partial(pass_on, 1))
    tasks[9].append(two_done)
    for c in range(count):
        tasks[place_of[c, order[-1]] + LATE].append(functools.partial(finish_chunk, c))
    tasks[place_of[count - 3 - EARLIER, order[-1]] + LATE].append(
        lambda: sums.append(gather_small(threes, met_three, 2))
    )
    for f in range(field_count - 1):
        near_end = count - field_count + 1 + f - EARLIER
        tasks[place_of[near_end - 1, order[-1]] + LATE].append(functools.partial(lambda f: along(f, sums[0]), f))
    sent_at = {slot: k + 1 for k, slot in enumerate(slots[:LEAD])}
    arrived = set()

    def await_arrival(slot):
        if slot[1] and slot not in arrived:
            arrived.add(slot)
            out_arrival(*slot).wait_recv()

    reached = LEAD
    for k in range(LEAD, len(slots) + LATE):
        if k < len(slots):
            await_arrival(slots[k])
            for side in range(2):
                pl.when(inner[side])(lambda k=k, side=side: halo_copy(*slots[k - LEAD], side).wait_send())
            start_halo(*slots[k])
            until = min(len(slots), LEAD + -(-(k - LEAD + 1) * RING // (RING - 1)))
            for slot in slots[reached:until]:
                await_arrival(slot)
                start_edge(*slot)
                sent_at[slot] = k
            reached = until
        for slot in slots:
            if slot[1] in RELAYED and slot in sent_at and max(sent_at[slot] + HOPS, LEAD) == k:
                pass_along(*slot)
        for task in tasks[k]:
            task()

    for d in near:
        @pl.when(inside(d))
        def _(d=d):
            for copy in meta_copies(d):
                copy.wait_send()
    for copy in ones + twos + threes:
        copy.wait_send()
    for c in range(count):
        for dy in order:
            out_copy(c, dy).wait_send()
    for k, slot in enumerate(slots):
        for side in range(2):
            if k >= len(slots) - LEAD:
                pl.when(inner[side])(lambda slot=slot, side=side: halo_copy(*slot, side).wait_send())
            pl.when(edge[side])(lambda slot=slot, side=side: halo_copy(*slot, side).wait_send())
        if slot[1] in RELAYED:
            passed_along(*slot)
    along(field_count - 1, sums[0])
    for c in range(count):
        for dy in order:
            for group_of in groups_of(c):
                back_copy(c, dy, *group_of).wait_send()


def exchange(lat_t, lon_t, shift, departure_row, extents, area, fields):
    bands, levs = lax.axis_size("lat"), lax.axis_size("lev")
    rows, field_count, levels, lon_count = fields.shape
    crosses = bands // RING // DEEP
    piece = lon_count // RING
    tile = (8, LANES)
    dma = pltpu.SemaphoreType.DMA
    ones = RING * levs - 1
    near = 2 * REACH
    chunks = chunks_of(field_count, piece // LANES)
    count = len(chunks)
    return pl.pallas_call(
        functools.partial(exchange_kernel, bands, levs),
        out_shape=pltpu.VMEM(fields.shape, fields.dtype),
        in_specs=[pl.BlockSpec(memory_space=pltpu.SMEM)] * 6 + [pl.BlockSpec(memory_space=pl.ANY)],
        out_specs=pl.BlockSpec(memory_space=pltpu.VMEM),
        scratch_shapes=[
            pltpu.VMEM(fields.shape, jnp.float32),
            pltpu.VMEM(fields.shape, jnp.float32),
            *[pltpu.VMEM((3 * RING * rows, levels, width), jnp.float32) for _, _, width in chunks],
            *[pltpu.VMEM((RING * rows, levels, width), jnp.float32) for _, _, width in chunks],
            *[pltpu.VMEM((len(RELAYED) * rows, levels, width), jnp.float32) for _, _, width in chunks],
            pltpu.VMEM((near + 1,) + tile, jnp.float32),
            pltpu.VMEM((near + 1,) + tile, jnp.int32),
            pltpu.SMEM((RING,) + tile, jnp.float32),
            pltpu.SMEM((RING,) + tile, jnp.int32),
            pltpu.VMEM((3,) + tile, jnp.float32),
            pltpu.VMEM((ones,) + tile, jnp.float32),
            pltpu.VMEM((max(crosses - 1, 1),) + tile, jnp.float32),
            pltpu.VMEM((DEEP - 1,) + tile, jnp.float32),
            dma,
            dma((2, count)),
            dma((2,)),
            dma((2, near)),
            dma((2, near)),
            dma((count, RING - 1)),
            dma((count, RING - 1)),
            dma((2, count, RING)),
            dma((2, count, RING)),
            dma((count, RING - 1, TAIL)),
            dma((count, RING - 1, TAIL)),
            dma((ones,)),
            dma((ones,)),
            dma((max(crosses - 1, 1),)),
            dma((max(crosses - 1, 1),)),
            dma((DEEP - 1,)),
            dma((DEEP - 1,)),
            pltpu.SemaphoreType.REGULAR((4,)),
            dma((count, len(RELAYED))),
            dma((count, len(RELAYED))),
        ],
        compiler_params=pltpu.CompilerParams(
            collective_id=0, has_side_effects=True, vmem_limit_bytes=60000 * 1024
        ),
        name="exchange",
    )(lat_t, lon_t, shift, departure_row, extents, area, fields)


def per_device(fields, lat_fraction, lon_fraction, lon_shift, departure_row, extents):
    bands = lax.axis_size("lat")
    total_rows = bands * fields.shape[0]
    row_ids = np.arange(total_rows)
    area = jnp.asarray(np.cos(math.pi * (row_ids + 0.5) / total_rows - math.pi / 2.0), jnp.float32)
    return exchange(lat_fraction, lon_fraction, lon_shift, departure_row, extents, area, fields)


def solution(mesh):
    return jax.shard_map(
        per_device,
        mesh=mesh,
        in_specs=(
            P("lat", None, "lev", None),
            P("lat"),
            P("lat"),
            P("lat"),
            P("lat"),
            P("lat", None),
        ),
        out_specs=P("lat", None, "lev", None),
        check_vma=False,
    )
```
